256 devices in a mesh: gx: 16 (over x, z_lo), gy: 4 (over z_hi, core), gz: 4 (over y).
Axes of the slice: x: 4, y: 4, z: 8 (z_hi: 2, z_lo: 4; z = z_hi * 4 + z_lo), core: 2. Of those that a mesh axis runs over, the one named last changes fastest.
Arguments:
- state_old: float32 [5, 256, 128, 512], P(None, 'gx', 'gy', 'gz'), as said below
- state_section: float32 [5, 256, 128, 512], P(None, 'gx', 'gy', 'gz'), as said below
- panel_record: bfloat16 [1048576, 512], P(('gx', 'gy', 'gz')), may hold values from -6 to 6
- panel_cell: int32 [8192, 128], P(('gx', 'gy', 'gz')), may hold values from 0 to 65535
- panel_angles: float32 [2, 1048576], P(None, ('gx', 'gy', 'gz')), may hold values from -3.140625 to 3.140625
- owned_blocks: int32 [256], P(('gx', 'gy', 'gz')), may hold values from 1 to 32, 2048 in all
- listener_angles: float32 [2, 1024], replicated, may hold values from -3.140625 to 3.140625
- listener_range: float32 [1024], replicated, may hold values from 1.2 to 2.5
Outputs:
- state_next: float32 [5, 256, 128, 512], P(None, 'gx', 'gy', 'gz')
- observer_spectra: float32 [2, 1024, 128], P(None, 'gz')
The draws below stay inside these ranges and needn't reach their ends.
Inputs may be any that keep to these rules, and one draw needn't show every extreme that they name: `state_old`: density between 0.5 and 2, velocity components of magnitude 0.3 at most, stiffened-gas pressure between 0.3 and 2. `state_section`: density between 0.5 and 2, velocity components of magnitude 0.3 at most, stiffened-gas pressure between 0.3 and 2. A device's live blocks fill its first owned_blocks slots; some device owns 32 blocks, and they total 8 times the number of devices.
All inputs are finite; a program needn't handle non-finite values.
Results may differ from the reference program's by a relative error of at most 0.0003.
The reference program's roundings to bfloat16 on the way count: a program that leaves them out, or rounds other values in their place, can miss the bound.
Values may be sent and summed in bfloat16 or wider, within the bound.
A program may use at most 64 MiB of HBM per device.

```python
import math
import jax
import jax.numpy as jnp
import numpy as np
from jax import lax

CX = 16
CY = 32
CZ = 128
SAMPLES = 512
FREQS = 128
BLOCK_PANELS = 128
SLOTS = 32
LIVE_DEV = 8
NX = 256
NY = 128
NZ = 512
CELLS = 65536
BLOCKS = 8192
PANELS = 1048576
OBS = 1024
N_GX = 16
N_GY = 4
N_GZ = 4
DEVICES = 256


GAMMA_GAS = 4.4


PRESSURE_INF = 1.0


def state_field(base_key):
    subkeys = jax.random.split(base_key, 3)
    grid_shape = (NX, NY, NZ)
    density = jnp.exp(jax.random.uniform(subkeys[0], grid_shape, jnp.float32, math.log(0.5), math.log(2.0)))
    velocity = jax.random.uniform(subkeys[1], (3,) + grid_shape, jnp.float32, -0.3, 0.3)
    pressure = jax.random.uniform(subkeys[2], grid_shape, jnp.float32, 0.3, 2.0)
    momenta = density[None] * velocity
    energy = (pressure + GAMMA_GAS * PRESSURE_INF) / (GAMMA_GAS - 1.0) + 0.5 * density * jnp.sum(velocity * velocity, axis=0)
    return jnp.concatenate([density[None], momenta, energy[None]], axis=0)


def draw_state_old(key, part):
    return state_field(jax.random.fold_in(key, 11))


def draw_state_section(key, part):
    return state_field(jax.random.fold_in(key, 23))


def touch_ends(values, stream_key, least, largest):
    longest = values.shape.index(max(values.shape))
    spots = []
    for shift in (0, 1):
        where = [jax.random.randint(jax.random.fold_in(stream_key, axis), (), 0, length) for axis, length in enumerate(values.shape)]
        where[longest] = (where[longest] + shift) % values.shape[longest]
        spots.append(tuple(where))
    return values.at[spots[0]].set(least).at[spots[1]].set(largest)


def steps_of(rng, extent, cuts, low, high):
    level, own = 1.0, jax.random.fold_in(rng, 6)
    for position, shards_of in cuts:
        steps = jnp.exp(jax.random.uniform(jax.random.fold_in(own, position), (shards_of,), jnp.float32, low / len(cuts), high / len(cuts)))
        level = level * jnp.repeat(steps, extent[position] // shards_of).reshape([-1 if axis == position else 1 for axis in range(len(extent))])
    return level


def profile(count, total, bound, lean):
    portions = [(1 << 20) // math.isqrt(grade ** lean) + 1 for grade in range(2, count + 1)]
    spare, given = total - bound - (count - 1), [1] * (count - 1)
    while spare > 0:
        movable = [i for i in range(count - 1) if given[i] < bound]
        whole, left = sum([portions[i] for i in movable]), spare
        for i in movable:
            more = min(bound - given[i], max(1, left * portions[i] // whole), spare)
            given[i] = given[i] + more
            spare = spare - more
    return np.array([bound] + given)


def uneven(rng, number_of, total, reach, skew):
    if number_of == 2:
        one = jax.random.randint(rng, (), max(1, total - reach), min(reach, total - 1) + 1)
        return jnp.stack([one, total - one])
    sizes = jnp.asarray(profile(number_of, total, reach, skew), jnp.int32)
    pairs = (number_of - 1) // 2
    donor, sink = sizes[1:1 + 2 * pairs:2], sizes[2:2 + 2 * pairs:2]
    slack = jnp.minimum(donor - 1, reach - sink)
    moved = jax.random.randint(jax.random.fold_in(rng, 1), (pairs,), 0, 1 << 20) % (slack + 1)
    sizes = sizes.at[1:1 + 2 * pairs:2].set(donor - moved).at[2:2 + 2 * pairs:2].set(sink + moved)
    return sizes[jax.random.permutation(jax.random.fold_in(rng, 2), number_of)]


def noise(rng, dims, spread, bound, cuts=(), held_as=jnp.bfloat16):
    result = jax.random.normal(rng, dims, jnp.float32) * spread
    if len(cuts) > 0:
        result = steps_of(rng, dims, cuts, -0.22, 0.18) * result
    return jnp.clip(result, min=-bound, max=bound).astype(held_as)


def setup_inputs(seed: int = 0) -> dict:
    keys = jax.random.split(jax.random.key(seed), 9)
    return {
        "state_old": draw_state_old(jax.random.fold_in(keys[8], 71), 0),
        "state_section": draw_state_section(jax.random.fold_in(keys[8], 71), 0),
        "panel_record": noise(keys[2], (PANELS, SAMPLES), 1.0, 6.0, ((0, 256),)),
        "panel_cell": touch_ends(jax.random.randint(keys[3], (BLOCKS, BLOCK_PANELS), 0, CELLS), jax.random.fold_in(keys[3], 1), 0, CELLS - 1).astype(jnp.int32),
        "panel_angles": jnp.clip(jax.random.uniform(keys[4], (2, PANELS), jnp.float32, -3.140625, 3.140625), -3.140625, 3.140625),
        "owned_blocks": uneven(keys[5], DEVICES, LIVE_DEV * DEVICES, SLOTS, 2).astype(jnp.int32),
        "listener_angles": jnp.clip(jax.random.uniform(keys[6], (2, OBS), jnp.float32, -3.140625, 3.140625), -3.140625, 3.140625),
        "listener_range": jnp.clip(jnp.exp(jax.random.uniform(keys[7], (OBS,), jnp.float32, math.log(1.2), math.log(2.5))), 1.2, 2.5),
    }


GAMMA_GAS = 4.4
PRESSURE_INF = 1.0
WENO_EPS = 1e-06
WAVE_STEP = 0.25
COURANT = 0.08

def weno_face(far_left, near_left, middle, near_right, far_right):
    cand_a = (2.0 * far_left - 7.0 * near_left + 11.0 * middle) / 6.0
    cand_b = (-near_left + 5.0 * middle + 2.0 * near_right) / 6.0
    cand_c = (2.0 * middle + 5.0 * near_right - far_right) / 6.0
    rough_a = 13.0 / 12.0 * (far_left - 2.0 * near_left + middle) ** 2 + 0.25 * (far_left - 4.0 * near_left + 3.0 * middle) ** 2
    rough_b = 13.0 / 12.0 * (near_left - 2.0 * middle + near_right) ** 2 + 0.25 * (near_left - near_right) ** 2
    rough_c = 13.0 / 12.0 * (middle - 2.0 * near_right + far_right) ** 2 + 0.25 * (3.0 * middle - 4.0 * near_right + far_right) ** 2
    weight_a = 0.1 / (WENO_EPS + rough_a) ** 2
    weight_b = 0.6 / (WENO_EPS + rough_b) ** 2
    weight_c = 0.3 / (WENO_EPS + rough_c) ** 2
    return (weight_a * cand_a + weight_b * cand_b + weight_c * cand_c) / (weight_a + weight_b + weight_c)

def euler_flux(state_slab, axis_d):
    density = state_slab[0]
    momenta = state_slab[1:4]
    energy = state_slab[4]
    velocity = momenta / density[None]
    kinetic = 0.5 * lax.optimization_barrier(jnp.sum(momenta * velocity, axis=0))
    pressure = (GAMMA_GAS - 1.0) * (energy - kinetic) - GAMMA_GAS * PRESSURE_INF
    normal_speed = velocity[axis_d]
    sound_speed = jnp.sqrt(GAMMA_GAS * (pressure + PRESSURE_INF) / density)
    rows_out = [momenta[axis_d]]
    for component in range(3):
        carried = momenta[component] * normal_speed
        if component == axis_d:
            carried = carried + pressure
        rows_out.append(carried)
    rows_out.append((energy + pressure) * normal_speed)
    return (jnp.stack(rows_out), jnp.abs(normal_speed) + sound_speed)

def face_difference(padded, axis_d, count_d):
    array_axis = axis_d + 1
    picker = [slice(None), slice(3, -3), slice(3, -3), slice(3, -3)]
    picker[array_axis] = slice(None)
    state_slab = padded[tuple(picker)]
    fluxes, speeds = euler_flux(state_slab, axis_d)
    cell_count = state_slab.shape[array_axis] - 6

    def shifted(values, offset, along):
        return lax.slice_in_dim(values, offset, offset + cell_count + 1, axis=along)
    wave_speed = shifted(speeds, 0, axis_d)
    for offset in range(1, 6):
        wave_speed = jnp.maximum(wave_speed, shifted(speeds, offset, axis_d))
    split_up = [0.5 * (shifted(fluxes, offset, array_axis) + wave_speed[None] * shifted(state_slab, offset, array_axis)) for offset in range(6)]
    split_down = [0.5 * (shifted(fluxes, offset, array_axis) - wave_speed[None] * shifted(state_slab, offset, array_axis)) for offset in range(6)]
    face_flux = weno_face(split_up[0], split_up[1], split_up[2], split_up[3], split_up[4]) + weno_face(split_down[5], split_down[4], split_down[3], split_down[2], split_down[1])
    after = lax.slice_in_dim(face_flux, 1, cell_count + 1, axis=array_axis)
    before = lax.slice_in_dim(face_flux, 0, cell_count, axis=array_axis)
    return (after - before) * float(count_d)

def section_update(padded, old_block, counts, step_size):
    change = face_difference(padded, 0, counts[0]) + face_difference(padded, 1, counts[1]) + face_difference(padded, 2, counts[2])
    return 0.75 * old_block + 0.25 * (padded[:, 3:-3, 3:-3, 3:-3] - step_size * change)

def directions(angles):
    polar_angle = 0.5 * angles[0]
    azimuth = angles[1]
    return jnp.stack([jnp.cos(polar_angle) * jnp.cos(azimuth), jnp.cos(polar_angle) * jnp.sin(azimuth), jnp.sin(polar_angle)])

def panel_places(cell_rows, block_x, block_y, block_z, cells_x, cells_y, cells_z, counts):
    along_x = cell_rows // (cells_y * cells_z)
    along_y = cell_rows // cells_z % cells_y
    along_z = cell_rows % cells_z
    place_x = ((block_x * cells_x + along_x).astype(jnp.float32) + 0.5) / counts[0]
    place_y = ((block_y * cells_y + along_y).astype(jnp.float32) + 0.5) / counts[1]
    place_z = ((block_z * cells_z + along_z).astype(jnp.float32) + 0.5) / counts[2]
    return jnp.stack([place_x, place_y, place_z], axis=1)

def dft_table(sample_count, freq_count):
    times = jnp.arange(sample_count, dtype=jnp.int32)[:, None]
    orders = jnp.arange(1, freq_count + 1, dtype=jnp.int32)[None, :]
    phases = 2.0 * math.pi / sample_count * (times * orders % sample_count).astype(jnp.float32)
    scaling = 1.0 / math.sqrt(sample_count)
    return (jnp.concatenate([jnp.cos(phases), -jnp.sin(phases)], axis=1) * scaling).astype(jnp.bfloat16)

def observer_terms(sources, places, normals, live_flags, dft_rows, listeners, wave_numbers):
    spectra = jnp.einsum('gpt,tk->gpk', sources.astype(jnp.float32), dft_rows.astype(jnp.float32)).astype(jnp.bfloat16)
    offsets = listeners[None, :, :, None] - places[:, :, None, :]
    dist_sq = lax.optimization_barrier(jnp.sum(offsets * offsets, axis=1))
    facing = lax.optimization_barrier(jnp.sum(normals[:, :, None, :] * offsets, axis=1))
    weights = (facing / (4.0 * math.pi * dist_sq)).astype(jnp.bfloat16)
    product = jnp.einsum('gop,gpk->gok', weights.astype(jnp.float32), spectra.astype(jnp.float32))
    centres = lax.optimization_barrier(jnp.mean(places, axis=2))
    separation = listeners[None, :, :] - centres[:, :, None]
    centre_reach = jnp.sqrt(lax.optimization_barrier(jnp.sum(separation * separation, axis=1)))
    phase_now = centre_reach[:, :, None] * wave_numbers[None, None, :]
    cosine = jnp.cos(phase_now)
    sine_part = jnp.sin(phase_now)
    freq_count = wave_numbers.shape[0]
    real_part = product[:, :, :freq_count] * cosine + product[:, :, freq_count:] * sine_part
    imag_part = product[:, :, freq_count:] * cosine - product[:, :, :freq_count] * sine_part
    masks = live_flags[:, None, None]
    return jnp.stack([lax.optimization_barrier(jnp.sum(masks * real_part, axis=0)), lax.optimization_barrier(jnp.sum(masks * imag_part, axis=0))])

def reference(state_old, state_section, panel_record, panel_cell, panel_angles, owned_blocks, listener_angles, listener_range):
    counts = (NX, NY, NZ)
    step_size = COURANT / max(NX, NY, NZ)
    padded_all = jnp.pad(state_section, ((0, 0), (3, 3), (3, 3), (3, 3)), mode='wrap')
    dft_rows = dft_table(SAMPLES, FREQS)
    listeners = 0.5 + listener_range[None, :] * directions(listener_angles)
    wave_numbers = WAVE_STEP * jnp.arange(1, FREQS + 1, dtype=jnp.int32).astype(jnp.float32)
    records = panel_record.reshape(DEVICES, SLOTS, BLOCK_PANELS, SAMPLES)
    cell_all = panel_cell.reshape(DEVICES, SLOTS, BLOCK_PANELS)
    angle_all = panel_angles.reshape(2, DEVICES, SLOTS, BLOCK_PANELS)

    def per_device(running, device):
        block_x = device // (N_GY * N_GZ)
        block_y = device // N_GZ % N_GY
        block_z = device % N_GZ
        corner = (jnp.int32(0), (block_x * CX).astype(jnp.int32), (block_y * CY).astype(jnp.int32), (block_z * CZ).astype(jnp.int32))
        padded = lax.dynamic_slice(padded_all, corner, (5, CX + 6, CY + 6, CZ + 6))
        old_block = lax.dynamic_slice(state_old, corner, (5, CX, CY, CZ))
        updated = section_update(padded, old_block, counts, step_size)
        density = updated[0].reshape(CX * CY * CZ)
        cell_rows = cell_all[device]
        sampled = density[cell_rows]
        sources = (records[device].astype(jnp.float32) * sampled[:, :, None]).astype(jnp.bfloat16)
        places = panel_places(cell_rows, block_x, block_y, block_z, CX, CY, CZ, counts)
        normals = jnp.transpose(directions(angle_all[:, device]), (1, 0, 2))
        live_flags = (jnp.arange(SLOTS, dtype=jnp.int32) < owned_blocks[device]).astype(jnp.float32)
        running = running + observer_terms(sources, places, normals, live_flags, dft_rows, listeners, wave_numbers)
        return (running, updated)
    running, blocks_out = lax.scan(per_device, jnp.zeros((2, OBS, FREQS), jnp.float32), jnp.arange(DEVICES, dtype=jnp.int32))
    state_next = blocks_out.reshape(N_GX, N_GY, N_GZ, 5, CX, CY, CZ).transpose(3, 0, 4, 1, 5, 2, 6).reshape(5, NX, NY, NZ)
    return (state_next, running)
```

```python
import functools
import math

import jax
import jax.numpy as jnp
from jax import lax
from jax.experimental import pallas as pl
from jax.experimental.pallas import tpu as pltpu
from jax.sharding import PartitionSpec as P

FREQS = 128
GAMMA_GAS = 4.4
PRESSURE_INF = 1.0
WENO_EPS = 1e-06
WAVE_STEP = 0.25
COURANT = 0.08

SCALE = 4.0
EPS = 4.0 * SCALE * SCALE * WENO_EPS


def summed_on_arrival(blocks, axis):
    return jnp.sum(lax.all_to_all(blocks, axis, 0, 0, tiled=True), axis=0)


def collect(shard, axis):
    copies = jnp.broadcast_to(shard, (lax.axis_size(axis), *shard.shape))
    return lax.all_to_all(copies, axis, split_axis=0, concat_axis=0, tiled=True)


def sum_by_parts(shard, axes):
    size = lax.axis_size(axes)
    lines = shard.reshape(size, -1, shard.shape[-1])
    own = summed_on_arrival(lines, axes)
    return collect(own, axes).reshape(shard.shape)


def edge_swap(low_edge, high_edge, axis):
    size = lax.axis_size(axis)
    up = [(i, (i + 1) % size) for i in range(size)]
    down = [(b, a) for a, b in up]
    return lax.ppermute(high_edge, axis, up), lax.ppermute(low_edge, axis, down)


def flux_of(state, axis_d):
    density, energy = state[0], state[4]
    momenta = state[1:4]
    inverse = 1.0 / density
    velocity = [m * inverse for m in momenta]
    kinetic = 0.5 * (momenta[0] * velocity[0] + momenta[1] * velocity[1] + momenta[2] * velocity[2])
    pressure = (GAMMA_GAS - 1.0) * (energy - kinetic) - GAMMA_GAS * PRESSURE_INF * SCALE
    normal = velocity[axis_d]
    sound = jnp.sqrt(GAMMA_GAS * (pressure + PRESSURE_INF * SCALE) * inverse)
    rows = [momenta[axis_d]]
    for component in range(3):
        carried = momenta[component] * normal
        rows.append(carried + pressure if component == axis_d else carried)
    rows.append((energy + pressure) * normal)
    return rows, jnp.abs(normal) + sound


def weno_terms(e0, e1, e2, d1, d2):
    base1 = d1 * d1 + EPS
    base2 = d2 * d2 + EPS
    t0 = e0 * ((4.0 / 3.0) * e0 + d1) + base1
    t1 = e1 * ((4.0 / 3.0) * e1 + d1) + base1
    t2 = e2 * ((4.0 / 3.0) * e2 - d2) + base2
    p01, p02, p12 = t0 * t1, t0 * t2, t1 * t2
    wa = p12 * p12
    wb = 6.0 * (p02 * p02)
    wc = 1.5 * (p01 * p01)
    return wa * (e0 - e1) + wc * (e1 - e2), (wa + wb) + (wc + wc)


def face_value(alpha, df, dq, fsum):
    aq = [alpha * v for v in dq]
    up = [df[j] + aq[j] for j in range(4)]
    dn = [None] + [df[j] - aq[j] for j in range(1, 5)]
    num_p, den_p = weno_terms(up[1] - up[0], up[2] - up[1], up[3] - up[2], up[1], up[2])
    num_m, den_m = weno_terms(dn[4] - dn[3], dn[3] - dn[2], dn[2] - dn[1], -dn[3], -dn[2])
    ratio = (num_p * den_m + num_m * den_p) / (den_p * den_m)
    return fsum + ((0.5 * (up[1] - dn[3]) - aq[2]) + ratio) * (1.0 / 3.0)


def sweep(planes, dq, df, fs, m2, faces, axis_d, cells, chunks):
    for r in range(chunks):
        rows = pl.ds(8 * r, 8)

        def load(j):
            return [planes[c, j, rows, :] for c in range(5)]

        def step(j, carry):
            state, flux, speed = carry
            next_state = load(j + 1)
            next_flux, next_speed = flux_of(next_state, axis_d)
            for c in range(5):
                dq[c, j, rows, :] = next_state[c] - state[c]
                df[c, j, rows, :] = next_flux[c] - flux[c]
                fs[c, j, rows, :] = next_flux[c] + flux[c]
            m2[j, rows, :] = jnp.maximum(next_speed, speed)
            return next_state, next_flux, next_speed

        first = load(0)
        first_flux, first_speed = flux_of(first, axis_d)
        lax.fori_loop(0, cells + 5, step, (first, first_flux, first_speed))

    def face(i, carry):
        for r in range(chunks):
            rows = pl.ds(8 * r, 8)
            alpha = jnp.maximum(jnp.maximum(m2[i, rows, :], m2[i + 2, rows, :]), m2[i + 4, rows, :])
            for c in range(5):
                faces[c, i, rows, :] = face_value(
                    alpha,
                    [df[c, i + j, rows, :] for j in range(5)],
                    [dq[c, i + j, rows, :] for j in range(5)],
                    fs[c, i + 2, rows, :],
                )
        return carry

    lax.fori_loop(0, cells + 1, face, 0)


def z_kernel(coef, q, lo, hi, out, turned, planes, dq, df, fs, m2, faces, diff):
    for c in range(5):
        for blk in range(4):
            tile = jnp.transpose(q[c, pl.ds(128 * blk, 128), :]) * SCALE
            base = 160 * blk
            turned[c, pl.ds(base, 8), :] = lo[c, blk] * SCALE
            turned[c, pl.ds(base + 8, 72), :] = tile[:72]
            turned[c, pl.ds(base + 80, 72), :] = tile[56:]
            turned[c, pl.ds(base + 152, 8), :] = hi[c, blk] * SCALE

    def gather(j, carry):
        for c in range(5):
            planes[c, j] = turned[c, pl.ds(j + 5, 8, stride=80), :]
        return carry

    lax.fori_loop(0, 70, gather, 0)
    sweep(planes, dq, df, fs, m2, faces, 2, 64, 1)

    def difference(i, carry):
        for c in range(5):
            diff[c, pl.ds(pl.multiple_of(8 * i, 8), 8), :] = coef * (faces[c, i + 1] - faces[c, i])
        return carry

    lax.fori_loop(0, 64, difference, 0)
    for c in range(5):
        for blk in range(4):
            tile = jnp.concatenate(
                [diff[c, pl.ds(2 * blk + half, 64, stride=8), :] for half in range(2)], axis=0
            )
            out[c, pl.ds(128 * blk, 128), :] = jnp.transpose(tile)


def y_kernel(coef, q, lo, hi, add, out, planes, dq, df, fs, m2, faces, diff):
    for c in range(5):
        for h in range(2):
            rows = pl.ds(8 * h, 8)
            for k in range(3):
                planes[c, k, rows, :] = lo[c, pl.ds(24 * h + k, 8, stride=3), :] * SCALE
                planes[c, 35 + k, rows, :] = hi[c, pl.ds(24 * h + k, 8, stride=3), :] * SCALE

    def gather(j, carry):
        for c in range(5):
            for h in range(2):
                planes[c, j + 3, pl.ds(8 * h, 8), :] = (
                    q[c, pl.ds(j + 256 * h, 8, stride=32), :] * SCALE
                )
        return carry

    lax.fori_loop(0, 32, gather, 0)
    sweep(planes, dq, df, fs, m2, faces, 1, 32, 2)

    def difference(i, carry):
        for c in range(5):
            diff[c, pl.ds(pl.multiple_of(16 * i, 16), 16), :] = coef * (
                faces[c, i + 1] - faces[c, i]
            )
        return carry

    lax.fori_loop(0, 32, difference, 0)

    def back(x, carry):
        for c in range(5):
            for y8 in range(4):
                rows = pl.ds(pl.multiple_of(32 * x + 8 * y8, 8), 8)
                out[c, rows, :] = add[c, rows, :] + diff[c, pl.ds(128 * y8 + x, 8, stride=16), :]
        return carry

    lax.fori_loop(0, 16, back, 0)


def x_kernel(coef, q, lo, hi, add, old, out, planes, dq, df, fs, m2, faces):
    for c in range(5):
        for k in range(3):
            planes[c, k] = lo[c, k] * SCALE
            planes[c, 19 + k] = hi[c, k] * SCALE

    def gather(j, carry):
        for c in range(5):
            planes[c, j + 3] = q[c, j] * SCALE
        return carry

    lax.fori_loop(0, 16, gather, 0)
    sweep(planes, dq, df, fs, m2, faces, 0, 16, 4)

    def finish(i, carry):
        for c in range(5):
            change = add[c, i] + coef * (faces[c, i + 1] - faces[c, i])
            out[c, i] = 0.75 * old[c, i] + 0.25 * q[c, i] - change
        return carry

    lax.fori_loop(0, 16, finish, 0)


def sweep_scratch(cells, rows):
    f32 = jnp.float32
    return [
        pltpu.VMEM((5, cells + 6, rows, 128), f32),
        pltpu.VMEM((5, cells + 5, rows, 128), f32),
        pltpu.VMEM((5, cells + 5, rows, 128), f32),
        pltpu.VMEM((5, cells + 5, rows, 128), f32),
        pltpu.VMEM((cells + 5, rows, 128), f32),
        pltpu.VMEM((5, cells + 1, rows, 128), f32),
    ]


FLOW_PARAMS = dict(
    compiler_params=pltpu.CompilerParams(vmem_limit_bytes=56 * 2**20),
    cost_estimate=pl.CostEstimate(flops=30_000_000, bytes_accessed=4_000_000, transcendentals=0),
)


def flow_update(state_old, state_section, counts, step_size):
    f32 = jnp.float32
    rows = state_section.reshape(5, 512, 128)
    strips = jnp.concatenate([state_section[..., :8], state_section[..., 120:]], axis=-1)
    strips = jnp.transpose(strips.reshape(5, 4, 128, 16), (0, 1, 3, 2))
    z_lo, z_hi = edge_swap(strips[:, :, :8], strips[:, :, 8:], "gz")
    y_lo, y_hi = edge_swap(
        state_section[:, :, :3].reshape(5, 48, 128), state_section[:, :, 29:].reshape(5, 48, 128), "gy"
    )
    x_lo, x_hi = edge_swap(state_section[:, :3], state_section[:, 13:], "gx")
    coefs = [0.25 * step_size * n / (2.0 * SCALE) for n in counts]
    part = pl.pallas_call(
        functools.partial(z_kernel, coefs[2]),
        out_shape=jax.ShapeDtypeStruct((5, 512, 128), f32),
        scratch_shapes=[pltpu.VMEM((5, 640, 128), f32)]
        + sweep_scratch(64, 8)
        + [pltpu.VMEM((5, 512, 128), f32)],
        name="flow_z",
        **FLOW_PARAMS,
    )(rows, z_lo, z_hi)
    part = pl.pallas_call(
        functools.partial(y_kernel, coefs[1]),
        out_shape=jax.ShapeDtypeStruct((5, 512, 128), f32),
        scratch_shapes=sweep_scratch(32, 16) + [pltpu.VMEM((5, 512, 128), f32)],
        name="flow_y",
        **FLOW_PARAMS,
    )(rows, y_lo, y_hi, part)
    return pl.pallas_call(
        functools.partial(x_kernel, coefs[0]),
        out_shape=jax.ShapeDtypeStruct((5, 16, 32, 128), f32),
        scratch_shapes=sweep_scratch(16, 32),
        name="flow_x",
        **FLOW_PARAMS,
    )(state_section, x_lo, x_hi, part.reshape(5, 16, 32, 128), state_old)


def directions(angles):
    polar_angle = 0.5 * angles[0]
    azimuth = angles[1]
    return jnp.stack(
        [
            jnp.cos(polar_angle) * jnp.cos(azimuth),
            jnp.cos(polar_angle) * jnp.sin(azimuth),
            jnp.sin(polar_angle),
        ]
    )


def panel_places(cell_rows, blocks, cells, counts):
    along = (
        cell_rows // (cells[1] * cells[2]),
        cell_rows // cells[2] % cells[1],
        cell_rows % cells[2],
    )
    return [
        ((blocks[d] * cells[d] + along[d]).astype(jnp.float32) + 0.5) / counts[d] for d in range(3)
    ]


def dft_table(sample_count, freq_count):
    times = jnp.arange(sample_count, dtype=jnp.int32)[None, :]
    orders = jnp.arange(1, freq_count + 1, dtype=jnp.int32)[:, None]
    phases = 2.0 * math.pi / sample_count * (times * orders % sample_count).astype(jnp.float32)
    scaling = 1.0 / math.sqrt(sample_count)
    return (jnp.concatenate([jnp.cos(phases), -jnp.sin(phases)], axis=0) * scaling).astype(
        jnp.bfloat16
    )


def sin_cos(turns):
    rest = turns - jnp.round(turns)
    half = rest * rest
    s = (3.1996934769709044, -14.868610848632139, 42.01616577638672, -76.70155116950977,
         81.60502462208919, -41.341697068940945, 6.283185307179586)
    c = (6.529609897637814, -25.96831291454545, 60.167831622681774, -85.45016553628534,
         64.93911898307624, -19.73920453207708, 1.0)
    sine = jnp.full_like(half, s[0])
    for k in s[1:]:
        sine = sine * half + k
    cosine = jnp.full_like(half, c[0])
    for k in c[1:]:
        cosine = cosine * half + k
    return sine * rest, cosine


OBS_CHUNK = 256


def panel_kernel(live, density, record, cells, geo, turns, listeners, table, out, pieces):
    b = pl.program_id(0)

    @pl.when(b == 0)
    def _():
        out[...] = jnp.zeros_like(out)
        turned = jnp.concatenate(
            [jnp.transpose(density[pl.ds(128 * k, 128), :]) for k in range(4)], axis=1
        )
        high = turned.astype(jnp.bfloat16)
        rest = turned - high.astype(jnp.float32)
        middle = rest.astype(jnp.bfloat16)
        pieces[pl.ds(0, 128), :] = high
        pieces[pl.ds(128, 128), :] = middle
        pieces[pl.ds(256, 128), :] = (rest - middle.astype(jnp.float32)).astype(jnp.bfloat16)

    @pl.when(b < live[0])
    def _():
        cell = cells[0]
        grid_row = lax.broadcasted_iota(jnp.int32, (512, 128), 0)
        chosen = jnp.where(grid_row == cell // 128, 1.0, 0.0).astype(jnp.bfloat16)
        found = jnp.dot(pieces[...], chosen, preferred_element_type=jnp.float32)
        found = (found[:128] + found[128:256]) + found[256:]
        lane = lax.broadcasted_iota(jnp.int32, (128, 128), 0)
        sampled = jnp.sum(jnp.where(lane == cell % 128, found, 0.0), axis=0, keepdims=True)
        place = lax.broadcasted_iota(jnp.int32, (8, 128), 0)
        columns = jnp.transpose(jnp.where(place == 6, sampled, geo[0]))
        sources = (record[...].astype(jnp.float32) * columns[:, 6:7]).astype(jnp.bfloat16)
        spectra = lax.dot_general(
            table[...], sources, (((1,), (1,)), ((), ())), preferred_element_type=jnp.float32
        ).astype(jnp.bfloat16)
        order = (lax.broadcasted_iota(jnp.int32, (8, 128), 0) + 1).astype(jnp.float32)
        for o in range(1024 // OBS_CHUNK):
            span = pl.ds(OBS_CHUNK * o, OBS_CHUNK)
            offs = [listeners[pl.ds(d, 1), span] - columns[:, d : d + 1] for d in range(3)]
            reach = (offs[0] * offs[0] + offs[1] * offs[1]) + offs[2] * offs[2]
            facing = (offs[0] * columns[:, 3:4] + offs[1] * columns[:, 4:5]) + offs[2] * columns[:, 5:6]
            weights = (facing / reach).astype(jnp.bfloat16)
            product = jnp.dot(spectra, weights, preferred_element_type=jnp.float32)
            for h in range(OBS_CHUNK // 128):
                lanes = slice(128 * h, 128 * h + 128)
                base = turns[0, :, pl.ds(OBS_CHUNK * o + 128 * h, 128)]
                sine, cosine = sin_cos(base * order)
                step_s = jnp.broadcast_to(sine[7:8], (8, 128))
                step_c = jnp.broadcast_to(cosine[7:8], (8, 128))
                for a in range(FREQS // 8):
                    re = product[8 * a : 8 * a + 8, lanes]
                    im = product[FREQS + 8 * a : FREQS + 8 * a + 8, lanes]
                    out[o, 0, pl.ds(8 * a, 8), lanes] += re * cosine + im * sine
                    out[o, 1, pl.ds(8 * a, 8), lanes] += im * cosine - re * sine
                    if a + 1 < FREQS // 8:
                        sine, cosine = (
                            sine * step_c + cosine * step_s,
                            cosine * step_c - sine * step_s,
                        )


def panel_sums(live_count, density, record, cells, geo, turns, listeners, table):
    def at(b, live):
        return jnp.minimum(b, live[0] - 1)

    return pl.pallas_call(
        panel_kernel,
        out_shape=jax.ShapeDtypeStruct((1024 // OBS_CHUNK, 2, FREQS, OBS_CHUNK), jnp.float32),
        grid_spec=pltpu.PrefetchScalarGridSpec(
            num_scalar_prefetch=1,
            grid=(32,),
            in_specs=[
                pl.BlockSpec((512, 128), lambda b, live: (0, 0)),
                pl.BlockSpec((128, 512), lambda b, live: (at(b, live), 0)),
                pl.BlockSpec((1, 1, 128), lambda b, live: (at(b, live), 0, 0)),
                pl.BlockSpec((1, 8, 128), lambda b, live: (at(b, live), 0, 0)),
                pl.BlockSpec((1, 1, 1024), lambda b, live: (at(b, live), 0, 0)),
                pl.BlockSpec((8, 1024), lambda b, live: (0, 0)),
                pl.BlockSpec((256, 512), lambda b, live: (0, 0)),
            ],
            out_specs=pl.BlockSpec(
                (1024 // OBS_CHUNK, 2, FREQS, OBS_CHUNK), lambda b, live: (0, 0, 0, 0)
            ),
            scratch_shapes=[pltpu.VMEM((384, 512), jnp.bfloat16)],
        ),
        compiler_params=pltpu.CompilerParams(
            dimension_semantics=("arbitrary",), vmem_limit_bytes=48 * 2**20
        ),
        cost_estimate=pl.CostEstimate(
            flops=4_000_000_000, bytes_accessed=8_000_000, transcendentals=0
        ),
        name="panels",
    )(live_count, density, record, cells, geo, turns, listeners, table)


def panel_geometry(panel_cell, panel_angles, listener_angles, listener_range, blocks, cells, counts):
    slot_count, block_rows = panel_cell.shape
    places = panel_places(panel_cell, blocks, cells, counts)
    normals = directions(panel_angles.reshape(2, slot_count, block_rows)) * (0.25 / math.pi)
    blank = jnp.zeros_like(places[0])
    geo = jnp.stack([*places, normals[0], normals[1], normals[2], blank, blank], axis=1)
    listeners = 0.5 + listener_range[None, :] * directions(listener_angles)
    centres = [jnp.mean(p, axis=1, keepdims=True) for p in places]
    apart = sum((listeners[d][None, :] - centres[d]) ** 2 for d in range(3))
    turns = jnp.sqrt(apart) * (WAVE_STEP / (2.0 * math.pi))
    listeners = jnp.concatenate([listeners, jnp.zeros((5, listeners.shape[1]), jnp.float32)], axis=0)
    return geo, turns.reshape(slot_count, 1, -1), listeners


def local(
    state_old,
    state_section,
    panel_record,
    panel_cell,
    panel_angles,
    owned_blocks,
    listener_angles,
    listener_range,
):
    cells = state_section.shape[1:]
    axes = ("gx", "gy", "gz")
    counts = tuple(n * lax.axis_size(a) for n, a in zip(cells, axes))
    step_size = COURANT / max(counts)
    geo, turns, listeners = panel_geometry(
        panel_cell,
        panel_angles,
        listener_angles,
        listener_range,
        [lax.axis_index(a) for a in axes],
        cells,
        counts,
    )
    updated = flow_update(state_old, state_section, counts, step_size)
    partial = panel_sums(
        owned_blocks,
        updated[0].reshape(512, 128),
        panel_record,
        panel_cell.reshape(32, 1, 128),
        geo,
        turns,
        listeners,
        dft_table(panel_record.shape[1], FREQS),
    )
    gz_share = summed_on_arrival(partial, "gz")
    spectra_out = sum_by_parts(gz_share.reshape(2 * FREQS, OBS_CHUNK), ("gx", "gy"))
    return updated, jnp.transpose(spectra_out.reshape(2, FREQS, OBS_CHUNK), (0, 2, 1))


def solution(mesh):
    return jax.shard_map(
        local,
        mesh=mesh,
        in_specs=(
            P(None, "gx", "gy", "gz"),
            P(None, "gx", "gy", "gz"),
            P(("gx", "gy", "gz"), None),
            P(("gx", "gy", "gz"), None),
            P(None, ("gx", "gy", "gz")),
            P(("gx", "gy", "gz")),
            P(),
            P(),
        ),
        out_specs=(P(None, "gx", "gy", "gz"), P(None, "gz", None)),
        check_vma=False,
    )
```

```python
import functools
import math

import jax
import jax.numpy as jnp
from jax import lax
from jax.experimental import pallas as pl
from jax.experimental.pallas import tpu as pltpu
from jax.sharding import PartitionSpec as P

FREQS = 128
GAMMA_GAS = 4.4
PRESSURE_INF = 1.0
WENO_EPS = 1e-06
WAVE_STEP = 0.25
COURANT = 0.08

SCALE = 4.0
EPS = 0.75 * 4.0 * SCALE * SCALE * WENO_EPS


def summed_on_arrival(blocks, axis):
    return jnp.sum(lax.all_to_all(blocks, axis, 0, 0, tiled=True), axis=0)


def collect(shard, axis):
    copies = jnp.broadcast_to(shard, (lax.axis_size(axis), *shard.shape))
    return lax.all_to_all(copies, axis, split_axis=0, concat_axis=0, tiled=True)


def sum_by_parts(shard, axes):
    size = lax.axis_size(axes)
    lines = shard.reshape(size, -1, shard.shape[-1])
    own = summed_on_arrival(lines, axes)
    return collect(own, axes).reshape(shard.shape)


def edge_swap(low_edge, high_edge, axis):
    size = lax.axis_size(axis)
    up = [(i, (i + 1) % size) for i in range(size)]
    down = [(b, a) for a, b in up]
    return lax.ppermute(high_edge, axis, up), lax.ppermute(low_edge, axis, down)


def flux_of(state, axis_d):
    density, energy = state[0], state[4]
    momenta = state[1:4]
    inverse = 1.0 / density
    velocity = [m * inverse for m in momenta]
    kinetic = 0.5 * (momenta[0] * velocity[0] + momenta[1] * velocity[1] + momenta[2] * velocity[2])
    pressure = (GAMMA_GAS - 1.0) * (energy - kinetic) - GAMMA_GAS * PRESSURE_INF * SCALE
    normal = velocity[axis_d]
    square = GAMMA_GAS * (pressure + PRESSURE_INF * SCALE) * inverse
    sound = square * lax.rsqrt(square)
    rows = [momenta[axis_d]]
    for component in range(3):
        carried = momenta[component] * normal
        rows.append(carried + pressure if component == axis_d else carried)
    rows.append((energy + pressure) * normal)
    return rows, jnp.abs(normal) + sound


def weno_terms(e0, e1, e2, d1, d2):
    q1, q2 = 0.75 * d1, 0.75 * d2
    base1 = d1 * q1 + EPS
    base2 = d2 * q2 + EPS
    t0 = e0 * (e0 + q1) + base1
    t1 = e1 * (e1 + q1) + base1
    t2 = e2 * (e2 - q2) + base2
    p01, p02, p12 = t0 * t1, t0 * t2, t1 * t2
    wa = p12 * p12
    wb = 6.0 * (p02 * p02)
    wc = 1.5 * (p01 * p01)
    return wa * (e0 - e1) + wc * (e1 - e2), (wa + wb) + (wc + wc)


def face_value(alpha, df, dq, fsum):
    aq = [alpha * v for v in dq]
    up = [df[j] + aq[j] for j in range(4)]
    dn = [None] + [df[j] - aq[j] for j in range(1, 5)]
    num_p, den_p = weno_terms(up[1] - up[0], up[2] - up[1], up[3] - up[2], up[1], up[2])
    num_m, den_m = weno_terms(dn[4] - dn[3], dn[3] - dn[2], dn[2] - dn[1], -dn[3], -dn[2])
    ratio = (num_p * den_m + num_m * den_p) / (den_p * den_m)
    return fsum + ((0.5 * (up[1] - dn[3]) - aq[2]) + ratio) * (1.0 / 3.0)


def sweep(planes, dq, df, fs, m2, faces, axis_d, cells, chunks, streams):
    def load(r, j):
        return [planes[c, j, pl.ds(8 * r, 8), :] for c in range(5)]

    for group, length in streams:

        def step(k, carry):
            after = []
            for (r, start), (state, flux, speed) in zip(group, carry):
                j, rows = start + k, pl.ds(8 * r, 8)
                next_state = load(r, j + 1)
                next_flux, next_speed = flux_of(next_state, axis_d)
                for c in range(5):
                    dq[c, j, rows, :] = next_state[c] - state[c]
                    df[c, j, rows, :] = next_flux[c] - flux[c]
                    fs[c, j, rows, :] = next_flux[c] + flux[c]
                m2[j, rows, :] = jnp.maximum(next_speed, speed)
                after.append((next_state, next_flux, next_speed))
            return after

        begin = []
        for r, start in group:
            state = load(r, start)
            begin.append((state, *flux_of(state, axis_d)))
        lax.fori_loop(0, length, step, begin)

    def face(i, carry):
        for r in range(chunks):
            rows = pl.ds(8 * r, 8)
            alpha = jnp.maximum(jnp.maximum(m2[i, rows, :], m2[i + 2, rows, :]), m2[i + 4, rows, :])
            for c in range(5):
                faces[c, i, rows, :] = face_value(
                    alpha,
                    [df[c, i + j, rows, :] for j in range(5)],
                    [dq[c, i + j, rows, :] for j in range(5)],
                    fs[c, i + 2, rows, :],
                )
        return carry

    lax.fori_loop(0, cells + 1, face, 0)


def z_part(coef, q, lo, hi, out, turned, planes, dq, df, fs, m2, faces, diff):
    for c in range(5):
        for blk in range(4):
            tile = jnp.transpose(q[c, pl.ds(128 * blk, 128), :]) * SCALE
            base = 160 * blk
            turned[c, pl.ds(base, 8), :] = lo[c, blk] * SCALE
            turned[c, pl.ds(base + 8, 72), :] = tile[:72]
            turned[c, pl.ds(base + 80, 72), :] = tile[56:]
            turned[c, pl.ds(base + 152, 8), :] = hi[c, blk] * SCALE

    def gather(j, carry):
        for c in range(5):
            planes[c, j] = turned[c, pl.ds(j + 5, 8, stride=80), :]
        return carry

    lax.fori_loop(0, 70, gather, 0, unroll=2)
    sweep(planes, dq, df, fs, m2, faces, 2, 64, 1, [(((0, 0), (0, 23), (0, 46)), 23)])

    def difference(i, carry):
        for c in range(5):
            diff[c, pl.ds(pl.multiple_of(8 * i, 8), 8), :] = coef * (faces[c, i + 1] - faces[c, i])
        return carry

    lax.fori_loop(0, 64, difference, 0, unroll=2)
    for c in range(5):
        for blk in range(4):
            tile = jnp.concatenate(
                [diff[c, pl.ds(2 * blk + half, 64, stride=8), :] for half in range(2)], axis=0
            )
            out[c, pl.ds(128 * blk, 128), :] = jnp.transpose(tile)


def y_part(coef, q, lo, hi, out, planes, dq, df, fs, m2, faces, diff):
    for c in range(5):
        for h in range(2):
            rows = pl.ds(8 * h, 8)
            for k in range(3):
                planes[c, k, rows, :] = lo[c, pl.ds(24 * h + k, 8, stride=3), :] * SCALE
                planes[c, 35 + k, rows, :] = hi[c, pl.ds(24 * h + k, 8, stride=3), :] * SCALE

    def gather(j, carry):
        for c in range(5):
            for h in range(2):
                planes[c, j + 3, pl.ds(8 * h, 8), :] = (
                    q[c, pl.ds(j + 256 * h, 8, stride=32), :] * SCALE
                )
        return carry

    lax.fori_loop(0, 32, gather, 0)
    sweep(planes, dq, df, fs, m2, faces, 1, 32, 2, [(((0, 0), (1, 0)), 37)])

    def difference(i, carry):
        for c in range(5):
            diff[c, pl.ds(pl.multiple_of(16 * i, 16), 16), :] = coef * (
                faces[c, i + 1] - faces[c, i]
            )
        return carry

    lax.fori_loop(0, 32, difference, 0)

    def back(x, carry):
        for c in range(5):
            for y8 in range(4):
                rows = pl.ds(pl.multiple_of(32 * x + 8 * y8, 8), 8)
                out[c, rows, :] += diff[c, pl.ds(128 * y8 + x, 8, stride=16), :]
        return carry

    lax.fori_loop(0, 16, back, 0)


def x_part(coef, q, lo, hi, add, old, out, planes, dq, df, fs, m2, faces):
    for c in range(5):
        for k in range(3):
            planes[c, k] = lo[c, pl.ds(32 * k, 32), :] * SCALE
            planes[c, 19 + k] = hi[c, pl.ds(32 * k, 32), :] * SCALE

    def gather(j, carry):
        for c in range(5):
            planes[c, j + 3] = q[c, pl.ds(pl.multiple_of(32 * j, 32), 32), :] * SCALE
        return carry

    lax.fori_loop(0, 16, gather, 0)
    streams = [(((0, 0), (1, 0)), 21), (((2, 0), (3, 0)), 21)]
    sweep(planes, dq, df, fs, m2, faces, 0, 16, 4, streams)

    def finish(i, carry):
        rows = pl.ds(pl.multiple_of(32 * i, 32), 32)
        for c in range(5):
            change = add[c, rows, :] + coef * (faces[c, i + 1] - faces[c, i])
            out[c, rows, :] = (0.75 * old[c, rows, :] + 0.25 * q[c, rows, :]) - change
        return carry

    lax.fori_loop(0, 16, finish, 0)


def flow_kernel(coefs, q, old, z_lo, z_hi, y_lo, y_hi, x_lo, x_hi, out, turned, diff, add, *spaces):
    z_part(coefs[2], q, z_lo, z_hi, add, turned, *spaces[0:6], diff)
    y_part(coefs[1], q, y_lo, y_hi, add, *spaces[6:12], diff)
    x_part(coefs[0], q, x_lo, x_hi, add, old, out, *spaces[12:18])


def sweep_scratch(cells, rows):
    f32 = jnp.float32
    return [
        pltpu.VMEM((5, cells + 6, rows, 128), f32),
        pltpu.VMEM((5, cells + 5, rows, 128), f32),
        pltpu.VMEM((5, cells + 5, rows, 128), f32),
        pltpu.VMEM((5, cells + 5, rows, 128), f32),
        pltpu.VMEM((cells + 5, rows, 128), f32),
        pltpu.VMEM((5, cells + 1, rows, 128), f32),
    ]


def flow_update(state_old, state_section, counts, step_size):
    f32 = jnp.float32
    rows = state_section.reshape(5, 512, 128)
    x_lo, x_hi = edge_swap(rows[:, :96], rows[:, 416:], "gx")
    y_lo, y_hi = edge_swap(
        state_section[:, :, :3].reshape(5, 48, 128), state_section[:, :, 29:].reshape(5, 48, 128), "gy"
    )
    strips = jnp.concatenate([state_section[..., :8], state_section[..., 120:]], axis=-1)
    strips = jnp.transpose(strips.reshape(5, 4, 128, 16), (0, 1, 3, 2))
    z_lo, z_hi = edge_swap(strips[:, :, :8], strips[:, :, 8:], "gz")
    coefs = [0.25 * step_size * n / (2.0 * SCALE) for n in counts]
    return pl.pallas_call(
        functools.partial(flow_kernel, coefs),
        out_shape=jax.ShapeDtypeStruct((5, 512, 128), f32),
        scratch_shapes=[pltpu.VMEM((5, 640, 128), f32)]
        + [pltpu.VMEM((5, 512, 128), f32)] * 2
        + sweep_scratch(64, 8)
        + sweep_scratch(32, 16)
        + sweep_scratch(16, 32),
        compiler_params=pltpu.CompilerParams(vmem_limit_bytes=56 * 2**20),
        cost_estimate=pl.CostEstimate(flops=100_000_000, bytes_accessed=6_000_000, transcendentals=0),
        name="flow",
    )(rows, state_old.reshape(5, 512, 128), z_lo, z_hi, y_lo, y_hi, x_lo, x_hi)


def directions(angles):
    polar_angle = 0.5 * angles[0]
    azimuth = angles[1]
    return jnp.stack(
        [
            jnp.cos(polar_angle) * jnp.cos(azimuth),
            jnp.cos(polar_angle) * jnp.sin(azimuth),
            jnp.sin(polar_angle),
        ]
    )


def panel_places(cell_rows, blocks, cells, counts):
    along = (
        cell_rows // (cells[1] * cells[2]),
        cell_rows // cells[2] % cells[1],
        cell_rows % cells[2],
    )
    return [
        ((blocks[d] * cells[d] + along[d]).astype(jnp.float32) + 0.5) / counts[d] for d in range(3)
    ]


def dft_table(sample_count, freq_count):
    times = jnp.arange(sample_count, dtype=jnp.int32)[None, :]
    orders = jnp.arange(1, freq_count + 1, dtype=jnp.int32)[:, None]
    phases = 2.0 * math.pi / sample_count * (times * orders % sample_count).astype(jnp.float32)
    scaling = 1.0 / math.sqrt(sample_count)
    return (jnp.concatenate([jnp.cos(phases), -jnp.sin(phases)], axis=0) * scaling).astype(
        jnp.bfloat16
    )


def sin_cos(turns):
    rest = turns - jnp.round(turns)
    half = rest * rest
    s = (3.1996934769709044, -14.868610848632139, 42.01616577638672, -76.70155116950977,
         81.60502462208919, -41.341697068940945, 6.283185307179586)
    c = (6.529609897637814, -25.96831291454545, 60.167831622681774, -85.45016553628534,
         64.93911898307624, -19.73920453207708, 1.0)
    sine = jnp.full_like(half, s[0])
    for k in s[1:]:
        sine = sine * half + k
    cosine = jnp.full_like(half, c[0])
    for k in c[1:]:
        cosine = cosine * half + k
    return sine * rest, cosine


OBS_CHUNK = 256


def in_pieces(values):
    pieces = []
    for _ in range(3):
        piece = values.astype(jnp.bfloat16).astype(jnp.float32)
        pieces.append(piece)
        values = values - piece
    return pieces


PAIRS = ((0, 0), (0, 1), (1, 0), (0, 2), (1, 1), (2, 0))


def panel_kernel(
    live, density, record, cells, geo, turns, listeners, table, out, pieces, heard, spectra
):
    b = pl.program_id(0)

    def front():
        cell = cells[0]
        grid_row = lax.broadcasted_iota(jnp.int32, (512, 128), 0)
        chosen = jnp.where(grid_row == cell // 128, 1.0, 0.0).astype(jnp.bfloat16)
        found = jnp.dot(pieces[...], chosen, preferred_element_type=jnp.float32)
        found = (found[:128] + found[128:256]) + found[256:]
        lane = lax.broadcasted_iota(jnp.int32, (128, 128), 0)
        sampled = jnp.sum(jnp.where(lane == cell % 128, found, 0.0), axis=0, keepdims=True)
        column = jnp.transpose(jnp.broadcast_to(sampled, (8, 128)))[:, 0:1]
        sources = (record[...].astype(jnp.float32) * column).astype(jnp.bfloat16)
        spectra[lax.rem(b, 2)] = lax.dot_general(
            table[...], sources, (((1,), (1,)), ((), ())), preferred_element_type=jnp.float32
        ).astype(jnp.bfloat16)

    def back():
        spectrum = spectra[lax.rem(b + 1, 2)]
        facing_pieces, apart_pieces = in_pieces(geo[0, 0:8]), in_pieces(geo[0, 8:16])
        seen = jnp.concatenate(
            [
                jnp.concatenate([facing_pieces[s], apart_pieces[s]], axis=1)
                for s, _ in PAIRS
            ],
            axis=0,
        ).astype(jnp.bfloat16)
        order = (lax.broadcasted_iota(jnp.int32, (8, 128), 0) + 1).astype(jnp.float32)
        for o in range(1024 // OBS_CHUNK):
            both = lax.dot_general(
                seen,
                heard[:, OBS_CHUNK * o : OBS_CHUNK * (o + 1)],
                (((0,), (0,)), ((), ())),
                preferred_element_type=jnp.float32,
            )
            weights = (both[:128] / both[128:]).astype(jnp.bfloat16)
            product = jnp.dot(spectrum, weights, preferred_element_type=jnp.float32)
            for h in range(OBS_CHUNK // 128):
                lanes = slice(128 * h, 128 * h + 128)
                base = turns[0, :, pl.ds(OBS_CHUNK * o + 128 * h, 128)]
                sine, cosine = sin_cos(base * order)
                step_s = jnp.broadcast_to(sine[7:8], (8, 128))
                step_c = jnp.broadcast_to(cosine[7:8], (8, 128))
                before_s = sine * step_c - cosine * step_s
                before_c = cosine * step_c + sine * step_s
                twice = step_c + step_c
                for a in range(FREQS // 8):
                    re = product[8 * a : 8 * a + 8, lanes]
                    im = product[FREQS + 8 * a : FREQS + 8 * a + 8, lanes]
                    out[o, 0, pl.ds(8 * a, 8), lanes] += re * cosine + im * sine
                    out[o, 1, pl.ds(8 * a, 8), lanes] += im * cosine - re * sine
                    if a + 1 < FREQS // 8:
                        sine, before_s = twice * sine - before_s, sine
                        cosine, before_c = twice * cosine - before_c, cosine

    @pl.when(b == 0)
    def _():
        out[...] = jnp.zeros_like(out)
        turned = jnp.concatenate(
            [jnp.transpose(density[pl.ds(128 * k, 128), :]) for k in range(4)], axis=1
        )
        for k, piece in enumerate(in_pieces(turned)):
            pieces[pl.ds(128 * k, 128), :] = piece.astype(jnp.bfloat16)
        split = in_pieces(listeners[...])
        heard[...] = jnp.concatenate([split[t] for _, t in PAIRS], axis=0).astype(jnp.bfloat16)
        front()

    @pl.when((b > 0) & (b <= live[0]))
    def _():
        front()
        back()


def panel_sums(live_count, density, record, cells, geo, turns, listeners, table):
    def now(b, live):
        return jnp.minimum(b, live[0] - 1)

    def last(b, live):
        return jnp.maximum(jnp.minimum(b, live[0]) - 1, 0)

    return pl.pallas_call(
        panel_kernel,
        out_shape=jax.ShapeDtypeStruct((1024 // OBS_CHUNK, 2, FREQS, OBS_CHUNK), jnp.float32),
        grid_spec=pltpu.PrefetchScalarGridSpec(
            num_scalar_prefetch=1,
            grid=(33,),
            in_specs=[
                pl.BlockSpec((512, 128), lambda b, live: (0, 0)),
                pl.BlockSpec((128, 512), lambda b, live: (now(b, live), 0)),
                pl.BlockSpec((1, 1, 128), lambda b, live: (now(b, live), 0, 0)),
                pl.BlockSpec((1, 16, 128), lambda b, live: (last(b, live), 0, 0)),
                pl.BlockSpec((1, 1, 1024), lambda b, live: (last(b, live), 0, 0)),
                pl.BlockSpec((8, 1024), lambda b, live: (0, 0)),
                pl.BlockSpec((256, 512), lambda b, live: (0, 0)),
            ],
            out_specs=pl.BlockSpec(
                (1024 // OBS_CHUNK, 2, FREQS, OBS_CHUNK), lambda b, live: (0, 0, 0, 0)
            ),
            scratch_shapes=[
                pltpu.VMEM((384, 512), jnp.bfloat16),
                pltpu.VMEM((8 * len(PAIRS), 1024), jnp.bfloat16),
                pltpu.VMEM((2, 256, 128), jnp.bfloat16),
            ],
        ),
        compiler_params=pltpu.CompilerParams(
            dimension_semantics=("arbitrary",), vmem_limit_bytes=48 * 2**20
        ),
        cost_estimate=pl.CostEstimate(
            flops=4_000_000_000, bytes_accessed=8_000_000, transcendentals=0
        ),
        name="panels",
    )(live_count, density, record, cells, geo, turns, listeners, table)


def panel_geometry(panel_cell, panel_angles, listener_angles, listener_range, blocks, cells, counts):
    slot_count, block_rows = panel_cell.shape
    places = [p - 0.5 for p in panel_places(panel_cell, blocks, cells, counts)]
    normals = directions(panel_angles.reshape(2, slot_count, block_rows)) * (0.25 / math.pi)
    across = -sum(normals[d] * places[d] for d in range(3))
    square = sum(p * p for p in places)
    blank = jnp.zeros_like(square)
    geo = jnp.stack(
        [normals[0], normals[1], normals[2], across, blank, blank, blank, blank]
        + [-2.0 * p for p in places]
        + [square, blank + 1.0, blank, blank, blank],
        axis=1,
    )
    heard = listener_range[None, :] * directions(listener_angles)
    centres = [jnp.mean(p, axis=1, keepdims=True) for p in places]
    apart = sum((heard[d][None, :] - centres[d]) ** 2 for d in range(3))
    turns = jnp.sqrt(apart) * (WAVE_STEP / (2.0 * math.pi))
    listeners = jnp.concatenate(
        [heard, jnp.ones_like(heard[:1]), jnp.sum(heard * heard, axis=0, keepdims=True), jnp.zeros_like(heard)],
        axis=0,
    )
    return geo, turns.reshape(slot_count, 1, -1), listeners


def local(
    state_old,
    state_section,
    panel_record,
    panel_cell,
    panel_angles,
    owned_blocks,
    listener_angles,
    listener_range,
):
    cells = state_section.shape[1:]
    axes = ("gx", "gy", "gz")
    counts = tuple(n * lax.axis_size(a) for n, a in zip(cells, axes))
    step_size = COURANT / max(counts)
    geo, turns, listeners = panel_geometry(
        panel_cell,
        panel_angles,
        listener_angles,
        listener_range,
        [lax.axis_index(a) for a in axes],
        cells,
        counts,
    )
    updated = flow_update(state_old, state_section, counts, step_size)
    partial = panel_sums(
        owned_blocks,
        updated[0],
        panel_record,
        panel_cell.reshape(32, 1, 128),
        geo,
        turns,
        listeners,
        dft_table(panel_record.shape[1], FREQS),
    )
    gz_share = summed_on_arrival(partial, "gz")
    spectra_out = sum_by_parts(gz_share.reshape(2 * FREQS, OBS_CHUNK), ("gx", "gy"))
    return updated.reshape(state_section.shape), jnp.transpose(spectra_out.reshape(2, FREQS, OBS_CHUNK), (0, 2, 1))


def solution(mesh):
    return jax.shard_map(
        local,
        mesh=mesh,
        in_specs=(
            P(None, "gx", "gy", "gz"),
            P(None, "gx", "gy", "gz"),
            P(("gx", "gy", "gz"), None),
            P(("gx", "gy", "gz"), None),
            P(None, ("gx", "gy", "gz")),
            P(("gx", "gy", "gz")),
            P(),
            P(),
        ),
        out_specs=(P(None, "gx", "gy", "gz"), P(None, "gz", None)),
        check_vma=False,
    )
```

```python
import functools
import math

import jax
import jax.numpy as jnp
from jax import lax
from jax.experimental import pallas as pl
from jax.experimental.pallas import tpu as pltpu
from jax.sharding import PartitionSpec as P

FREQS = 128
GAMMA_GAS = 4.4
PRESSURE_INF = 1.0
WENO_EPS = 1e-06
WAVE_STEP = 0.25
COURANT = 0.08

SCALE = 4.0
EPS = 0.75 * 4.0 * SCALE * SCALE * WENO_EPS


def summed_on_arrival(blocks, axis):
    return jnp.sum(lax.all_to_all(blocks, axis, 0, 0, tiled=True), axis=0)


def collect(shard, axis):
    copies = jnp.broadcast_to(shard, (lax.axis_size(axis), *shard.shape))
    return lax.all_to_all(copies, axis, split_axis=0, concat_axis=0, tiled=True)


def sum_by_parts(shard, axes):
    size = lax.axis_size(axes)
    lines = shard.reshape(size, -1, shard.shape[-1])
    own = summed_on_arrival(lines, axes)
    return collect(own, axes).reshape(shard.shape)


def edge_swap(low_edge, high_edge, axis):
    size = lax.axis_size(axis)
    up = [(i, (i + 1) % size) for i in range(size)]
    down = [(b, a) for a, b in up]
    return lax.ppermute(high_edge, axis, up), lax.ppermute(low_edge, axis, down)


def flux_of(state, axis_d):
    density, energy = state[0], state[4]
    momenta = state[1:4]
    inverse = 1.0 / density
    velocity = [m * inverse for m in momenta]
    kinetic = 0.5 * (momenta[0] * velocity[0] + momenta[1] * velocity[1] + momenta[2] * velocity[2])
    pressure = (GAMMA_GAS - 1.0) * (energy - kinetic) - GAMMA_GAS * PRESSURE_INF * SCALE
    normal = velocity[axis_d]
    square = GAMMA_GAS * (pressure + PRESSURE_INF * SCALE) * inverse
    sound = square * lax.rsqrt(square)
    rows = [momenta[axis_d]]
    for component in range(3):
        carried = momenta[component] * normal
        rows.append(carried + pressure if component == axis_d else carried)
    rows.append((energy + pressure) * normal)
    return rows, jnp.abs(normal) + sound


def weno_terms(e0, e1, e2, d1, d2):
    q1, q2 = 0.75 * d1, 0.75 * d2
    base1 = d1 * q1 + EPS
    base2 = d2 * q2 + EPS
    t0 = e0 * (e0 + q1) + base1
    t1 = e1 * (e1 + q1) + base1
    t2 = e2 * (e2 - q2) + base2
    p01, p02, p12 = t0 * t1, t0 * t2, t1 * t2
    wa = p12 * p12
    wb = 6.0 * (p02 * p02)
    wc = 1.5 * (p01 * p01)
    return wa * (e0 - e1) + wc * (e1 - e2), (wa + wb) + (wc + wc)


def face_value(alpha, df, dq, fsum):
    aq = [alpha * v for v in dq]
    up = [df[j] + aq[j] for j in range(4)]
    dn = [None] + [df[j] - aq[j] for j in range(1, 5)]
    num_p, den_p = weno_terms(up[1] - up[0], up[2] - up[1], up[3] - up[2], up[1], up[2])
    num_m, den_m = weno_terms(dn[4] - dn[3], dn[3] - dn[2], dn[2] - dn[1], -dn[3], -dn[2])
    ratio = (num_p * den_m + num_m * den_p) / (den_p * den_m)
    return fsum + ((0.5 * (up[1] - dn[3]) - aq[2]) + ratio) * (1.0 / 3.0)


def sweep(planes, dq, df, fs, m2, faces, axis_d, cells, chunks, streams):
    def load(r, j):
        return [planes[c, j, pl.ds(8 * r, 8), :] for c in range(5)]

    for group, length in streams:

        def step(k, carry):
            for u in range(3):
                after = []
                for (r, start), (state, flux, speed) in zip(group, carry):
                    j, rows = start + 3 * k + u, pl.ds(8 * r, 8)
                    next_state = load(r, j + 1)
                    next_flux, next_speed = flux_of(next_state, axis_d)
                    for c in range(5):
                        dq[c, j, rows, :] = next_state[c] - state[c]
                        df[c, j, rows, :] = next_flux[c] - flux[c]
                        fs[c, j, rows, :] = next_flux[c] + flux[c]
                    m2[j, rows, :] = jnp.maximum(next_speed, speed)
                    after.append((next_state, next_flux, next_speed))
                carry = after
            return carry

        begin = []
        for r, start in group:
            state = load(r, start)
            begin.append((state, *flux_of(state, axis_d)))
        lax.fori_loop(0, length, step, begin)

    def face(i, carry):
        for r in range(chunks):
            rows = pl.ds(8 * r, 8)
            alpha = jnp.maximum(jnp.maximum(m2[i, rows, :], m2[i + 2, rows, :]), m2[i + 4, rows, :])
            for c in range(5):
                faces[c, i, rows, :] = face_value(
                    alpha,
                    [df[c, i + j, rows, :] for j in range(5)],
                    [dq[c, i + j, rows, :] for j in range(5)],
                    fs[c, i + 2, rows, :],
                )
        return carry

    lax.fori_loop(0, cells + 1, face, 0)


def z_part(coef, q, lo, hi, out, turned, planes, dq, df, fs, m2, faces, diff):
    for c in range(5):
        for blk in range(4):
            tile = jnp.transpose(q[c, pl.ds(128 * blk, 128), :]) * SCALE
            base = 160 * blk
            turned[c, pl.ds(base, 8), :] = lo[c, blk] * SCALE
            turned[c, pl.ds(base + 8, 72), :] = tile[:72]
            turned[c, pl.ds(base + 80, 72), :] = tile[56:]
            turned[c, pl.ds(base + 152, 8), :] = hi[c, blk] * SCALE

    def gather(j, carry):
        for c in range(5):
            planes[c, j] = turned[c, pl.ds(j + 5, 8, stride=80), :]
        return carry

    lax.fori_loop(0, 70, gather, 0, unroll=2)
    sweep(planes, dq, df, fs, m2, faces, 2, 64, 1, [(((0, 0), (0, 33)), 12)])

    def difference(i, carry):
        for c in range(5):
            diff[c, pl.ds(pl.multiple_of(8 * i, 8), 8), :] = coef * (faces[c, i + 1] - faces[c, i])
        return carry

    lax.fori_loop(0, 64, difference, 0, unroll=2)
    for c in range(5):
        for blk in range(4):
            tile = jnp.concatenate(
                [diff[c, pl.ds(2 * blk + half, 64, stride=8), :] for half in range(2)], axis=0
            )
            out[c, pl.ds(128 * blk, 128), :] = jnp.transpose(tile)


def y_part(coef, q, lo, hi, out, planes, dq, df, fs, m2, faces, diff):
    for c in range(5):
        for h in range(2):
            rows = pl.ds(8 * h, 8)
            for k in range(3):
                planes[c, k, rows, :] = lo[c, pl.ds(24 * h + k, 8, stride=3), :] * SCALE
                planes[c, 35 + k, rows, :] = hi[c, pl.ds(24 * h + k, 8, stride=3), :] * SCALE

    def gather(j, carry):
        for c in range(5):
            for h in range(2):
                planes[c, j + 3, pl.ds(8 * h, 8), :] = (
                    q[c, pl.ds(j + 256 * h, 8, stride=32), :] * SCALE
                )
        return carry

    lax.fori_loop(0, 32, gather, 0)
    sweep(planes, dq, df, fs, m2, faces, 1, 32, 2, [(((0, 0), (1, 0)), 13)])

    def difference(i, carry):
        for c in range(5):
            diff[c, pl.ds(pl.multiple_of(16 * i, 16), 16), :] = coef * (
                faces[c, i + 1] - faces[c, i]
            )
        return carry

    lax.fori_loop(0, 32, difference, 0)

    def back(x, carry):
        for c in range(5):
            for y8 in range(4):
                rows = pl.ds(pl.multiple_of(32 * x + 8 * y8, 8), 8)
                out[c, rows, :] += diff[c, pl.ds(128 * y8 + x, 8, stride=16), :]
        return carry

    lax.fori_loop(0, 16, back, 0)


def x_part(coef, q, lo, hi, add, old, out, planes, dq, df, fs, m2, faces):
    for c in range(5):
        for k in range(3):
            planes[c, k] = lo[c, pl.ds(32 * k, 32), :] * SCALE
            planes[c, 19 + k] = hi[c, pl.ds(32 * k, 32), :] * SCALE

    def gather(j, carry):
        for c in range(5):
            planes[c, j + 3] = q[c, pl.ds(pl.multiple_of(32 * j, 32), 32), :] * SCALE
        return carry

    lax.fori_loop(0, 16, gather, 0)
    streams = [(((0, 0), (1, 0)), 7), (((2, 0), (3, 0)), 7)]
    sweep(planes, dq, df, fs, m2, faces, 0, 16, 4, streams)

    def finish(i, carry):
        rows = pl.ds(pl.multiple_of(32 * i, 32), 32)
        for c in range(5):
            change = add[c, rows, :] + coef * (faces[c, i + 1] - faces[c, i])
            out[c, rows, :] = (0.75 * old[c, rows, :] + 0.25 * q[c, rows, :]) - change
        return carry

    lax.fori_loop(0, 16, finish, 0)


def flow_kernel(coefs, q, old, z_lo, z_hi, y_lo, y_hi, x_lo, x_hi, out, turned, diff, add, *spaces):
    z_part(coefs[2], q, z_lo, z_hi, add, turned, *spaces[0:6], diff)
    y_part(coefs[1], q, y_lo, y_hi, add, *spaces[6:12], diff)
    x_part(coefs[0], q, x_lo, x_hi, add, old, out, *spaces[12:18])


def sweep_scratch(cells, rows):
    f32 = jnp.float32
    steps = -(-(cells + 5) // 3) * 3
    return [
        pltpu.VMEM((5, steps + 1, rows, 128), f32),
        pltpu.VMEM((5, steps, rows, 128), f32),
        pltpu.VMEM((5, steps, rows, 128), f32),
        pltpu.VMEM((5, steps, rows, 128), f32),
        pltpu.VMEM((steps, rows, 128), f32),
        pltpu.VMEM((5, cells + 1, rows, 128), f32),
    ]


def flow_update(state_old, state_section, counts, step_size):
    f32 = jnp.float32
    rows = state_section.reshape(5, 512, 128)
    x_lo, x_hi = edge_swap(rows[:, :96], rows[:, 416:], "gx")
    y_lo, y_hi = edge_swap(
        state_section[:, :, :3].reshape(5, 48, 128), state_section[:, :, 29:].reshape(5, 48, 128), "gy"
    )
    strips = jnp.concatenate([state_section[..., :8], state_section[..., 120:]], axis=-1)
    strips = jnp.transpose(strips.reshape(5, 4, 128, 16), (0, 1, 3, 2))
    z_lo, z_hi = edge_swap(strips[:, :, :8], strips[:, :, 8:], "gz")
    coefs = [0.25 * step_size * n / (2.0 * SCALE) for n in counts]
    return pl.pallas_call(
        functools.partial(flow_kernel, coefs),
        out_shape=jax.ShapeDtypeStruct((5, 512, 128), f32),
        scratch_shapes=[pltpu.VMEM((5, 640, 128), f32)]
        + [pltpu.VMEM((5, 512, 128), f32)] * 2
        + sweep_scratch(64, 8)
        + sweep_scratch(32, 16)
        + sweep_scratch(16, 32),
        compiler_params=pltpu.CompilerParams(vmem_limit_bytes=56 * 2**20),
        cost_estimate=pl.CostEstimate(flops=100_000_000, bytes_accessed=6_000_000, transcendentals=0),
        name="flow",
    )(rows, state_old.reshape(5, 512, 128), z_lo, z_hi, y_lo, y_hi, x_lo, x_hi)


def directions(angles):
    polar_angle = 0.5 * angles[0]
    azimuth = angles[1]
    return jnp.stack(
        [
            jnp.cos(polar_angle) * jnp.cos(azimuth),
            jnp.cos(polar_angle) * jnp.sin(azimuth),
            jnp.sin(polar_angle),
        ]
    )


def panel_places(cell_rows, blocks, cells, counts):
    along = (
        cell_rows // (cells[1] * cells[2]),
        cell_rows // cells[2] % cells[1],
        cell_rows % cells[2],
    )
    return [
        ((blocks[d] * cells[d] + along[d]).astype(jnp.float32) + 0.5) / counts[d] for d in range(3)
    ]


def dft_table(sample_count, freq_count):
    times = jnp.arange(sample_count, dtype=jnp.int32)[None, :]
    orders = jnp.arange(1, freq_count + 1, dtype=jnp.int32)[:, None]
    phases = 2.0 * math.pi / sample_count * (times * orders % sample_count).astype(jnp.float32)
    scaling = 1.0 / math.sqrt(sample_count)
    return (jnp.concatenate([jnp.cos(phases), -jnp.sin(phases)], axis=0) * scaling).astype(
        jnp.bfloat16
    )


def sin_cos(turns):
    rest = turns - jnp.round(turns)
    half = rest * rest
    s = (3.1996934769709044, -14.868610848632139, 42.01616577638672, -76.70155116950977,
         81.60502462208919, -41.341697068940945, 6.283185307179586)
    c = (6.529609897637814, -25.96831291454545, 60.167831622681774, -85.45016553628534,
         64.93911898307624, -19.73920453207708, 1.0)
    sine = jnp.full_like(half, s[0])
    for k in s[1:]:
        sine = sine * half + k
    cosine = jnp.full_like(half, c[0])
    for k in c[1:]:
        cosine = cosine * half + k
    return sine * rest, cosine


OBS_CHUNK = 256


def in_pieces(values):
    pieces = []
    for _ in range(3):
        piece = values.astype(jnp.bfloat16).astype(jnp.float32)
        pieces.append(piece)
        values = values - piece
    return pieces


PAIRS = ((0, 0), (0, 1), (1, 0), (0, 2), (1, 1), (2, 0))


GROUP = 4
GROUPS = 8
PAIR = 2


def panel_kernel(
    live, updated, record, cells, geo, turns, listeners, table, out, density, records, pieces, heard, spectra, sems
):
    groups = (live[0] + GROUP - 1) // GROUP

    def fetch(g):
        return pltpu.make_async_copy(
            record.at[pl.ds(128 * GROUP * g, 128 * GROUP)], records.at[g], sems.at[g]
        )

    first = pltpu.make_async_copy(updated.at[0], density, sems.at[GROUPS])
    first.start()
    for g in range(GROUPS):
        pl.when(g < groups)(fetch(g).start)

    out[...] = jnp.zeros_like(out)
    split = in_pieces(listeners[...])
    heard[...] = jnp.concatenate([split[t] for _, t in PAIRS], axis=0).astype(jnp.bfloat16)
    first.wait()
    turned = jnp.concatenate(
        [jnp.transpose(density[pl.ds(128 * k, 128), :]) for k in range(4)], axis=1
    )
    for k, piece in enumerate(in_pieces(turned)):
        pieces[pl.ds(128 * k, 128), :] = piece.astype(jnp.bfloat16)

    def front(g, carry):
        cell = cells[g]
        grid_row = lax.broadcasted_iota(jnp.int32, (512, 128 * GROUP), 0)
        chosen = jnp.where(grid_row == cell // 128, 1.0, 0.0).astype(jnp.bfloat16)
        found = jnp.dot(pieces[...], chosen, preferred_element_type=jnp.float32)
        found = (found[:128] + found[128:256]) + found[256:]
        lane = lax.broadcasted_iota(jnp.int32, (128, 128 * GROUP), 0)
        sampled = jnp.sum(jnp.where(lane == cell % 128, found, 0.0), axis=0, keepdims=True)
        column = jnp.transpose(jnp.broadcast_to(sampled, (8, 128 * GROUP)))[:, 0:1]
        fetch(g).wait()
        sources = (records[g].astype(jnp.float32) * column).astype(jnp.bfloat16)
        made = lax.dot_general(
            table[...], sources, (((1,), (1,)), ((), ())), preferred_element_type=jnp.float32
        ).astype(jnp.bfloat16)
        for k in range(GROUP):
            spectra[GROUP * g + k] = made[:, 128 * k : 128 * (k + 1)]
        return carry

    lax.fori_loop(0, groups, front, 0)

    order = (lax.broadcasted_iota(jnp.int32, (8, 128), 0) + 1).astype(jnp.float32)

    def features(b, alive):
        facing, apart = in_pieces(geo[b, 0:8] * alive), in_pieces(geo[b, 8:16])
        return jnp.concatenate(
            [jnp.concatenate([facing[s], apart[s]], axis=1) for s, _ in PAIRS], axis=0
        ).astype(jnp.bfloat16)

    def weights_of(seen, o):
        both = lax.dot_general(
            seen,
            heard[:, OBS_CHUNK * o : OBS_CHUNK * (o + 1)],
            (((0,), (0,)), ((), ())),
            preferred_element_type=jnp.float32,
        )
        return (both[:128] / both[128:]).astype(jnp.bfloat16)

    def add_turned(b, o, product):
        for h in range(OBS_CHUNK // 128):
            lanes = slice(128 * h, 128 * h + 128)
            base = turns[b, :, pl.ds(OBS_CHUNK * o + 128 * h, 128)]
            sine, cosine = sin_cos(base * order)
            step_s = jnp.broadcast_to(sine[7:8], (8, 128))
            step_c = jnp.broadcast_to(cosine[7:8], (8, 128))
            before_s = sine * step_c - cosine * step_s
            before_c = cosine * step_c + sine * step_s
            twice = step_c + step_c
            for a in range(FREQS // 8):
                re = product[8 * a : 8 * a + 8, lanes]
                im = product[FREQS + 8 * a : FREQS + 8 * a + 8, lanes]
                out[o, 0, pl.ds(8 * a, 8), lanes] += re * cosine + im * sine
                out[o, 1, pl.ds(8 * a, 8), lanes] += im * cosine - re * sine
                if a + 1 < FREQS // 8:
                    sine, before_s = twice * sine - before_s, sine
                    cosine, before_c = twice * cosine - before_c, cosine

    def back(pair, carry):
        blocks = []
        for k in range(PAIR):
            b = PAIR * pair + k
            alive = jnp.where(b < live[0], 1.0, 0.0)
            blocks.append((b, features(b, alive), spectra[b]))
        for o in range(1024 // OBS_CHUNK):
            for b, seen, spectrum in blocks:
                product = jnp.dot(
                    spectrum, weights_of(seen, o), preferred_element_type=jnp.float32
                )
                add_turned(b, o, product)
        return carry

    lax.fori_loop(0, (live[0] + PAIR - 1) // PAIR, back, 0)


def panel_sums(live_count, updated, record, cells, geo, turns, listeners, table):
    vmem = pl.BlockSpec(memory_space=pltpu.VMEM)
    bf16 = jnp.bfloat16
    return pl.pallas_call(
        panel_kernel,
        out_shape=jax.ShapeDtypeStruct((1024 // OBS_CHUNK, 2, FREQS, OBS_CHUNK), jnp.float32),
        in_specs=[
            pl.BlockSpec(memory_space=pltpu.SMEM),
            pl.BlockSpec(memory_space=pl.ANY),
            pl.BlockSpec(memory_space=pl.ANY),
        ]
        + [vmem] * 5,
        out_specs=vmem,
        scratch_shapes=[
            pltpu.VMEM((512, 128), jnp.float32),
            pltpu.VMEM((GROUPS, 128 * GROUP, 512), bf16),
            pltpu.VMEM((384, 512), bf16),
            pltpu.VMEM((8 * len(PAIRS), 1024), bf16),
            pltpu.VMEM((32, 256, 128), bf16),
            pltpu.SemaphoreType.DMA((GROUPS + 1,)),
        ],
        compiler_params=pltpu.CompilerParams(vmem_limit_bytes=48 * 2**20),
        cost_estimate=pl.CostEstimate(
            flops=4_000_000_000, bytes_accessed=8_000_000, transcendentals=0
        ),
        name="panels",
    )(live_count, updated, record, cells, geo, turns, listeners, table)


def panel_geometry(panel_cell, panel_angles, listener_angles, listener_range, blocks, cells, counts):
    slot_count, block_rows = panel_cell.shape
    places = [p - 0.5 for p in panel_places(panel_cell, blocks, cells, counts)]
    normals = directions(panel_angles.reshape(2, slot_count, block_rows)) * (0.25 / math.pi)
    across = -sum(normals[d] * places[d] for d in range(3))
    square = sum(p * p for p in places)
    blank = jnp.zeros_like(square)
    geo = jnp.stack(
        [normals[0], normals[1], normals[2], across, blank, blank, blank, blank]
        + [-2.0 * p for p in places]
        + [square, blank + 1.0, blank, blank, blank],
        axis=1,
    )
    heard = listener_range[None, :] * directions(listener_angles)
    centres = [jnp.mean(p, axis=1, keepdims=True) for p in places]
    apart = sum((heard[d][None, :] - centres[d]) ** 2 for d in range(3))
    turns = jnp.sqrt(apart) * (WAVE_STEP / (2.0 * math.pi))
    listeners = jnp.concatenate(
        [heard, jnp.ones_like(heard[:1]), jnp.sum(heard * heard, axis=0, keepdims=True), jnp.zeros_like(heard)],
        axis=0,
    )
    return geo, turns.reshape(slot_count, 1, -1), listeners


def local(
    state_old,
    state_section,
    panel_record,
    panel_cell,
    panel_angles,
    owned_blocks,
    listener_angles,
    listener_range,
):
    cells = state_section.shape[1:]
    axes = ("gx", "gy", "gz")
    counts = tuple(n * lax.axis_size(a) for n, a in zip(cells, axes))
    step_size = COURANT / max(counts)
    geo, turns, listeners = panel_geometry(
        panel_cell,
        panel_angles,
        listener_angles,
        listener_range,
        [lax.axis_index(a) for a in axes],
        cells,
        counts,
    )
    updated = flow_update(state_old, state_section, counts, step_size)
    partial = panel_sums(
        owned_blocks,
        updated,
        panel_record,
        panel_cell.reshape(GROUPS, 1, 128 * GROUP),
        geo,
        turns,
        listeners,
        dft_table(panel_record.shape[1], FREQS),
    )
    gz_share = summed_on_arrival(partial, "gz")
    spectra_out = sum_by_parts(gz_share.reshape(2 * FREQS, OBS_CHUNK), ("gx", "gy"))
    return updated.reshape(state_section.shape), jnp.transpose(spectra_out.reshape(2, FREQS, OBS_CHUNK), (0, 2, 1))


def solution(mesh):
    return jax.shard_map(
        local,
        mesh=mesh,
        in_specs=(
            P(None, "gx", "gy", "gz"),
            P(None, "gx", "gy", "gz"),
            P(("gx", "gy", "gz"), None),
            P(("gx", "gy", "gz"), None),
            P(None, ("gx", "gy", "gz")),
            P(("gx", "gy", "gz")),
            P(),
            P(),
        ),
        out_specs=(P(None, "gx", "gy", "gz"), P(None, "gz", None)),
        check_vma=False,
    )
```

```python
import functools
import math

import jax
import jax.numpy as jnp
from jax import lax
from jax.experimental import pallas as pl
from jax.experimental.pallas import tpu as pltpu
from jax.sharding import PartitionSpec as P

FREQS = 128
GAMMA_GAS = 4.4
PRESSURE_INF = 1.0
WENO_EPS = 1e-06
WAVE_STEP = 0.25
COURANT = 0.08

SCALE = 4.0
EPS = 0.75 * 4.0 * SCALE * SCALE * WENO_EPS


MESH = pl.DeviceIdType.MESH
TILES = 32


def sum_kernel(part, out, came0, sums, came1, total, came2, mine, full, other, s0, r0, s1, r1, s2, r2, s3, r3, s4, r4):
    gx, gy, gz = (lax.axis_index(a) for a in ("gx", "gy", "gz"))
    core, upper = lax.rem(gy, 2), gy // 2
    m = gx * 2 + upper
    partner = {"gx": gx, "gy": upper * 2 + (1 - core), "gz": gz}

    def along(k):
        return {"gx": gx, "gy": gy, "gz": lax.rem(gz + k, 4)}

    def chip(r):
        t = lax.rem(m + r, TILES)
        return t, {"gx": t // 2, "gy": lax.rem(t, 2) * 2 + core, "gz": gz}

    barrier = pltpu.get_barrier_semaphore()

    def greet(device):
        pl.semaphore_signal(barrier, inc=1, device_id=device, device_id_type=MESH)

    greet(partner)
    for k in (1, 2, 3):
        greet(along(k))

    def greet_chip(r, carry):
        greet(chip(r)[1])
        return carry

    lax.fori_loop(1, TILES, greet_chip, 0)
    pl.semaphore_wait(barrier, TILES + 3)

    def remote(src, dst, send, recv, device):
        return pltpu.make_async_remote_copy(
            src_ref=src, dst_ref=dst, send_sem=send, recv_sem=recv, device_id=device, device_id_type=MESH
        )

    shares, along_gz = {}, {}
    for k in (2, 1, 3, 0):
        shares[k] = remote(
            part.at[lax.rem(gz + k, 4), 1 - core], came0.at[k], s0.at[k], r0.at[k], partner
        )
        shares[k].start()
    for k in (2, 1, 3, 0):
        shares[k].wait_recv()
        sums[k] = part[lax.rem(gz + k, 4), core] + came0[k]
        if k > 0:
            along_gz[k] = remote(sums.at[k], came1.at[k - 1], s1.at[k - 1], r1.at[k - 1], along(k))
            along_gz[k].start()
    for k in (1, 3, 2):
        along_gz[k].wait_recv()
    total[...] = (sums[0] + came1[0]) + (came1[1] + came1[2])

    def scatter(r, carry):
        t, device = chip(r)
        remote(total.at[t], came2.at[r - 1], s2, r2, device).start()
        return carry

    lax.fori_loop(1, TILES, scatter, 0)
    pltpu.make_async_copy(came2, came2, r2).wait()
    own = total[m]
    for r in range(TILES - 1):
        own = own + came2[r]
    mine[...] = own
    full[m] = own

    def gather(r, carry):
        remote(mine, full.at[m], s3, r3, chip(r)[1]).start()
        return carry

    lax.fori_loop(1, TILES, gather, 0)
    pltpu.make_async_copy(came2, came2, r3).wait()
    swap = remote(full, other, s4, r4, partner)
    swap.start()

    def lay(which, tiles):
        for h in range(2):
            block = jnp.concatenate([tiles[2 * a + h] for a in range(16)], axis=0)
            out[which, pl.ds(128 * h, 128), :] = jnp.transpose(block)

    lay(core, full)
    swap.wait_recv()
    lay(1 - core, other)
    for k in (0, 1, 2, 3):
        shares[k].wait_send()
        if k > 0:
            along_gz[k].wait_send()
    pltpu.make_async_copy(came2, came2, s2).wait()
    pltpu.make_async_copy(came2, came2, s3).wait()
    swap.wait_send()


def summed_spectra(part):
    vmem = pl.BlockSpec(memory_space=pltpu.VMEM)
    f32 = jnp.float32
    tiles = (TILES, 8, 128)
    dma = pltpu.SemaphoreType.DMA
    return pl.pallas_call(
        sum_kernel,
        out_shape=jax.ShapeDtypeStruct((2, 256, FREQS), f32),
        in_specs=[vmem],
        out_specs=vmem,
        scratch_shapes=[
            pltpu.VMEM((4, *tiles), f32),
            pltpu.VMEM((4, *tiles), f32),
            pltpu.VMEM((3, *tiles), f32),
            pltpu.VMEM(tiles, f32),
            pltpu.VMEM((TILES - 1, 8, 128), f32),
            pltpu.VMEM((8, 128), f32),
            pltpu.VMEM(tiles, f32),
            pltpu.VMEM(tiles, f32),
            dma((4,)),
            dma((4,)),
            dma((3,)),
            dma((3,)),
            dma,
            dma,
            dma,
            dma,
            dma,
            dma,
        ],
        compiler_params=pltpu.CompilerParams(collective_id=1, has_side_effects=True),
        name="sum_spectra",
    )(part)


def edge_swap(low_edge, high_edge, axis):
    size = lax.axis_size(axis)
    up = [(i, (i + 1) % size) for i in range(size)]
    down = [(b, a) for a, b in up]
    return lax.ppermute(high_edge, axis, up), lax.ppermute(low_edge, axis, down)


def flux_of(state, axis_d):
    density, energy = state[0], state[4]
    momenta = state[1:4]
    inverse = 1.0 / density
    velocity = [m * inverse for m in momenta]
    kinetic = 0.5 * (momenta[0] * velocity[0] + momenta[1] * velocity[1] + momenta[2] * velocity[2])
    pressure = (GAMMA_GAS - 1.0) * (energy - kinetic) - GAMMA_GAS * PRESSURE_INF * SCALE
    normal = velocity[axis_d]
    square = GAMMA_GAS * (pressure + PRESSURE_INF * SCALE) * inverse
    sound = square * lax.rsqrt(square)
    rows = [momenta[axis_d]]
    for component in range(3):
        carried = momenta[component] * normal
        rows.append(carried + pressure if component == axis_d else carried)
    rows.append((energy + pressure) * normal)
    return rows, jnp.abs(normal) + sound


def weno_terms(e0, e1, e2, d1, d2):
    q1, q2 = 0.75 * d1, 0.75 * d2
    base1 = d1 * q1 + EPS
    base2 = d2 * q2 + EPS
    t0 = e0 * (e0 + q1) + base1
    t1 = e1 * (e1 + q1) + base1
    t2 = e2 * (e2 - q2) + base2
    p01, p02, p12 = t0 * t1, t0 * t2, t1 * t2
    wa = p12 * p12
    wb = 6.0 * (p02 * p02)
    wc = 1.5 * (p01 * p01)
    return wa * (e0 - e1) + wc * (e1 - e2), (wa + wb) + (wc + wc)


def face_value(alpha, df, dq, fsum):
    aq = [alpha * v for v in dq]
    up = [df[j] + aq[j] for j in range(4)]
    dn = [None] + [df[j] - aq[j] for j in range(1, 5)]
    num_p, den_p = weno_terms(up[1] - up[0], up[2] - up[1], up[3] - up[2], up[1], up[2])
    num_m, den_m = weno_terms(dn[4] - dn[3], dn[3] - dn[2], dn[2] - dn[1], -dn[3], -dn[2])
    ratio = (num_p * den_m + num_m * den_p) / (den_p * den_m)
    return fsum + ((0.5 * (up[1] - dn[3]) - aq[2]) + ratio) * (1.0 / 3.0)


def sweep(planes, dq, df, fs, m2, faces, axis_d, cells, chunks, streams):
    def load(r, j):
        return [planes[c, j, pl.ds(8 * r, 8), :] for c in range(5)]

    for group, length in streams:

        def step(k, carry):
            for u in range(3):
                after = []
                for (r, start), (state, flux, speed) in zip(group, carry):
                    j, rows = start + 3 * k + u, pl.ds(8 * r, 8)
                    next_state = load(r, j + 1)
                    next_flux, next_speed = flux_of(next_state, axis_d)
                    for c in range(5):
                        dq[c, j, rows, :] = next_state[c] - state[c]
                        df[c, j, rows, :] = next_flux[c] - flux[c]
                        fs[c, j, rows, :] = next_flux[c] + flux[c]
                    m2[j, rows, :] = jnp.maximum(next_speed, speed)
                    after.append((next_state, next_flux, next_speed))
                carry = after
            return carry

        begin = []
        for r, start in group:
            state = load(r, start)
            begin.append((state, *flux_of(state, axis_d)))
        lax.fori_loop(0, length, step, begin)

    def face(i, carry):
        for r in range(chunks):
            rows = pl.ds(8 * r, 8)
            alpha = jnp.maximum(jnp.maximum(m2[i, rows, :], m2[i + 2, rows, :]), m2[i + 4, rows, :])
            for c in range(5):
                faces[c, i, rows, :] = face_value(
                    alpha,
                    [df[c, i + j, rows, :] for j in range(5)],
                    [dq[c, i + j, rows, :] for j in range(5)],
                    fs[c, i + 2, rows, :],
                )
        return carry

    lax.fori_loop(0, cells + 1, face, 0)


def z_part(coef, q, lo, hi, out, turned, planes, dq, df, fs, m2, faces, diff):
    for c in range(5):
        for blk in range(4):
            tile = jnp.transpose(q[c, pl.ds(128 * blk, 128), :]) * SCALE
            base = 160 * blk
            turned[c, pl.ds(base, 8), :] = lo[c, blk] * SCALE
            turned[c, pl.ds(base + 8, 72), :] = tile[:72]
            turned[c, pl.ds(base + 80, 72), :] = tile[56:]
            turned[c, pl.ds(base + 152, 8), :] = hi[c, blk] * SCALE

    def gather(j, carry):
        for c in range(5):
            planes[c, j] = turned[c, pl.ds(j + 5, 8, stride=80), :]
        return carry

    lax.fori_loop(0, 70, gather, 0, unroll=2)
    sweep(planes, dq, df, fs, m2, faces, 2, 64, 1, [(((0, 0), (0, 33)), 12)])

    def difference(i, carry):
        for c in range(5):
            diff[c, pl.ds(pl.multiple_of(8 * i, 8), 8), :] = coef * (faces[c, i + 1] - faces[c, i])
        return carry

    lax.fori_loop(0, 64, difference, 0, unroll=2)
    for c in range(5):
        for blk in range(4):
            tile = jnp.concatenate(
                [diff[c, pl.ds(2 * blk + half, 64, stride=8), :] for half in range(2)], axis=0
            )
            out[c, pl.ds(128 * blk, 128), :] = jnp.transpose(tile)


def y_part(coef, q, lo, hi, out, planes, dq, df, fs, m2, faces, diff):
    for c in range(5):
        for h in range(2):
            rows = pl.ds(8 * h, 8)
            for k in range(3):
                planes[c, k, rows, :] = lo[c, pl.ds(24 * h + k, 8, stride=3), :] * SCALE
                planes[c, 35 + k, rows, :] = hi[c, pl.ds(24 * h + k, 8, stride=3), :] * SCALE

    def gather(j, carry):
        for c in range(5):
            for h in range(2):
                planes[c, j + 3, pl.ds(8 * h, 8), :] = (
                    q[c, pl.ds(j + 256 * h, 8, stride=32), :] * SCALE
                )
        return carry

    lax.fori_loop(0, 32, gather, 0)
    sweep(planes, dq, df, fs, m2, faces, 1, 32, 2, [(((0, 0), (1, 0)), 13)])

    def difference(i, carry):
        for c in range(5):
            diff[c, pl.ds(pl.multiple_of(16 * i, 16), 16), :] = coef * (
                faces[c, i + 1] - faces[c, i]
            )
        return carry

    lax.fori_loop(0, 32, difference, 0)

    def back(x, carry):
        for c in range(5):
            for y8 in range(4):
                rows = pl.ds(pl.multiple_of(32 * x + 8 * y8, 8), 8)
                out[c, rows, :] += diff[c, pl.ds(128 * y8 + x, 8, stride=16), :]
        return carry

    lax.fori_loop(0, 16, back, 0)


def x_part(coef, q, lo, hi, add, old, out, planes, dq, df, fs, m2, faces):
    for c in range(5):
        for k in range(3):
            planes[c, k] = lo[c, pl.ds(32 * k, 32), :] * SCALE
            planes[c, 19 + k] = hi[c, pl.ds(32 * k, 32), :] * SCALE

    def gather(j, carry):
        for c in range(5):
            planes[c, j + 3] = q[c, pl.ds(pl.multiple_of(32 * j, 32), 32), :] * SCALE
        return carry

    lax.fori_loop(0, 16, gather, 0)
    streams = [(((0, 0), (1, 0)), 7), (((2, 0), (3, 0)), 7)]
    sweep(planes, dq, df, fs, m2, faces, 0, 16, 4, streams)

    def finish(i, carry):
        rows = pl.ds(pl.multiple_of(32 * i, 32), 32)
        for c in range(5):
            change = add[c, rows, :] + coef * (faces[c, i + 1] - faces[c, i])
            out[c, rows, :] = (0.75 * old[c, rows, :] + 0.25 * q[c, rows, :]) - change
        return carry

    lax.fori_loop(0, 16, finish, 0)


def flow_kernel(coefs, q, old, z_lo, z_hi, y_lo, y_hi, x_lo, x_hi, out, turned, diff, add, *spaces):
    z_part(coefs[2], q, z_lo, z_hi, add, turned, *spaces[0:6], diff)
    y_part(coefs[1], q, y_lo, y_hi, add, *spaces[6:12], diff)
    x_part(coefs[0], q, x_lo, x_hi, add, old, out, *spaces[12:18])


def sweep_scratch(cells, rows):
    f32 = jnp.float32
    steps = -(-(cells + 5) // 3) * 3
    return [
        pltpu.VMEM((5, steps + 1, rows, 128), f32),
        pltpu.VMEM((5, steps, rows, 128), f32),
        pltpu.VMEM((5, steps, rows, 128), f32),
        pltpu.VMEM((5, steps, rows, 128), f32),
        pltpu.VMEM((steps, rows, 128), f32),
        pltpu.VMEM((5, cells + 1, rows, 128), f32),
    ]


def flow_update(state_old, state_section, counts, step_size):
    f32 = jnp.float32
    rows = state_section.reshape(5, 512, 128)
    x_lo, x_hi = edge_swap(rows[:, :96], rows[:, 416:], "gx")
    y_lo, y_hi = edge_swap(
        state_section[:, :, :3].reshape(5, 48, 128), state_section[:, :, 29:].reshape(5, 48, 128), "gy"
    )
    strips = jnp.concatenate([state_section[..., :8], state_section[..., 120:]], axis=-1)
    strips = jnp.transpose(strips.reshape(5, 4, 128, 16), (0, 1, 3, 2))
    z_lo, z_hi = edge_swap(strips[:, :, :8], strips[:, :, 8:], "gz")
    coefs = [0.25 * step_size * n / (2.0 * SCALE) for n in counts]
    return pl.pallas_call(
        functools.partial(flow_kernel, coefs),
        out_shape=jax.ShapeDtypeStruct((5, 512, 128), f32),
        scratch_shapes=[pltpu.VMEM((5, 640, 128), f32)]
        + [pltpu.VMEM((5, 512, 128), f32)] * 2
        + sweep_scratch(64, 8)
        + sweep_scratch(32, 16)
        + sweep_scratch(16, 32),
        compiler_params=pltpu.CompilerParams(vmem_limit_bytes=56 * 2**20),
        cost_estimate=pl.CostEstimate(flops=100_000_000, bytes_accessed=6_000_000, transcendentals=0),
        name="flow",
    )(rows, state_old.reshape(5, 512, 128), z_lo, z_hi, y_lo, y_hi, x_lo, x_hi)


def directions(angles):
    polar_angle = 0.5 * angles[0]
    azimuth = angles[1]
    return jnp.stack(
        [
            jnp.cos(polar_angle) * jnp.cos(azimuth),
            jnp.cos(polar_angle) * jnp.sin(azimuth),
            jnp.sin(polar_angle),
        ]
    )


def panel_places(cell_rows, blocks, cells, counts):
    along = (
        cell_rows // (cells[1] * cells[2]),
        cell_rows // cells[2] % cells[1],
        cell_rows % cells[2],
    )
    return [
        ((blocks[d] * cells[d] + along[d]).astype(jnp.float32) + 0.5) / counts[d] for d in range(3)
    ]


def dft_table(sample_count, freq_count):
    times = jnp.arange(sample_count, dtype=jnp.int32)[None, :]
    orders = jnp.arange(1, freq_count + 1, dtype=jnp.int32)[:, None]
    phases = 2.0 * math.pi / sample_count * (times * orders % sample_count).astype(jnp.float32)
    scaling = 1.0 / math.sqrt(sample_count)
    return (jnp.concatenate([jnp.cos(phases), -jnp.sin(phases)], axis=0) * scaling).astype(
        jnp.bfloat16
    )


def sin_cos(turns):
    rest = turns - jnp.round(turns)
    half = rest * rest
    s = (3.1996934769709044, -14.868610848632139, 42.01616577638672, -76.70155116950977,
         81.60502462208919, -41.341697068940945, 6.283185307179586)
    c = (6.529609897637814, -25.96831291454545, 60.167831622681774, -85.45016553628534,
         64.93911898307624, -19.73920453207708, 1.0)
    sine = jnp.full_like(half, s[0])
    for k in s[1:]:
        sine = sine * half + k
    cosine = jnp.full_like(half, c[0])
    for k in c[1:]:
        cosine = cosine * half + k
    return sine * rest, cosine


OBS_CHUNK = 256


def in_pieces(values):
    pieces = []
    for _ in range(3):
        piece = values.astype(jnp.bfloat16).astype(jnp.float32)
        pieces.append(piece)
        values = values - piece
    return pieces


PAIRS = ((0, 0), (0, 1), (1, 0), (0, 2), (1, 1), (2, 0))


GROUP = 4
GROUPS = 8
PAIR = 2


def panel_kernel(
    live, updated, record, cells, geo, turns, listeners, table, out, density, records, pieces, heard, spectra, sems
):
    groups = (live[0] + GROUP - 1) // GROUP

    def fetch(g):
        return pltpu.make_async_copy(
            record.at[pl.ds(128 * GROUP * g, 128 * GROUP)], records.at[g], sems.at[g]
        )

    first = pltpu.make_async_copy(updated.at[0], density, sems.at[GROUPS])
    first.start()
    for g in range(GROUPS):
        pl.when(g < groups)(fetch(g).start)

    out[...] = jnp.zeros_like(out)
    split = in_pieces(listeners[...])
    heard[...] = jnp.concatenate([split[t] for _, t in PAIRS], axis=0).astype(jnp.bfloat16)
    first.wait()
    turned = jnp.concatenate(
        [jnp.transpose(density[pl.ds(128 * k, 128), :]) for k in range(4)], axis=1
    )
    for k, piece in enumerate(in_pieces(turned)):
        pieces[pl.ds(128 * k, 128), :] = piece.astype(jnp.bfloat16)

    def front(g, carry):
        cell = cells[g]
        grid_row = lax.broadcasted_iota(jnp.int32, (512, 128 * GROUP), 0)
        chosen = jnp.where(grid_row == cell // 128, 1.0, 0.0).astype(jnp.bfloat16)
        found = jnp.dot(pieces[...], chosen, preferred_element_type=jnp.float32)
        found = (found[:128] + found[128:256]) + found[256:]
        lane = lax.broadcasted_iota(jnp.int32, (128, 128 * GROUP), 0)
        sampled = jnp.sum(jnp.where(lane == cell % 128, found, 0.0), axis=0, keepdims=True)
        column = jnp.transpose(jnp.broadcast_to(sampled, (8, 128 * GROUP)))[:, 0:1]
        fetch(g).wait()
        sources = (records[g].astype(jnp.float32) * column).astype(jnp.bfloat16)
        made = lax.dot_general(
            table[...], sources, (((1,), (1,)), ((), ())), preferred_element_type=jnp.float32
        ).astype(jnp.bfloat16)
        for k in range(GROUP):
            spectra[GROUP * g + k] = made[:, 128 * k : 128 * (k + 1)]
        return carry

    lax.fori_loop(0, groups, front, 0)

    order = (lax.broadcasted_iota(jnp.int32, (8, 128), 0) + 1).astype(jnp.float32)

    def features(b, alive):
        facing, apart = in_pieces(geo[b, 0:8] * alive), in_pieces(geo[b, 8:16])
        return jnp.concatenate(
            [jnp.concatenate([facing[s], apart[s]], axis=1) for s, _ in PAIRS], axis=0
        ).astype(jnp.bfloat16)

    def weights_of(seen, o):
        both = lax.dot_general(
            seen,
            heard[:, OBS_CHUNK * o : OBS_CHUNK * (o + 1)],
            (((0,), (0,)), ((), ())),
            preferred_element_type=jnp.float32,
        )
        return (both[:128] / both[128:]).astype(jnp.bfloat16)

    def add_turned(b, o, product):
        for h in range(OBS_CHUNK // 128):
            lanes = slice(128 * h, 128 * h + 128)
            base = turns[b, :, pl.ds(OBS_CHUNK * o + 128 * h, 128)]
            sine, cosine = sin_cos(base * order)
            step_s = jnp.broadcast_to(sine[7:8], (8, 128))
            step_c = jnp.broadcast_to(cosine[7:8], (8, 128))
            before_s = sine * step_c - cosine * step_s
            before_c = cosine * step_c + sine * step_s
            twice = step_c + step_c
            for a in range(FREQS // 8):
                re = product[8 * a : 8 * a + 8, lanes]
                im = product[FREQS + 8 * a : FREQS + 8 * a + 8, lanes]
                out[o, 0, 2 * a + h] += re * cosine + im * sine
                out[o, 1, 2 * a + h] += im * cosine - re * sine
                if a + 1 < FREQS // 8:
                    sine, before_s = twice * sine - before_s, sine
                    cosine, before_c = twice * cosine - before_c, cosine

    def back(pair, carry):
        blocks = []
        for k in range(PAIR):
            b = PAIR * pair + k
            alive = jnp.where(b < live[0], 1.0, 0.0)
            blocks.append((b, features(b, alive), spectra[b]))
        for o in range(1024 // OBS_CHUNK):
            for b, seen, spectrum in blocks:
                product = jnp.dot(
                    spectrum, weights_of(seen, o), preferred_element_type=jnp.float32
                )
                add_turned(b, o, product)
        return carry

    lax.fori_loop(0, (live[0] + PAIR - 1) // PAIR, back, 0)


def panel_sums(live_count, updated, record, cells, geo, turns, listeners, table):
    vmem = pl.BlockSpec(memory_space=pltpu.VMEM)
    bf16 = jnp.bfloat16
    return pl.pallas_call(
        panel_kernel,
        out_shape=jax.ShapeDtypeStruct((1024 // OBS_CHUNK, 2, 32, 8, 128), jnp.float32),
        in_specs=[
            pl.BlockSpec(memory_space=pltpu.SMEM),
            pl.BlockSpec(memory_space=pl.ANY),
            pl.BlockSpec(memory_space=pl.ANY),
        ]
        + [vmem] * 5,
        out_specs=vmem,
        scratch_shapes=[
            pltpu.VMEM((512, 128), jnp.float32),
            pltpu.VMEM((GROUPS, 128 * GROUP, 512), bf16),
            pltpu.VMEM((384, 512), bf16),
            pltpu.VMEM((8 * len(PAIRS), 1024), bf16),
            pltpu.VMEM((32, 256, 128), bf16),
            pltpu.SemaphoreType.DMA((GROUPS + 1,)),
        ],
        compiler_params=pltpu.CompilerParams(vmem_limit_bytes=48 * 2**20),
        cost_estimate=pl.CostEstimate(
            flops=4_000_000_000, bytes_accessed=8_000_000, transcendentals=0
        ),
        name="panels",
    )(live_count, updated, record, cells, geo, turns, listeners, table)


def panel_geometry(panel_cell, panel_angles, listener_angles, listener_range, blocks, cells, counts):
    slot_count, block_rows = panel_cell.shape
    places = [p - 0.5 for p in panel_places(panel_cell, blocks, cells, counts)]
    normals = directions(panel_angles.reshape(2, slot_count, block_rows)) * (0.25 / math.pi)
    across = -sum(normals[d] * places[d] for d in range(3))
    square = sum(p * p for p in places)
    blank = jnp.zeros_like(square)
    geo = jnp.stack(
        [normals[0], normals[1], normals[2], across, blank, blank, blank, blank]
        + [-2.0 * p for p in places]
        + [square, blank + 1.0, blank, blank, blank],
        axis=1,
    )
    heard = listener_range[None, :] * directions(listener_angles)
    centres = [jnp.mean(p, axis=1, keepdims=True) for p in places]
    apart = sum((heard[d][None, :] - centres[d]) ** 2 for d in range(3))
    turns = jnp.sqrt(apart) * (WAVE_STEP / (2.0 * math.pi))
    listeners = jnp.concatenate(
        [heard, jnp.ones_like(heard[:1]), jnp.sum(heard * heard, axis=0, keepdims=True), jnp.zeros_like(heard)],
        axis=0,
    )
    return geo, turns.reshape(slot_count, 1, -1), listeners


def local(
    state_old,
    state_section,
    panel_record,
    panel_cell,
    panel_angles,
    owned_blocks,
    listener_angles,
    listener_range,
):
    cells = state_section.shape[1:]
    axes = ("gx", "gy", "gz")
    counts = tuple(n * lax.axis_size(a) for n, a in zip(cells, axes))
    step_size = COURANT / max(counts)
    geo, turns, listeners = panel_geometry(
        panel_cell,
        panel_angles,
        listener_angles,
        listener_range,
        [lax.axis_index(a) for a in axes],
        cells,
        counts,
    )
    updated = flow_update(state_old, state_section, counts, step_size)
    partial = panel_sums(
        owned_blocks,
        updated,
        panel_record,
        panel_cell.reshape(GROUPS, 1, 128 * GROUP),
        geo,
        turns,
        listeners,
        dft_table(panel_record.shape[1], FREQS),
    )
    return updated.reshape(state_section.shape), summed_spectra(partial)


def solution(mesh):
    return jax.shard_map(
        local,
        mesh=mesh,
        in_specs=(
            P(None, "gx", "gy", "gz"),
            P(None, "gx", "gy", "gz"),
            P(("gx", "gy", "gz"), None),
            P(("gx", "gy", "gz"), None),
            P(None, ("gx", "gy", "gz")),
            P(("gx", "gy", "gz")),
            P(),
            P(),
        ),
        out_specs=(P(None, "gx", "gy", "gz"), P(None, "gz", None)),
        check_vma=False,
    )
```

```python
import functools
import math

import jax
import jax.numpy as jnp
from jax import lax
from jax.experimental import pallas as pl
from jax.experimental.pallas import tpu as pltpu
from jax.sharding import PartitionSpec as P

FREQS = 128
GAMMA_GAS = 4.4
PRESSURE_INF = 1.0
WENO_EPS = 1e-06
WAVE_STEP = 0.25
COURANT = 0.08

SCALE = 4.0
EPS = 0.75 * 4.0 * SCALE * SCALE * WENO_EPS


MESH = pl.DeviceIdType.MESH
TILES = 32


def sum_kernel(part, out, came0, sums, came1, total, came2, mine, full, other, s0, r0, s1, r1, s2, r2, s3, r3, s4, r4):
    gx, gy, gz = (lax.axis_index(a) for a in ("gx", "gy", "gz"))
    core, upper = lax.rem(gy, 2), gy // 2
    m = gx * 2 + upper
    partner = {"gx": gx, "gy": upper * 2 + (1 - core), "gz": gz}

    def along(k):
        return {"gx": gx, "gy": gy, "gz": lax.rem(gz + k, 4)}

    def chip(r):
        t = lax.rem(m + r, TILES)
        return t, {"gx": t // 2, "gy": lax.rem(t, 2) * 2 + core, "gz": gz}

    barrier = pltpu.get_barrier_semaphore()

    def greet(device):
        pl.semaphore_signal(barrier, inc=1, device_id=device, device_id_type=MESH)

    greet(partner)
    for k in (1, 2, 3):
        greet(along(k))

    def greet_chip(r, carry):
        greet(chip(r)[1])
        return carry

    lax.fori_loop(1, TILES, greet_chip, 0)
    pl.semaphore_wait(barrier, TILES + 3)

    def remote(src, dst, send, recv, device):
        return pltpu.make_async_remote_copy(
            src_ref=src, dst_ref=dst, send_sem=send, recv_sem=recv, device_id=device, device_id_type=MESH
        )

    shares, along_gz = {}, {}
    for k in (2, 1, 3, 0):
        shares[k] = remote(
            part.at[lax.rem(gz + k, 4), 1 - core], came0.at[k], s0.at[k], r0.at[k], partner
        )
        shares[k].start()
    for k in (2, 1, 3, 0):
        shares[k].wait_recv()
        sums[k] = part[lax.rem(gz + k, 4), core] + came0[k]
        if k > 0:
            along_gz[k] = remote(sums.at[k], came1.at[k - 1], s1.at[k - 1], r1.at[k - 1], along(k))
            along_gz[k].start()
    for k in (1, 3, 2):
        along_gz[k].wait_recv()
    total[...] = (sums[0] + came1[0]) + (came1[1] + came1[2])

    def scatter(r, carry):
        t, device = chip(r)
        remote(total.at[t], came2.at[r - 1], s2, r2, device).start()
        return carry

    lax.fori_loop(1, TILES, scatter, 0)
    pltpu.make_async_copy(came2, came2, r2).wait()
    own = total[m]
    for r in range(TILES - 1):
        own = own + came2[r]
    mine[...] = own
    full[m] = own

    def gather(r, carry):
        remote(mine, full.at[m], s3, r3, chip(r)[1]).start()
        return carry

    lax.fori_loop(1, TILES, gather, 0)
    pltpu.make_async_copy(came2, came2, r3).wait()
    swap = remote(full, other, s4, r4, partner)
    swap.start()

    def lay(which, tiles):
        for h in range(2):
            block = jnp.concatenate([tiles[2 * a + h] for a in range(16)], axis=0)
            out[which, pl.ds(128 * h, 128), :] = jnp.transpose(block)

    lay(core, full)
    swap.wait_recv()
    lay(1 - core, other)
    for k in (0, 1, 2, 3):
        shares[k].wait_send()
        if k > 0:
            along_gz[k].wait_send()
    pltpu.make_async_copy(came2, came2, s2).wait()
    pltpu.make_async_copy(came2, came2, s3).wait()
    swap.wait_send()


def summed_spectra(part):
    vmem = pl.BlockSpec(memory_space=pltpu.VMEM)
    f32 = jnp.float32
    tiles = (TILES, 8, 128)
    dma = pltpu.SemaphoreType.DMA
    return pl.pallas_call(
        sum_kernel,
        out_shape=jax.ShapeDtypeStruct((2, 256, FREQS), f32),
        in_specs=[vmem],
        out_specs=vmem,
        scratch_shapes=[
            pltpu.VMEM((4, *tiles), f32),
            pltpu.VMEM((4, *tiles), f32),
            pltpu.VMEM((3, *tiles), f32),
            pltpu.VMEM(tiles, f32),
            pltpu.VMEM((TILES - 1, 8, 128), f32),
            pltpu.VMEM((8, 128), f32),
            pltpu.VMEM(tiles, f32),
            pltpu.VMEM(tiles, f32),
            dma((4,)),
            dma((4,)),
            dma((3,)),
            dma((3,)),
            dma,
            dma,
            dma,
            dma,
            dma,
            dma,
        ],
        compiler_params=pltpu.CompilerParams(collective_id=1, has_side_effects=True),
        name="sum_spectra",
    )(part)


def flux_of(state, axis_d):
    density, energy = state[0], state[4]
    momenta = state[1:4]
    inverse = 1.0 / density
    velocity = [m * inverse for m in momenta]
    kinetic = 0.5 * (momenta[0] * velocity[0] + momenta[1] * velocity[1] + momenta[2] * velocity[2])
    pressure = (GAMMA_GAS - 1.0) * (energy - kinetic) - GAMMA_GAS * PRESSURE_INF * SCALE
    normal = velocity[axis_d]
    square = GAMMA_GAS * (pressure + PRESSURE_INF * SCALE) * inverse
    sound = square * lax.rsqrt(square)
    rows = [momenta[axis_d]]
    for component in range(3):
        carried = momenta[component] * normal
        rows.append(carried + pressure if component == axis_d else carried)
    rows.append((energy + pressure) * normal)
    return rows, jnp.abs(normal) + sound


def weno_terms(e0, e1, e2, d1, d2):
    q1, q2 = 0.75 * d1, 0.75 * d2
    base1 = d1 * q1 + EPS
    base2 = d2 * q2 + EPS
    t0 = e0 * (e0 + q1) + base1
    t1 = e1 * (e1 + q1) + base1
    t2 = e2 * (e2 - q2) + base2
    p01, p02, p12 = t0 * t1, t0 * t2, t1 * t2
    wa = p12 * p12
    wb = 6.0 * (p02 * p02)
    wc = 1.5 * (p01 * p01)
    return wa * (e0 - e1) + wc * (e1 - e2), (wa + wb) + (wc + wc)


def face_value(alpha, df, dq, fsum):
    aq = [alpha * v for v in dq]
    up = [df[j] + aq[j] for j in range(4)]
    dn = [None] + [df[j] - aq[j] for j in range(1, 5)]
    num_p, den_p = weno_terms(up[1] - up[0], up[2] - up[1], up[3] - up[2], up[1], up[2])
    num_m, den_m = weno_terms(dn[4] - dn[3], dn[3] - dn[2], dn[2] - dn[1], -dn[3], -dn[2])
    ratio = (num_p * den_m + num_m * den_p) / (den_p * den_m)
    return fsum + ((0.5 * (up[1] - dn[3]) - aq[2]) + ratio) * (1.0 / 3.0)


def sweep(planes, dq, df, fs, m2, faces, axis_d, cells, chunks, streams):
    def load(r, j):
        return [planes[c, j, pl.ds(8 * r, 8), :] for c in range(5)]

    for group, length in streams:

        def step(k, carry):
            for u in range(3):
                after = []
                for (r, start), (state, flux, speed) in zip(group, carry):
                    j, rows = start + 3 * k + u, pl.ds(8 * r, 8)
                    next_state = load(r, j + 1)
                    next_flux, next_speed = flux_of(next_state, axis_d)
                    for c in range(5):
                        dq[c, j, rows, :] = next_state[c] - state[c]
                        df[c, j, rows, :] = next_flux[c] - flux[c]
                        fs[c, j, rows, :] = next_flux[c] + flux[c]
                    m2[j, rows, :] = jnp.maximum(next_speed, speed)
                    after.append((next_state, next_flux, next_speed))
                carry = after
            return carry

        begin = []
        for r, start in group:
            state = load(r, start)
            begin.append((state, *flux_of(state, axis_d)))
        lax.fori_loop(0, length, step, begin)

    def face(i, carry):
        for r in range(chunks):
            rows = pl.ds(8 * r, 8)
            alpha = jnp.maximum(jnp.maximum(m2[i, rows, :], m2[i + 2, rows, :]), m2[i + 4, rows, :])
            for c in range(5):
                faces[c, i, rows, :] = face_value(
                    alpha,
                    [df[c, i + j, rows, :] for j in range(5)],
                    [dq[c, i + j, rows, :] for j in range(5)],
                    fs[c, i + 2, rows, :],
                )
        return carry

    lax.fori_loop(0, cells + 1, face, 0)


def z_turn(q, turned):
    for c in range(5):
        for blk in range(4):
            tile = jnp.transpose(q[c, pl.ds(128 * blk, 128), :]) * SCALE
            turned[c, pl.ds(160 * blk + 8, 72), :] = tile[:72]
            turned[c, pl.ds(160 * blk + 80, 72), :] = tile[56:]


def z_part(coef, out, turned, planes, dq, df, fs, m2, faces, diff):
    def gather(j, carry):
        for c in range(5):
            planes[c, j] = turned[c, pl.ds(j + 5, 8, stride=80), :]
        return carry

    lax.fori_loop(0, 70, gather, 0, unroll=2)
    sweep(planes, dq, df, fs, m2, faces, 2, 64, 1, [(((0, 0), (0, 33)), 12)])

    def difference(i, carry):
        for c in range(5):
            diff[c, pl.ds(pl.multiple_of(8 * i, 8), 8), :] = coef * (faces[c, i + 1] - faces[c, i])
        return carry

    lax.fori_loop(0, 64, difference, 0, unroll=2)
    for c in range(5):
        for blk in range(4):
            tile = jnp.concatenate(
                [diff[c, pl.ds(2 * blk + half, 64, stride=8), :] for half in range(2)], axis=0
            )
            out[c, pl.ds(128 * blk, 128), :] = jnp.transpose(tile)


def y_part(coef, out, planes, dq, df, fs, m2, faces, diff):
    sweep(planes, dq, df, fs, m2, faces, 1, 32, 2, [(((0, 0), (1, 0)), 13)])

    def difference(i, carry):
        for c in range(5):
            diff[c, pl.ds(pl.multiple_of(16 * i, 16), 16), :] = coef * (
                faces[c, i + 1] - faces[c, i]
            )
        return carry

    lax.fori_loop(0, 32, difference, 0)

    def back(x, carry):
        for c in range(5):
            for y8 in range(4):
                rows = pl.ds(pl.multiple_of(32 * x + 8 * y8, 8), 8)
                out[c, rows, :] += diff[c, pl.ds(128 * y8 + x, 8, stride=16), :]
        return carry

    lax.fori_loop(0, 16, back, 0)


def x_part(coef, q, add, old, out, planes, dq, df, fs, m2, faces):
    streams = [(((0, 0), (1, 0)), 7), (((2, 0), (3, 0)), 7)]
    sweep(planes, dq, df, fs, m2, faces, 0, 16, 4, streams)

    def finish(i, carry):
        rows = pl.ds(pl.multiple_of(32 * i, 32), 32)
        for c in range(5):
            change = add[c, rows, :] + coef * (faces[c, i + 1] - faces[c, i])
            out[c, rows, :] = (0.75 * old[c, rows, :] + 0.25 * q[c, rows, :]) - change
        return carry

    lax.fori_loop(0, 16, finish, 0)


def flow_kernel(coefs, q, old_in, out, turned, diff, add, old, send, recv, old_sem, *spaces):
    here = {a: lax.axis_index(a) for a in ("gx", "gy", "gz")}

    def beside(axis, step):
        return {**here, axis: lax.rem(here[axis] + step, lax.axis_size(axis))}

    sides = {a: (beside(a, 1), beside(a, lax.axis_size(a) - 1)) for a in here}
    barrier = pltpu.get_barrier_semaphore()
    for up, down in sides.values():
        for device in (up, down):
            pl.semaphore_signal(barrier, inc=1, device_id=device, device_id_type=MESH)

    fetch_old = pltpu.make_async_copy(old_in, old, old_sem)
    fetch_old.start()
    planes_x, planes_y = spaces[12], spaces[6]

    def gather_x(j, carry):
        for c in range(5):
            planes_x[c, j + 3] = q[c, pl.ds(pl.multiple_of(32 * j, 32), 32), :] * SCALE
        return carry

    lax.fori_loop(0, 16, gather_x, 0)

    def gather_y(j, carry):
        for c in range(5):
            for h in range(2):
                planes_y[c, j + 3, pl.ds(8 * h, 8), :] = (
                    q[c, pl.ds(j + 256 * h, 8, stride=32), :] * SCALE
                )
        return carry

    lax.fori_loop(0, 32, gather_y, 0)
    pl.semaphore_wait(barrier, 6)
    slots = iter(range(12))

    def move(src, dst, device):
        k = next(slots)
        copy = pltpu.make_async_remote_copy(
            src_ref=src,
            dst_ref=dst,
            send_sem=send.at[k],
            recv_sem=recv.at[k],
            device_id=device,
            device_id_type=MESH,
        )
        copy.start()
        return copy

    along_y = [
        move(planes_y.at[:, pl.ds(32, 3)], planes_y.at[:, pl.ds(0, 3)], sides["gy"][0]),
        move(planes_y.at[:, pl.ds(3, 3)], planes_y.at[:, pl.ds(35, 3)], sides["gy"][1]),
    ]
    along_x = [
        move(planes_x.at[:, pl.ds(16, 3)], planes_x.at[:, pl.ds(0, 3)], sides["gx"][0]),
        move(planes_x.at[:, pl.ds(3, 3)], planes_x.at[:, pl.ds(19, 3)], sides["gx"][1]),
    ]
    z_turn(q, turned)
    along_z = []
    for blk in range(4):
        low, high = turned.at[:, pl.ds(160 * blk, 8)], turned.at[:, pl.ds(160 * blk + 152, 8)]
        first, last = turned.at[:, pl.ds(160 * blk + 8, 8)], turned.at[:, pl.ds(160 * blk + 144, 8)]
        along_z.append(move(last, low, sides["gz"][0]))
        along_z.append(move(first, high, sides["gz"][1]))
    for copy in along_z:
        copy.wait_recv()
    z_part(coefs[2], add, turned, *spaces[0:6], diff)
    for copy in along_y:
        copy.wait_recv()
    y_part(coefs[1], add, *spaces[6:12], diff)
    for copy in along_x:
        copy.wait_recv()
    fetch_old.wait()
    x_part(coefs[0], q, add, old, out, *spaces[12:18])
    for copy in along_x + along_y + along_z:
        copy.wait_send()


def sweep_scratch(cells, rows):
    f32 = jnp.float32
    steps = -(-(cells + 5) // 3) * 3
    return [
        pltpu.VMEM((5, steps + 1, rows, 128), f32),
        pltpu.VMEM((5, steps, rows, 128), f32),
        pltpu.VMEM((5, steps, rows, 128), f32),
        pltpu.VMEM((5, steps, rows, 128), f32),
        pltpu.VMEM((steps, rows, 128), f32),
        pltpu.VMEM((5, cells + 1, rows, 128), f32),
    ]


def flow_update(state_old, state_section, counts, step_size):
    f32 = jnp.float32
    coefs = [0.25 * step_size * n / (2.0 * SCALE) for n in counts]
    return pl.pallas_call(
        functools.partial(flow_kernel, coefs),
        out_shape=jax.ShapeDtypeStruct((5, 512, 128), f32),
        in_specs=[pl.BlockSpec(memory_space=pltpu.VMEM), pl.BlockSpec(memory_space=pl.ANY)],
        scratch_shapes=[pltpu.VMEM((5, 640, 128), f32)]
        + [pltpu.VMEM((5, 512, 128), f32)] * 3
        + [pltpu.SemaphoreType.DMA((12,)), pltpu.SemaphoreType.DMA((12,)), pltpu.SemaphoreType.DMA]
        + sweep_scratch(64, 8)
        + sweep_scratch(32, 16)
        + sweep_scratch(16, 32),
        compiler_params=pltpu.CompilerParams(
            vmem_limit_bytes=56 * 2**20, collective_id=0, has_side_effects=True
        ),
        cost_estimate=pl.CostEstimate(flops=100_000_000, bytes_accessed=6_000_000, transcendentals=0),
        name="flow",
    )(state_section.reshape(5, 512, 128), state_old.reshape(5, 512, 128))


def directions(angles):
    polar_angle = 0.5 * angles[0]
    azimuth = angles[1]
    return jnp.stack(
        [
            jnp.cos(polar_angle) * jnp.cos(azimuth),
            jnp.cos(polar_angle) * jnp.sin(azimuth),
            jnp.sin(polar_angle),
        ]
    )


def panel_places(cell_rows, blocks, cells, counts):
    along = (
        cell_rows // (cells[1] * cells[2]),
        cell_rows // cells[2] % cells[1],
        cell_rows % cells[2],
    )
    return [
        ((blocks[d] * cells[d] + along[d]).astype(jnp.float32) + 0.5) / counts[d] for d in range(3)
    ]


def dft_table(sample_count, freq_count):
    times = jnp.arange(sample_count, dtype=jnp.int32)[None, :]
    orders = jnp.arange(1, freq_count + 1, dtype=jnp.int32)[:, None]
    phases = 2.0 * math.pi / sample_count * (times * orders % sample_count).astype(jnp.float32)
    scaling = 1.0 / math.sqrt(sample_count)
    return (jnp.concatenate([jnp.cos(phases), -jnp.sin(phases)], axis=0) * scaling).astype(
        jnp.bfloat16
    )


def sin_cos(turns):
    rest = turns - jnp.round(turns)
    half = rest * rest
    s = (3.1996934769709044, -14.868610848632139, 42.01616577638672, -76.70155116950977,
         81.60502462208919, -41.341697068940945, 6.283185307179586)
    c = (6.529609897637814, -25.96831291454545, 60.167831622681774, -85.45016553628534,
         64.93911898307624, -19.73920453207708, 1.0)
    sine = jnp.full_like(half, s[0])
    for k in s[1:]:
        sine = sine * half + k
    cosine = jnp.full_like(half, c[0])
    for k in c[1:]:
        cosine = cosine * half + k
    return sine * rest, cosine


OBS_CHUNK = 256


def in_pieces(values):
    pieces = []
    for _ in range(3):
        piece = values.astype(jnp.bfloat16).astype(jnp.float32)
        pieces.append(piece)
        values = values - piece
    return pieces


PAIRS = ((0, 0), (0, 1), (1, 0), (0, 2), (1, 1), (2, 0))


GROUP = 4
GROUPS = 8
PAIR = 2


def panel_kernel(
    live, updated, record, cells, geo, turns, listeners, table, out, density, records, pieces, heard, spectra, sems
):
    groups = (live[0] + GROUP - 1) // GROUP

    def fetch(g):
        return pltpu.make_async_copy(
            record.at[pl.ds(128 * GROUP * g, 128 * GROUP)], records.at[g], sems.at[g]
        )

    first = pltpu.make_async_copy(updated.at[0], density, sems.at[GROUPS])
    first.start()
    for g in range(GROUPS):
        pl.when(g < groups)(fetch(g).start)

    out[...] = jnp.zeros_like(out)
    split = in_pieces(listeners[...])
    heard[...] = jnp.concatenate([split[t] for _, t in PAIRS], axis=0).astype(jnp.bfloat16)
    first.wait()
    turned = jnp.concatenate(
        [jnp.transpose(density[pl.ds(128 * k, 128), :]) for k in range(4)], axis=1
    )
    for k, piece in enumerate(in_pieces(turned)):
        pieces[pl.ds(128 * k, 128), :] = piece.astype(jnp.bfloat16)

    def front(g, carry):
        cell = cells[g]
        grid_row = lax.broadcasted_iota(jnp.int32, (512, 128 * GROUP), 0)
        chosen = jnp.where(grid_row == cell // 128, 1.0, 0.0).astype(jnp.bfloat16)
        found = jnp.dot(pieces[...], chosen, preferred_element_type=jnp.float32)
        found = (found[:128] + found[128:256]) + found[256:]
        lane = lax.broadcasted_iota(jnp.int32, (128, 128 * GROUP), 0)
        sampled = jnp.sum(jnp.where(lane == cell % 128, found, 0.0), axis=0, keepdims=True)
        column = jnp.transpose(jnp.broadcast_to(sampled, (8, 128 * GROUP)))[:, 0:1]
        fetch(g).wait()
        sources = (records[g].astype(jnp.float32) * column).astype(jnp.bfloat16)
        made = lax.dot_general(
            table[...], sources, (((1,), (1,)), ((), ())), preferred_element_type=jnp.float32
        ).astype(jnp.bfloat16)
        for k in range(GROUP):
            spectra[GROUP * g + k] = made[:, 128 * k : 128 * (k + 1)]
        return carry

    lax.fori_loop(0, groups, front, 0)

    order = (lax.broadcasted_iota(jnp.int32, (8, 128), 0) + 1).astype(jnp.float32)

    def features(b, alive):
        facing, apart = in_pieces(geo[b, 0:8] * alive), in_pieces(geo[b, 8:16])
        return jnp.concatenate(
            [jnp.concatenate([facing[s], apart[s]], axis=1) for s, _ in PAIRS], axis=0
        ).astype(jnp.bfloat16)

    def weights_of(seen, o):
        both = lax.dot_general(
            seen,
            heard[:, OBS_CHUNK * o : OBS_CHUNK * (o + 1)],
            (((0,), (0,)), ((), ())),
            preferred_element_type=jnp.float32,
        )
        return (both[:128] / both[128:]).astype(jnp.bfloat16)

    def add_turned(b, o, product):
        for h in range(OBS_CHUNK // 128):
            lanes = slice(128 * h, 128 * h + 128)
            base = turns[b, :, pl.ds(OBS_CHUNK * o + 128 * h, 128)]
            sine, cosine = sin_cos(base * order)
            step_s = jnp.broadcast_to(sine[7:8], (8, 128))
            step_c = jnp.broadcast_to(cosine[7:8], (8, 128))
            before_s = sine * step_c - cosine * step_s
            before_c = cosine * step_c + sine * step_s
            twice = step_c + step_c
            for a in range(FREQS // 8):
                re = product[8 * a : 8 * a + 8, lanes]
                im = product[FREQS + 8 * a : FREQS + 8 * a + 8, lanes]
                out[o, 0, 2 * a + h] += re * cosine + im * sine
                out[o, 1, 2 * a + h] += im * cosine - re * sine
                if a + 1 < FREQS // 8:
                    sine, before_s = twice * sine - before_s, sine
                    cosine, before_c = twice * cosine - before_c, cosine

    def back(pair, carry):
        blocks = []
        for k in range(PAIR):
            b = PAIR * pair + k
            alive = jnp.where(b < live[0], 1.0, 0.0)
            blocks.append((b, features(b, alive), spectra[b]))
        for o in range(1024 // OBS_CHUNK):
            for b, seen, spectrum in blocks:
                product = jnp.dot(
                    spectrum, weights_of(seen, o), preferred_element_type=jnp.float32
                )
                add_turned(b, o, product)
        return carry

    lax.fori_loop(0, (live[0] + PAIR - 1) // PAIR, back, 0)


def panel_sums(live_count, updated, record, cells, geo, turns, listeners, table):
    vmem = pl.BlockSpec(memory_space=pltpu.VMEM)
    bf16 = jnp.bfloat16
    return pl.pallas_call(
        panel_kernel,
        out_shape=jax.ShapeDtypeStruct((1024 // OBS_CHUNK, 2, 32, 8, 128), jnp.float32),
        in_specs=[
            pl.BlockSpec(memory_space=pltpu.SMEM),
            pl.BlockSpec(memory_space=pl.ANY),
            pl.BlockSpec(memory_space=pl.ANY),
        ]
        + [vmem] * 5,
        out_specs=vmem,
        scratch_shapes=[
            pltpu.VMEM((512, 128), jnp.float32),
            pltpu.VMEM((GROUPS, 128 * GROUP, 512), bf16),
            pltpu.VMEM((384, 512), bf16),
            pltpu.VMEM((8 * len(PAIRS), 1024), bf16),
            pltpu.VMEM((32, 256, 128), bf16),
            pltpu.SemaphoreType.DMA((GROUPS + 1,)),
        ],
        compiler_params=pltpu.CompilerParams(vmem_limit_bytes=48 * 2**20),
        cost_estimate=pl.CostEstimate(
            flops=4_000_000_000, bytes_accessed=8_000_000, transcendentals=0
        ),
        name="panels",
    )(live_count, updated, record, cells, geo, turns, listeners, table)


def panel_geometry(panel_cell, panel_angles, listener_angles, listener_range, blocks, cells, counts):
    slot_count, block_rows = panel_cell.shape
    places = [p - 0.5 for p in panel_places(panel_cell, blocks, cells, counts)]
    normals = directions(panel_angles.reshape(2, slot_count, block_rows)) * (0.25 / math.pi)
    across = -sum(normals[d] * places[d] for d in range(3))
    square = sum(p * p for p in places)
    blank = jnp.zeros_like(square)
    geo = jnp.stack(
        [normals[0], normals[1], normals[2], across, blank, blank, blank, blank]
        + [-2.0 * p for p in places]
        + [square, blank + 1.0, blank, blank, blank],
        axis=1,
    )
    heard = listener_range[None, :] * directions(listener_angles)
    centres = [jnp.mean(p, axis=1, keepdims=True) for p in places]
    apart = sum((heard[d][None, :] - centres[d]) ** 2 for d in range(3))
    turns = jnp.sqrt(apart) * (WAVE_STEP / (2.0 * math.pi))
    listeners = jnp.concatenate(
        [heard, jnp.ones_like(heard[:1]), jnp.sum(heard * heard, axis=0, keepdims=True), jnp.zeros_like(heard)],
        axis=0,
    )
    return geo, turns.reshape(slot_count, 1, -1), listeners


def local(
    state_old,
    state_section,
    panel_record,
    panel_cell,
    panel_angles,
    owned_blocks,
    listener_angles,
    listener_range,
):
    cells = state_section.shape[1:]
    axes = ("gx", "gy", "gz")
    counts = tuple(n * lax.axis_size(a) for n, a in zip(cells, axes))
    step_size = COURANT / max(counts)
    geo, turns, listeners = panel_geometry(
        panel_cell,
        panel_angles,
        listener_angles,
        listener_range,
        [lax.axis_index(a) for a in axes],
        cells,
        counts,
    )
    updated = flow_update(state_old, state_section, counts, step_size)
    partial = panel_sums(
        owned_blocks,
        updated,
        panel_record,
        panel_cell.reshape(GROUPS, 1, 128 * GROUP),
        geo,
        turns,
        listeners,
        dft_table(panel_record.shape[1], FREQS),
    )
    return updated.reshape(state_section.shape), summed_spectra(partial)


def solution(mesh):
    return jax.shard_map(
        local,
        mesh=mesh,
        in_specs=(
            P(None, "gx", "gy", "gz"),
            P(None, "gx", "gy", "gz"),
            P(("gx", "gy", "gz"), None),
            P(("gx", "gy", "gz"), None),
            P(None, ("gx", "gy", "gz")),
            P(("gx", "gy", "gz")),
            P(),
            P(),
        ),
        out_specs=(P(None, "gx", "gy", "gz"), P(None, "gz", None)),
        check_vma=False,
    )
```

```python
import functools
import math

import jax
import jax.numpy as jnp
import numpy as np
from jax import lax
from jax.experimental import pallas as pl
from jax.experimental.pallas import tpu as pltpu
from jax.sharding import PartitionSpec as P

FREQS = 128
GAMMA_GAS = 4.4
PRESSURE_INF = 1.0
WENO_EPS = 1e-06
WAVE_STEP = 0.25
COURANT = 0.08

SCALE = 4.0
EPS = 0.75 * 4.0 * SCALE * SCALE * WENO_EPS


MESH = pl.DeviceIdType.MESH
TILES = 32


def sum_kernel(part, out, came0, sums, came1, total, came2, mine, full, other, s0, r0, s1, r1, s2, r2, s3, r3, s4, r4):
    gx, gy, gz = (lax.axis_index(a) for a in ("gx", "gy", "gz"))
    core, upper = lax.rem(gy, 2), gy // 2
    m = gx * 2 + upper
    partner = {"gx": gx, "gy": upper * 2 + (1 - core), "gz": gz}

    def along(k):
        return {"gx": gx, "gy": gy, "gz": lax.rem(gz + k, 4)}

    def chip(r):
        t = lax.rem(m + r, TILES)
        return t, {"gx": t // 2, "gy": lax.rem(t, 2) * 2 + core, "gz": gz}

    barrier = pltpu.get_barrier_semaphore()

    def greet(device):
        pl.semaphore_signal(barrier, inc=1, device_id=device, device_id_type=MESH)

    greet(partner)
    for k in (1, 2, 3):
        greet(along(k))

    def greet_chip(r, carry):
        greet(chip(r)[1])
        return carry

    lax.fori_loop(1, TILES, greet_chip, 0)
    pl.semaphore_wait(barrier, TILES + 3)

    def remote(src, dst, send, recv, device):
        return pltpu.make_async_remote_copy(
            src_ref=src, dst_ref=dst, send_sem=send, recv_sem=recv, device_id=device, device_id_type=MESH
        )

    shares, along_gz = {}, {}
    for k in (2, 1, 3, 0):
        shares[k] = remote(
            part.at[lax.rem(gz + k, 4), 1 - core], came0.at[k], s0.at[k], r0.at[k], partner
        )
        shares[k].start()
    for k in (2, 1, 3, 0):
        shares[k].wait_recv()
        sums[k] = part[lax.rem(gz + k, 4), core] + came0[k]
        if k > 0:
            along_gz[k] = remote(sums.at[k], came1.at[k - 1], s1.at[k - 1], r1.at[k - 1], along(k))
            along_gz[k].start()
    for k in (1, 3, 2):
        along_gz[k].wait_recv()
    total[...] = (sums[0] + came1[0]) + (came1[1] + came1[2])

    def scatter(r, carry):
        t, device = chip(r)
        remote(total.at[t], came2.at[r - 1], s2, r2, device).start()
        return carry

    lax.fori_loop(1, TILES, scatter, 0)
    pltpu.make_async_copy(came2, came2, r2).wait()
    own = total[m]
    for r in range(TILES - 1):
        own = own + came2[r]
    mine[...] = own
    full[m] = own

    def gather(r, carry):
        remote(mine, full.at[m], s3, r3, chip(r)[1]).start()
        return carry

    lax.fori_loop(1, TILES, gather, 0)
    pltpu.make_async_copy(came2, came2, r3).wait()
    swap = remote(full, other, s4, r4, partner)
    swap.start()

    def lay(which, tiles):
        for h in range(2):
            block = jnp.concatenate([tiles[2 * a + h] for a in range(16)], axis=0)
            out[which, pl.ds(128 * h, 128), :] = jnp.transpose(block)

    lay(core, full)
    swap.wait_recv()
    lay(1 - core, other)
    for k in (0, 1, 2, 3):
        shares[k].wait_send()
        if k > 0:
            along_gz[k].wait_send()
    pltpu.make_async_copy(came2, came2, s2).wait()
    pltpu.make_async_copy(came2, came2, s3).wait()
    swap.wait_send()


def summed_spectra(part):
    vmem = pl.BlockSpec(memory_space=pltpu.VMEM)
    f32 = jnp.float32
    tiles = (TILES, 8, 128)
    dma = pltpu.SemaphoreType.DMA
    return pl.pallas_call(
        sum_kernel,
        out_shape=jax.ShapeDtypeStruct((2, 256, FREQS), f32),
        in_specs=[vmem],
        out_specs=vmem,
        scratch_shapes=[
            pltpu.VMEM((4, *tiles), f32),
            pltpu.VMEM((4, *tiles), f32),
            pltpu.VMEM((3, *tiles), f32),
            pltpu.VMEM(tiles, f32),
            pltpu.VMEM((TILES - 1, 8, 128), f32),
            pltpu.VMEM((8, 128), f32),
            pltpu.VMEM(tiles, f32),
            pltpu.VMEM(tiles, f32),
            dma((4,)),
            dma((4,)),
            dma((3,)),
            dma((3,)),
            dma,
            dma,
            dma,
            dma,
            dma,
            dma,
        ],
        compiler_params=pltpu.CompilerParams(
            vmem_limit_bytes=63 * 2**20, collective_id=1, has_side_effects=True
        ),
        name="sum_spectra",
    )(part)


def flux_of(state, axis_d):
    density, energy = state[0], state[4]
    momenta = state[1:4]
    inverse = 1.0 / density
    velocity = [m * inverse for m in momenta]
    kinetic = 0.5 * (momenta[0] * velocity[0] + momenta[1] * velocity[1] + momenta[2] * velocity[2])
    pressure = (GAMMA_GAS - 1.0) * (energy - kinetic) - GAMMA_GAS * PRESSURE_INF * SCALE
    normal = velocity[axis_d]
    square = GAMMA_GAS * (pressure + PRESSURE_INF * SCALE) * inverse
    sound = square * lax.rsqrt(square)
    rows = [momenta[axis_d]]
    for component in range(3):
        carried = momenta[component] * normal
        rows.append(carried + pressure if component == axis_d else carried)
    rows.append((energy + pressure) * normal)
    return rows, jnp.abs(normal) + sound


def weno_terms(e0, e1, e2, d1, d2):
    q1, q2 = 0.75 * d1, 0.75 * d2
    base1 = d1 * q1 + EPS
    base2 = d2 * q2 + EPS
    t0 = e0 * (e0 + q1) + base1
    t1 = e1 * (e1 + q1) + base1
    t2 = e2 * (e2 - q2) + base2
    p01, p02, p12 = t0 * t1, t0 * t2, t1 * t2
    wa = p12 * p12
    wb = 6.0 * (p02 * p02)
    wc = 1.5 * (p01 * p01)
    return wa * (e0 - e1) + wc * (e1 - e2), (wa + wb) + (wc + wc)


def face_value(alpha, df, dq, fsum):
    aq = [alpha * v for v in dq]
    up = [df[j] + aq[j] for j in range(4)]
    dn = [None] + [df[j] - aq[j] for j in range(1, 5)]
    num_p, den_p = weno_terms(up[1] - up[0], up[2] - up[1], up[3] - up[2], up[1], up[2])
    num_m, den_m = weno_terms(dn[4] - dn[3], dn[3] - dn[2], dn[2] - dn[1], -dn[3], -dn[2])
    ratio = (num_p * den_m + num_m * den_p) / (den_p * den_m)
    return fsum + ((0.5 * (up[1] - dn[3]) - aq[2]) + ratio) * (1.0 / 3.0)


def sweep(planes, dq, df, fs, m2, faces, axis_d, cells, chunks, streams):
    def load(r, j):
        return [planes[c, j, pl.ds(8 * r, 8), :] for c in range(5)]

    for group, length in streams:

        def step(k, carry):
            for u in range(3):
                after = []
                for (r, start), (state, flux, speed) in zip(group, carry):
                    j, rows = start + 3 * k + u, pl.ds(8 * r, 8)
                    next_state = load(r, j + 1)
                    next_flux, next_speed = flux_of(next_state, axis_d)
                    for c in range(5):
                        dq[c, j, rows, :] = next_state[c] - state[c]
                        df[c, j, rows, :] = next_flux[c] - flux[c]
                        fs[c, j, rows, :] = next_flux[c] + flux[c]
                    m2[j, rows, :] = jnp.maximum(next_speed, speed)
                    after.append((next_state, next_flux, next_speed))
                carry = after
            return carry

        begin = []
        for r, start in group:
            state = load(r, start)
            begin.append((state, *flux_of(state, axis_d)))
        lax.fori_loop(0, length, step, begin)

    def face(i, carry):
        for r in range(chunks):
            rows = pl.ds(8 * r, 8)
            alpha = jnp.maximum(jnp.maximum(m2[i, rows, :], m2[i + 2, rows, :]), m2[i + 4, rows, :])
            for c in range(5):
                faces[c, i, rows, :] = face_value(
                    alpha,
                    [df[c, i + j, rows, :] for j in range(5)],
                    [dq[c, i + j, rows, :] for j in range(5)],
                    fs[c, i + 2, rows, :],
                )
        return carry

    lax.fori_loop(0, cells + 1, face, 0)


def z_turn(q, turned):
    for c in range(5):
        for blk in range(4):
            tile = jnp.transpose(q[c, pl.ds(128 * blk, 128), :]) * SCALE
            turned[c, pl.ds(160 * blk + 8, 72), :] = tile[:72]
            turned[c, pl.ds(160 * blk + 80, 72), :] = tile[56:]


def z_part(coef, out, turned, planes, dq, df, fs, m2, faces, diff):
    def gather(j, carry):
        for c in range(5):
            planes[c, j] = turned[c, pl.ds(j + 5, 8, stride=80), :]
        return carry

    lax.fori_loop(0, 70, gather, 0, unroll=2)
    sweep(planes, dq, df, fs, m2, faces, 2, 64, 1, [(((0, 0), (0, 33)), 12)])

    def difference(i, carry):
        for c in range(5):
            diff[c, pl.ds(pl.multiple_of(8 * i, 8), 8), :] = coef * (faces[c, i + 1] - faces[c, i])
        return carry

    lax.fori_loop(0, 64, difference, 0, unroll=2)
    for c in range(5):
        for blk in range(4):
            tile = jnp.concatenate(
                [diff[c, pl.ds(2 * blk + half, 64, stride=8), :] for half in range(2)], axis=0
            )
            out[c, pl.ds(128 * blk, 128), :] = jnp.transpose(tile)


def y_part(coef, out, planes, dq, df, fs, m2, faces, diff):
    sweep(planes, dq, df, fs, m2, faces, 1, 32, 2, [(((0, 0), (1, 0)), 13)])

    def difference(i, carry):
        for c in range(5):
            diff[c, pl.ds(pl.multiple_of(16 * i, 16), 16), :] = coef * (
                faces[c, i + 1] - faces[c, i]
            )
        return carry

    lax.fori_loop(0, 32, difference, 0)

    def back(x, carry):
        for c in range(5):
            for y8 in range(4):
                rows = pl.ds(pl.multiple_of(32 * x + 8 * y8, 8), 8)
                out[c, rows, :] += diff[c, pl.ds(128 * y8 + x, 8, stride=16), :]
        return carry

    lax.fori_loop(0, 16, back, 0)


def x_part(coef, add, out, planes, dq, df, fs, m2, faces):
    streams = [(((0, 0), (1, 0)), 7), (((2, 0), (3, 0)), 7)]
    sweep(planes, dq, df, fs, m2, faces, 0, 16, 4, streams)

    def finish(i, carry):
        rows = pl.ds(pl.multiple_of(32 * i, 32), 32)
        for c in range(5):
            out[c, rows, :] = add[c, rows, :] + coef * (faces[c, i + 1] - faces[c, i])
        return carry

    lax.fori_loop(0, 16, finish, 0)


def flow_kernel(coefs, q, out, turned, diff, add, send, recv, *spaces):
    here = {a: lax.axis_index(a) for a in ("gx", "gy", "gz")}

    def beside(axis, step):
        return {**here, axis: lax.rem(here[axis] + step, lax.axis_size(axis))}

    sides = {a: (beside(a, 1), beside(a, lax.axis_size(a) - 1)) for a in here}
    barrier = pltpu.get_barrier_semaphore()
    for up, down in sides.values():
        for device in (up, down):
            pl.semaphore_signal(barrier, inc=1, device_id=device, device_id_type=MESH)

    planes_x, planes_y = spaces[12], spaces[6]

    def gather_x(j, carry):
        for c in range(5):
            planes_x[c, j + 3] = q[c, pl.ds(pl.multiple_of(32 * j, 32), 32), :] * SCALE
        return carry

    lax.fori_loop(0, 16, gather_x, 0)

    def gather_y(j, carry):
        for c in range(5):
            for h in range(2):
                planes_y[c, j + 3, pl.ds(8 * h, 8), :] = (
                    q[c, pl.ds(j + 256 * h, 8, stride=32), :] * SCALE
                )
        return carry

    lax.fori_loop(0, 32, gather_y, 0)
    pl.semaphore_wait(barrier, 6)
    slots = iter(range(12))

    def move(src, dst, device):
        k = next(slots)
        copy = pltpu.make_async_remote_copy(
            src_ref=src,
            dst_ref=dst,
            send_sem=send.at[k],
            recv_sem=recv.at[k],
            device_id=device,
            device_id_type=MESH,
        )
        copy.start()
        return copy

    along_y = [
        move(planes_y.at[:, pl.ds(32, 3)], planes_y.at[:, pl.ds(0, 3)], sides["gy"][0]),
        move(planes_y.at[:, pl.ds(3, 3)], planes_y.at[:, pl.ds(35, 3)], sides["gy"][1]),
    ]
    along_x = [
        move(planes_x.at[:, pl.ds(16, 3)], planes_x.at[:, pl.ds(0, 3)], sides["gx"][0]),
        move(planes_x.at[:, pl.ds(3, 3)], planes_x.at[:, pl.ds(19, 3)], sides["gx"][1]),
    ]
    z_turn(q, turned)
    along_z = []
    for blk in range(4):
        low, high = turned.at[:, pl.ds(160 * blk, 8)], turned.at[:, pl.ds(160 * blk + 152, 8)]
        first, last = turned.at[:, pl.ds(160 * blk + 8, 8)], turned.at[:, pl.ds(160 * blk + 144, 8)]
        along_z.append(move(last, low, sides["gz"][0]))
        along_z.append(move(first, high, sides["gz"][1]))
    for copy in along_z:
        copy.wait_recv()
    z_part(coefs[2], add, turned, *spaces[0:6], diff)
    for copy in along_y:
        copy.wait_recv()
    y_part(coefs[1], add, *spaces[6:12], diff)
    for copy in along_x:
        copy.wait_recv()
    x_part(coefs[0], add, out, *spaces[12:18])
    for copy in along_x + along_y + along_z:
        copy.wait_send()


def sweep_scratch(cells, rows):
    f32 = jnp.float32
    steps = -(-(cells + 5) // 3) * 3
    return [
        pltpu.VMEM((5, steps + 1, rows, 128), f32),
        pltpu.VMEM((5, steps, rows, 128), f32),
        pltpu.VMEM((5, steps, rows, 128), f32),
        pltpu.VMEM((5, steps, rows, 128), f32),
        pltpu.VMEM((steps, rows, 128), f32),
        pltpu.VMEM((5, cells + 1, rows, 128), f32),
    ]


def flow_change(section, counts, step_size):
    f32 = jnp.float32
    coefs = [0.25 * step_size * n / (2.0 * SCALE) for n in counts]
    return pl.pallas_call(
        functools.partial(flow_kernel, coefs),
        out_shape=jax.ShapeDtypeStruct((5, 512, 128), f32),
        in_specs=[pl.BlockSpec(memory_space=pltpu.VMEM)],
        scratch_shapes=[pltpu.VMEM((5, 640, 128), f32)]
        + [pltpu.VMEM((5, 512, 128), f32)] * 2
        + [pltpu.SemaphoreType.DMA((12,)), pltpu.SemaphoreType.DMA((12,))]
        + sweep_scratch(64, 8)
        + sweep_scratch(32, 16)
        + sweep_scratch(16, 32),
        compiler_params=pltpu.CompilerParams(
            vmem_limit_bytes=63 * 2**20, collective_id=0, has_side_effects=True
        ),
        cost_estimate=pl.CostEstimate(flops=100_000_000, bytes_accessed=6_000_000, transcendentals=0),
        name="flow",
    )(section)


def dft_table(sample_count, freq_count):
    times = np.arange(sample_count)[None, :]
    orders = np.arange(1, freq_count + 1)[:, None]
    phases = 2.0 * math.pi / sample_count * (times * orders % sample_count)
    scaling = 1.0 / math.sqrt(sample_count)
    table = np.concatenate([np.cos(phases), -np.sin(phases)], axis=0).astype(np.float32) * scaling
    return jnp.asarray(table.astype(np.float32).astype(jnp.bfloat16))


def sin_cos(turns):
    rest = turns - jnp.round(turns)
    half = rest * rest
    s = (3.1996934769709044, -14.868610848632139, 42.01616577638672, -76.70155116950977,
         81.60502462208919, -41.341697068940945, 6.283185307179586)
    c = (6.529609897637814, -25.96831291454545, 60.167831622681774, -85.45016553628534,
         64.93911898307624, -19.73920453207708, 1.0)
    sine = jnp.full_like(half, s[0])
    for k in s[1:]:
        sine = sine * half + k
    cosine = jnp.full_like(half, c[0])
    for k in c[1:]:
        cosine = cosine * half + k
    return sine * rest, cosine


OBS_CHUNK = 256


def in_pieces(values):
    pieces = []
    for _ in range(3):
        piece = values.astype(jnp.bfloat16).astype(jnp.float32)
        pieces.append(piece)
        values = values - piece
    return pieces


PAIRS = ((0, 0), (0, 1), (1, 0), (0, 2), (1, 1), (2, 0))


GROUP = 4
GROUPS = 8
PAIR = 2


def panel_kernel(
    counts, live, change, old, section, record, cells, angles, ears, ranges, table,
    out, updated, state, olds, sections, records, pieces, heard, shown, spectra, sems,
):
    groups = (live[0] + GROUP - 1) // GROUP
    origin = [lax.axis_index(a) * n for a, n in zip(("gx", "gy", "gz"), (16, 32, 128))]

    def fetch(g):
        return pltpu.make_async_copy(
            record.at[pl.ds(128 * GROUP * g, 128 * GROUP)], records.at[g], sems.at[g]
        )

    def bring(first, count, sem):
        rows = pl.ds(first, count)
        return [
            pltpu.make_async_copy(change.at[rows], state.at[rows], sems.at[sem]),
            pltpu.make_async_copy(old.at[rows], olds.at[rows], sems.at[sem + 1]),
            pltpu.make_async_copy(section.at[rows], sections.at[rows], sems.at[sem + 2]),
        ]

    def finish(c):
        state[c] = (0.75 * olds[c] + 0.25 * sections[c]) - state[c]

    density_in, rest_in = bring(0, 1, GROUPS), bring(1, 4, GROUPS + 3)
    density_out = pltpu.make_async_copy(state.at[0], updated.at[0], sems.at[GROUPS + 6])
    rest_out = pltpu.make_async_copy(
        state.at[pl.ds(1, 4)], updated.at[pl.ds(1, 4)], sems.at[GROUPS + 7]
    )
    for copy in density_in:
        copy.start()
    for g in range(GROUPS):
        pl.when(g < groups)(fetch(g).start)
    for copy in rest_in:
        copy.start()

    out[...] = jnp.zeros_like(out)
    place = lax.broadcasted_iota(jnp.int32, (8, 128), 0)
    half_turn = 0.5 / math.pi

    def tile(*rows):
        made = jnp.where(place == 0, rows[0], 0.0)
        for k, row in enumerate(rows[1:], 1):
            made = jnp.where(place == k, row, made)
        return made

    def direction(sine, cosine):
        return cosine[0:1] * cosine[1:2], cosine[0:1] * sine[1:2], sine[0:1]

    def turned_angles(pair):
        row = lax.broadcasted_iota(jnp.int32, pair.shape, 0)
        return pair * jnp.where(row == 0, 0.5 * half_turn, half_turn)

    for k in range(8):
        lanes = pl.ds(128 * k, 128)
        reach = ranges[:, lanes]
        spot = [reach * d for d in direction(*sin_cos(turned_angles(ears[:, lanes])))]
        far = (spot[0] * spot[0] + spot[1] * spot[1]) + spot[2] * spot[2]
        split = in_pieces(tile(*spot, jnp.ones_like(far), far))
        heard[:, lanes] = jnp.concatenate([split[t] for _, t in PAIRS], axis=0).astype(jnp.bfloat16)
        shown[:, lanes] = tile(*spot)

    for copy in density_in:
        copy.wait()
    finish(0)
    turned = jnp.concatenate(
        [jnp.transpose(state[0, pl.ds(128 * k, 128), :]) for k in range(4)], axis=1
    )
    for k, piece in enumerate(in_pieces(turned)):
        pieces[pl.ds(128 * k, 128), :] = piece.astype(jnp.bfloat16)
    density_out.start()

    def front(g, carry):
        cell = cells[g]
        grid_row = lax.broadcasted_iota(jnp.int32, (512, 128 * GROUP), 0)
        chosen = jnp.where(grid_row == cell // 128, 1.0, 0.0).astype(jnp.bfloat16)
        found = jnp.dot(pieces[...], chosen, preferred_element_type=jnp.float32)
        found = (found[:128] + found[128:256]) + found[256:]
        lane = lax.broadcasted_iota(jnp.int32, (128, 128 * GROUP), 0)
        sampled = jnp.sum(jnp.where(lane == cell % 128, found, 0.0), axis=0, keepdims=True)
        column = jnp.transpose(jnp.broadcast_to(sampled, (8, 128 * GROUP)))[:, 0:1]
        fetch(g).wait()
        sources = (records[g].astype(jnp.float32) * column).astype(jnp.bfloat16)
        made = lax.dot_general(
            table[...], sources, (((1,), (1,)), ((), ())), preferred_element_type=jnp.float32
        ).astype(jnp.bfloat16)
        for k in range(GROUP):
            spectra[GROUP * g + k] = made[:, 128 * k : 128 * (k + 1)]
        return carry

    lax.fori_loop(0, groups, front, 0)

    for copy in rest_in:
        copy.wait()
    for c in range(1, 5):
        finish(c)
    rest_out.start()
    order = (place + 1).astype(jnp.float32)

    def features(b, alive):
        cell = cells[b // GROUP, :, pl.ds(pl.multiple_of(128 * lax.rem(b, GROUP), 128), 128)]
        along = (cell >> 12, (cell >> 7) & 31, cell & 127)
        spot = [
            ((origin[d] + along[d]).astype(jnp.float32) + 0.5) * (1.0 / counts[d]) - 0.5
            for d in range(3)
        ]
        lanes = pl.ds(pl.multiple_of(128 * b, 128), 128)
        normal = direction(*sin_cos(turned_angles(angles[:, lanes])))
        normal = [n * (alive * (0.25 / math.pi)) for n in normal]
        across = -((normal[0] * spot[0] + normal[1] * spot[1]) + normal[2] * spot[2])
        square = (spot[0] * spot[0] + spot[1] * spot[1]) + spot[2] * spot[2]
        twice = [-2.0 * p for p in spot]
        facing = in_pieces(tile(*normal, across))
        apart = in_pieces(tile(*twice, square, jnp.ones_like(square)))
        seen = jnp.concatenate(
            [jnp.concatenate([facing[s], apart[s]], axis=1) for s, _ in PAIRS], axis=0
        ).astype(jnp.bfloat16)
        return seen, jnp.sum(tile(*twice), axis=1, keepdims=True)

    def turns_of(centre, first):
        apart = shown[:, pl.ds(first, 128)] + centre * (1.0 / 256.0)
        square = jnp.sum(apart * apart, axis=0, keepdims=True)
        return square * lax.rsqrt(square) * (WAVE_STEP * half_turn)

    def weights_of(seen, o):
        both = lax.dot_general(
            seen,
            heard[:, OBS_CHUNK * o : OBS_CHUNK * (o + 1)],
            (((0,), (0,)), ((), ())),
            preferred_element_type=jnp.float32,
        )
        return (both[:128] / both[128:]).astype(jnp.bfloat16)

    def add_turned(centre, o, product):
        for h in range(OBS_CHUNK // 128):
            lanes = slice(128 * h, 128 * h + 128)
            base = turns_of(centre, OBS_CHUNK * o + 128 * h)
            sine, cosine = sin_cos(base * order)
            step_s = jnp.broadcast_to(sine[7:8], (8, 128))
            step_c = jnp.broadcast_to(cosine[7:8], (8, 128))
            before_s = sine * step_c - cosine * step_s
            before_c = cosine * step_c + sine * step_s
            twice = step_c + step_c
            for a in range(FREQS // 8):
                re = product[8 * a : 8 * a + 8, lanes]
                im = product[FREQS + 8 * a : FREQS + 8 * a + 8, lanes]
                out[o, 0, 2 * a + h] += re * cosine + im * sine
                out[o, 1, 2 * a + h] += im * cosine - re * sine
                if a + 1 < FREQS // 8:
                    sine, before_s = twice * sine - before_s, sine
                    cosine, before_c = twice * cosine - before_c, cosine

    def back(pair, carry):
        blocks = []
        for k in range(PAIR):
            b = PAIR * pair + k
            alive = jnp.where(b < live[0], 1.0, 0.0)
            blocks.append((*features(b, alive), spectra[b]))
        for o in range(1024 // OBS_CHUNK):
            for seen, centre, spectrum in blocks:
                product = jnp.dot(
                    spectrum, weights_of(seen, o), preferred_element_type=jnp.float32
                )
                add_turned(centre, o, product)
        return carry

    lax.fori_loop(0, (live[0] + PAIR - 1) // PAIR, back, 0)
    density_out.wait()
    rest_out.wait()


def panel_sums(counts, live_count, change, old, section, record, cells, angles, ears, ranges, table):
    vmem, anywhere = pl.BlockSpec(memory_space=pltpu.VMEM), pl.BlockSpec(memory_space=pl.ANY)
    bf16, f32 = jnp.bfloat16, jnp.float32
    return pl.pallas_call(
        functools.partial(panel_kernel, counts),
        out_shape=(
            jax.ShapeDtypeStruct((1024 // OBS_CHUNK, 2, TILES, 8, 128), f32),
            jax.ShapeDtypeStruct((5, 512, 128), f32),
        ),
        in_specs=[pl.BlockSpec(memory_space=pltpu.SMEM)] + [anywhere] * 4 + [vmem] * 5,
        out_specs=(vmem, anywhere),
        scratch_shapes=[pltpu.VMEM((5, 512, 128), f32)] * 3
        + [
            pltpu.VMEM((GROUPS, 128 * GROUP, 512), bf16),
            pltpu.VMEM((384, 512), bf16),
            pltpu.VMEM((8 * len(PAIRS), 1024), bf16),
            pltpu.VMEM((8, 1024), f32),
            pltpu.VMEM((32, 256, 128), bf16),
            pltpu.SemaphoreType.DMA((GROUPS + 8,)),
        ],
        compiler_params=pltpu.CompilerParams(vmem_limit_bytes=63 * 2**20),
        cost_estimate=pl.CostEstimate(
            flops=4_000_000_000, bytes_accessed=8_000_000, transcendentals=0
        ),
        name="panels",
    )(live_count, change, old, section, record, cells, angles, ears, ranges, table)


def local(
    state_old,
    state_section,
    panel_record,
    panel_cell,
    panel_angles,
    owned_blocks,
    listener_angles,
    listener_range,
):
    cells = state_section.shape[1:]
    counts = tuple(n * lax.axis_size(a) for n, a in zip(cells, ("gx", "gy", "gz")))
    section = state_section.reshape(5, 512, 128)
    change = flow_change(section, counts, COURANT / max(counts))
    part, updated = panel_sums(
        counts,
        owned_blocks,
        change,
        state_old.reshape(5, 512, 128),
        section,
        panel_record,
        panel_cell.reshape(GROUPS, 1, 128 * GROUP),
        panel_angles,
        listener_angles,
        listener_range.reshape(1, -1),
        dft_table(panel_record.shape[1], FREQS),
    )
    return updated.reshape(state_section.shape), summed_spectra(part)


def solution(mesh):
    return jax.shard_map(
        local,
        mesh=mesh,
        in_specs=(
            P(None, "gx", "gy", "gz"),
            P(None, "gx", "gy", "gz"),
            P(("gx", "gy", "gz"), None),
            P(("gx", "gy", "gz"), None),
            P(None, ("gx", "gy", "gz")),
            P(("gx", "gy", "gz")),
            P(),
            P(),
        ),
        out_specs=(P(None, "gx", "gy", "gz"), P(None, "gz", None)),
        check_vma=False,
    )
```

```python
import functools
import math

import jax
import jax.numpy as jnp
import numpy as np
from jax import lax
from jax.experimental import pallas as pl
from jax.experimental.pallas import tpu as pltpu
from jax.sharding import PartitionSpec as P

FREQS = 128
GAMMA_GAS = 4.4
PRESSURE_INF = 1.0
WENO_EPS = 1e-06
WAVE_STEP = 0.25
COURANT = 0.08

SCALE = 4.0
EPS = 0.75 * 4.0 * SCALE * SCALE * WENO_EPS


MESH = pl.DeviceIdType.MESH
TILES = 32


def sum_kernel(part, out, came0, sums, came1, total, came2, mine, full, other, s0, r0, s1, r1, s2, r2, s3, r3, s4, r4):
    gx, gy, gz = (lax.axis_index(a) for a in ("gx", "gy", "gz"))
    core, upper = lax.rem(gy, 2), gy // 2
    m = gx * 2 + upper
    partner = {"gx": gx, "gy": upper * 2 + (1 - core), "gz": gz}

    def along(k):
        return {"gx": gx, "gy": gy, "gz": lax.rem(gz + k, 4)}

    def chip(r):
        t = lax.rem(m + r, TILES)
        return t, {"gx": t // 2, "gy": lax.rem(t, 2) * 2 + core, "gz": gz}

    barrier = pltpu.get_barrier_semaphore()

    def greet(device):
        pl.semaphore_signal(barrier, inc=1, device_id=device, device_id_type=MESH)

    greet(partner)
    for k in (1, 2, 3):
        greet(along(k))

    def greet_chip(r, carry):
        greet(chip(r)[1])
        return carry

    lax.fori_loop(1, TILES, greet_chip, 0)
    pl.semaphore_wait(barrier, TILES + 3)

    def remote(src, dst, send, recv, device):
        return pltpu.make_async_remote_copy(
            src_ref=src, dst_ref=dst, send_sem=send, recv_sem=recv, device_id=device, device_id_type=MESH
        )

    shares, along_gz = {}, {}
    for k in (2, 1, 3, 0):
        shares[k] = remote(
            part.at[lax.rem(gz + k, 4), 1 - core], came0.at[k], s0.at[k], r0.at[k], partner
        )
        shares[k].start()
    for k in (2, 1, 3, 0):
        shares[k].wait_recv()
        sums[k] = part[lax.rem(gz + k, 4), core] + came0[k]
        if k > 0:
            along_gz[k] = remote(sums.at[k], came1.at[k - 1], s1.at[k - 1], r1.at[k - 1], along(k))
            along_gz[k].start()
    for k in (1, 3, 2):
        along_gz[k].wait_recv()
    total[...] = (sums[0] + came1[0]) + (came1[1] + came1[2])

    def scatter(r, carry):
        t, device = chip(r)
        remote(total.at[t], came2.at[r - 1], s2, r2, device).start()
        return carry

    lax.fori_loop(1, TILES, scatter, 0)
    pltpu.make_async_copy(came2, came2, r2).wait()
    own = total[m]
    for r in range(TILES - 1):
        own = own + came2[r]
    mine[...] = own
    full[m] = own

    def gather(r, carry):
        remote(mine, full.at[m], s3, r3, chip(r)[1]).start()
        return carry

    lax.fori_loop(1, TILES, gather, 0)
    pltpu.make_async_copy(came2, came2, r3).wait()
    swap = remote(full, other, s4, r4, partner)
    swap.start()

    def lay(which, tiles):
        for h in range(2):
            block = jnp.concatenate([tiles[2 * a + h] for a in range(16)], axis=0)
            out[which, pl.ds(128 * h, 128), :] = jnp.transpose(block)

    lay(core, full)
    swap.wait_recv()
    lay(1 - core, other)
    for k in (0, 1, 2, 3):
        shares[k].wait_send()
        if k > 0:
            along_gz[k].wait_send()
    pltpu.make_async_copy(came2, came2, s2).wait()
    pltpu.make_async_copy(came2, came2, s3).wait()
    swap.wait_send()


def summed_spectra(part):
    vmem = pl.BlockSpec(memory_space=pltpu.VMEM)
    f32 = jnp.float32
    tiles = (TILES, 8, 128)
    dma = pltpu.SemaphoreType.DMA
    return pl.pallas_call(
        sum_kernel,
        out_shape=jax.ShapeDtypeStruct((2, 256, FREQS), f32),
        in_specs=[vmem],
        out_specs=vmem,
        scratch_shapes=[
            pltpu.VMEM((4, *tiles), f32),
            pltpu.VMEM((4, *tiles), f32),
            pltpu.VMEM((3, *tiles), f32),
            pltpu.VMEM(tiles, f32),
            pltpu.VMEM((TILES - 1, 8, 128), f32),
            pltpu.VMEM((8, 128), f32),
            pltpu.VMEM(tiles, f32),
            pltpu.VMEM(tiles, f32),
            dma((4,)),
            dma((4,)),
            dma((3,)),
            dma((3,)),
            dma,
            dma,
            dma,
            dma,
            dma,
            dma,
        ],
        compiler_params=pltpu.CompilerParams(
            vmem_limit_bytes=63 * 2**20, collective_id=1, has_side_effects=True
        ),
        name="sum_spectra",
    )(part)


def flux_of(state, axis_d):
    density, energy = state[0], state[4]
    momenta = state[1:4]
    inverse = 1.0 / density
    velocity = [m * inverse for m in momenta]
    kinetic = 0.5 * (momenta[0] * velocity[0] + momenta[1] * velocity[1] + momenta[2] * velocity[2])
    pressure = (GAMMA_GAS - 1.0) * (energy - kinetic) - GAMMA_GAS * PRESSURE_INF * SCALE
    normal = velocity[axis_d]
    square = GAMMA_GAS * (pressure + PRESSURE_INF * SCALE) * inverse
    sound = square * lax.rsqrt(square)
    rows = [momenta[axis_d]]
    for component in range(3):
        carried = momenta[component] * normal
        rows.append(carried + pressure if component == axis_d else carried)
    rows.append((energy + pressure) * normal)
    return rows, jnp.abs(normal) + sound


def weno_terms(e0, e1, e2, d1, d2):
    q1, q2 = 0.75 * d1, 0.75 * d2
    base1 = d1 * q1 + EPS
    base2 = d2 * q2 + EPS
    t0 = e0 * (e0 + q1) + base1
    t1 = e1 * (e1 + q1) + base1
    t2 = e2 * (e2 - q2) + base2
    p01, p02, p12 = t0 * t1, t0 * t2, t1 * t2
    wa = p12 * p12
    wb = 6.0 * (p02 * p02)
    wc = 1.5 * (p01 * p01)
    return wa * (e0 - e1) + wc * (e1 - e2), (wa + wb) + (wc + wc)


def face_value(alpha, df, dq, fsum):
    aq = [alpha * v for v in dq]
    up = [df[j] + aq[j] for j in range(4)]
    dn = [None] + [df[j] - aq[j] for j in range(1, 5)]
    num_p, den_p = weno_terms(up[1] - up[0], up[2] - up[1], up[3] - up[2], up[1], up[2])
    num_m, den_m = weno_terms(dn[4] - dn[3], dn[3] - dn[2], dn[2] - dn[1], -dn[3], -dn[2])
    ratio = (num_p * den_m + num_m * den_p) / (den_p * den_m)
    return fsum + ((0.5 * (up[1] - dn[3]) - aq[2]) + ratio) * (1.0 / 3.0)


def differences(planes, dq, df, fs, m2, axis_d, group, length, unroll):
    def load(r, j):
        return [planes[c, j, pl.ds(8 * r, 8), :] for c in range(5)]

    def step(k, carry):
        for u in range(unroll):
            after = []
            for (r, start), (state, flux, speed) in zip(group, carry):
                j, rows = start + unroll * k + u, pl.ds(8 * r, 8)
                next_state = load(r, j + 1)
                next_flux, next_speed = flux_of(next_state, axis_d)
                for c in range(5):
                    dq[c, j, rows, :] = next_state[c] - state[c]
                    df[c, j, rows, :] = next_flux[c] - flux[c]
                    fs[c, j, rows, :] = next_flux[c] + flux[c]
                m2[j, rows, :] = jnp.maximum(next_speed, speed)
                after.append((next_state, next_flux, next_speed))
            carry = after
        return carry

    begin = []
    for r, start in group:
        state = load(r, start)
        begin.append((state, *flux_of(state, axis_d)))
    lax.fori_loop(0, length, step, begin)


def face_fluxes(dq, df, fs, m2, faces, chunks, count, which):
    def face(k, carry):
        i = which(k)
        for r in range(chunks):
            rows = pl.ds(8 * r, 8)
            alpha = jnp.maximum(jnp.maximum(m2[i, rows, :], m2[i + 2, rows, :]), m2[i + 4, rows, :])
            for c in range(5):
                faces[c, i, rows, :] = face_value(
                    alpha,
                    [df[c, i + j, rows, :] for j in range(5)],
                    [dq[c, i + j, rows, :] for j in range(5)],
                    fs[c, i + 2, rows, :],
                )
        return carry

    lax.fori_loop(0, count, face, 0)


def z_turn(q, turned):
    for c in range(5):
        for blk in range(4):
            tile = jnp.transpose(q[c, pl.ds(128 * blk, 128), :]) * SCALE
            turned[c, pl.ds(160 * blk + 8, 72), :] = tile[:72]
            turned[c, pl.ds(160 * blk + 80, 72), :] = tile[56:]


def z_part(coef, out, turned, planes, dq, df, fs, m2, faces, diff):
    def gather(j, carry):
        for c in range(5):
            planes[c, j] = turned[c, pl.ds(j + 5, 8, stride=80), :]
        return carry

    lax.fori_loop(0, 70, gather, 0, unroll=2)
    differences(planes, dq, df, fs, m2, 2, ((0, 0), (0, 33)), 12, 3)
    face_fluxes(dq, df, fs, m2, faces, 1, 65, lambda k: k)

    def difference(i, carry):
        for c in range(5):
            diff[c, pl.ds(pl.multiple_of(8 * i, 8), 8), :] = coef * (faces[c, i + 1] - faces[c, i])
        return carry

    lax.fori_loop(0, 64, difference, 0, unroll=2)
    for c in range(5):
        for blk in range(4):
            tile = jnp.concatenate(
                [diff[c, pl.ds(2 * blk + half, 64, stride=8), :] for half in range(2)], axis=0
            )
            out[c, pl.ds(128 * blk, 128), :] = jnp.transpose(tile)


def y_inner(planes, dq, df, fs, m2, faces):
    both = ((0, 3), (1, 3))
    differences(planes, dq, df, fs, m2, 1, both, 10, 3)
    differences(planes, dq, df, fs, m2, 1, ((0, 33), (1, 33)), 1, 1)
    face_fluxes(dq, df, fs, m2, faces, 2, 27, lambda k: k + 3)


def y_part(coef, out, planes, dq, df, fs, m2, faces, diff):
    differences(planes, dq, df, fs, m2, 1, ((0, 0), (1, 0)), 1, 3)
    differences(planes, dq, df, fs, m2, 1, ((0, 34), (1, 34)), 1, 3)
    face_fluxes(dq, df, fs, m2, faces, 2, 6, lambda k: k + 27 * (k // 3))

    def difference(i, carry):
        for c in range(5):
            diff[c, pl.ds(pl.multiple_of(16 * i, 16), 16), :] = coef * (
                faces[c, i + 1] - faces[c, i]
            )
        return carry

    lax.fori_loop(0, 32, difference, 0)

    def back(x, carry):
        for c in range(5):
            for y8 in range(4):
                rows = pl.ds(pl.multiple_of(32 * x + 8 * y8, 8), 8)
                out[c, rows, :] += diff[c, pl.ds(128 * y8 + x, 8, stride=16), :]
        return carry

    lax.fori_loop(0, 16, back, 0)


def x_inner(planes, dq, df, fs, m2, faces):
    differences(planes, dq, df, fs, m2, 0, ((0, 3), (1, 3)), 5, 3)
    differences(planes, dq, df, fs, m2, 0, ((2, 3), (3, 3)), 5, 3)
    face_fluxes(dq, df, fs, m2, faces, 4, 11, lambda k: k + 3)


def x_part(coef, add, out, planes, dq, df, fs, m2, faces):
    for start in (0, 18):
        differences(planes, dq, df, fs, m2, 0, ((0, start), (1, start)), 1, 3)
        differences(planes, dq, df, fs, m2, 0, ((2, start), (3, start)), 1, 3)
    face_fluxes(dq, df, fs, m2, faces, 4, 6, lambda k: k + 11 * (k // 3))

    def finish(i, carry):
        rows = pl.ds(pl.multiple_of(32 * i, 32), 32)
        for c in range(5):
            out[c, rows, :] = add[c, rows, :] + coef * (faces[c, i + 1] - faces[c, i])
        return carry

    lax.fori_loop(0, 16, finish, 0)


def flow_kernel(coefs, q, out, turned, diff, add, send, recv, *spaces):
    here = {a: lax.axis_index(a) for a in ("gx", "gy", "gz")}

    def beside(axis, step):
        return {**here, axis: lax.rem(here[axis] + step, lax.axis_size(axis))}

    sides = {a: (beside(a, 1), beside(a, lax.axis_size(a) - 1)) for a in here}
    barrier = pltpu.get_barrier_semaphore()
    for up, down in sides.values():
        for device in (up, down):
            pl.semaphore_signal(barrier, inc=1, device_id=device, device_id_type=MESH)

    planes_x, planes_y = spaces[12], spaces[6]

    def gather_x(j, carry):
        for c in range(5):
            planes_x[c, j + 3] = q[c, pl.ds(pl.multiple_of(32 * j, 32), 32), :] * SCALE
        return carry

    lax.fori_loop(0, 16, gather_x, 0)

    def gather_y(j, carry):
        for c in range(5):
            for h in range(2):
                planes_y[c, j + 3, pl.ds(8 * h, 8), :] = (
                    q[c, pl.ds(j + 256 * h, 8, stride=32), :] * SCALE
                )
        return carry

    lax.fori_loop(0, 32, gather_y, 0)
    pl.semaphore_wait(barrier, 6)
    slots = iter(range(12))

    def move(src, dst, device):
        k = next(slots)
        copy = pltpu.make_async_remote_copy(
            src_ref=src,
            dst_ref=dst,
            send_sem=send.at[k],
            recv_sem=recv.at[k],
            device_id=device,
            device_id_type=MESH,
        )
        copy.start()
        return copy

    along_y = [
        move(planes_y.at[:, pl.ds(32, 3)], planes_y.at[:, pl.ds(0, 3)], sides["gy"][0]),
        move(planes_y.at[:, pl.ds(3, 3)], planes_y.at[:, pl.ds(35, 3)], sides["gy"][1]),
    ]
    along_x = [
        move(planes_x.at[:, pl.ds(16, 3)], planes_x.at[:, pl.ds(0, 3)], sides["gx"][0]),
        move(planes_x.at[:, pl.ds(3, 3)], planes_x.at[:, pl.ds(19, 3)], sides["gx"][1]),
    ]
    z_turn(q, turned)
    along_z = []
    for blk in range(4):
        low, high = turned.at[:, pl.ds(160 * blk, 8)], turned.at[:, pl.ds(160 * blk + 152, 8)]
        first, last = turned.at[:, pl.ds(160 * blk + 8, 8)], turned.at[:, pl.ds(160 * blk + 144, 8)]
        along_z.append(move(last, low, sides["gz"][0]))
        along_z.append(move(first, high, sides["gz"][1]))
    y_inner(*spaces[6:12])
    for copy in along_z:
        copy.wait_recv()
    z_part(coefs[2], add, turned, *spaces[0:6], diff)
    x_inner(*spaces[12:18])
    for copy in along_y:
        copy.wait_recv()
    y_part(coefs[1], add, *spaces[6:12], diff)
    for copy in along_x:
        copy.wait_recv()
    x_part(coefs[0], add, out, *spaces[12:18])
    for copy in along_x + along_y + along_z:
        copy.wait_send()


def sweep_scratch(cells, rows):
    f32 = jnp.float32
    return [
        pltpu.VMEM((5, cells + 6, rows, 128), f32),
        pltpu.VMEM((5, cells + 5, rows, 128), f32),
        pltpu.VMEM((5, cells + 5, rows, 128), f32),
        pltpu.VMEM((5, cells + 5, rows, 128), f32),
        pltpu.VMEM((cells + 5, rows, 128), f32),
        pltpu.VMEM((5, cells + 1, rows, 128), f32),
    ]


def flow_change(section, counts, step_size):
    f32 = jnp.float32
    coefs = [0.25 * step_size * n / (2.0 * SCALE) for n in counts]
    return pl.pallas_call(
        functools.partial(flow_kernel, coefs),
        out_shape=jax.ShapeDtypeStruct((5, 512, 128), f32),
        in_specs=[pl.BlockSpec(memory_space=pltpu.VMEM)],
        scratch_shapes=[pltpu.VMEM((5, 640, 128), f32)]
        + [pltpu.VMEM((5, 512, 128), f32)] * 2
        + [pltpu.SemaphoreType.DMA((12,)), pltpu.SemaphoreType.DMA((12,))]
        + sweep_scratch(64, 8)
        + sweep_scratch(32, 16)
        + sweep_scratch(16, 32),
        compiler_params=pltpu.CompilerParams(
            vmem_limit_bytes=63 * 2**20, collective_id=0, has_side_effects=True
        ),
        cost_estimate=pl.CostEstimate(flops=100_000_000, bytes_accessed=6_000_000, transcendentals=0),
        name="flow",
    )(section)


def dft_table(sample_count, freq_count):
    times = np.arange(sample_count)[None, :]
    orders = np.arange(1, freq_count + 1)[:, None]
    phases = 2.0 * math.pi / sample_count * (times * orders % sample_count)
    scaling = 1.0 / math.sqrt(sample_count)
    table = np.concatenate([np.cos(phases), -np.sin(phases)], axis=0).astype(np.float32) * scaling
    return jnp.asarray(table.astype(np.float32).astype(jnp.bfloat16))


def sin_cos(turns):
    rest = turns - jnp.round(turns)
    half = rest * rest
    s = (3.1996934769709044, -14.868610848632139, 42.01616577638672, -76.70155116950977,
         81.60502462208919, -41.341697068940945, 6.283185307179586)
    c = (6.529609897637814, -25.96831291454545, 60.167831622681774, -85.45016553628534,
         64.93911898307624, -19.73920453207708, 1.0)
    sine = jnp.full_like(half, s[0])
    for k in s[1:]:
        sine = sine * half + k
    cosine = jnp.full_like(half, c[0])
    for k in c[1:]:
        cosine = cosine * half + k
    return sine * rest, cosine


OBS_CHUNK = 256


def in_pieces(values):
    pieces = []
    for _ in range(3):
        piece = values.astype(jnp.bfloat16).astype(jnp.float32)
        pieces.append(piece)
        values = values - piece
    return pieces


PAIRS = ((0, 0), (0, 1), (1, 0), (0, 2), (1, 1), (2, 0))


GROUP = 4
GROUPS = 8
PAIR = 2


def panel_kernel(
    counts, live, change, old, section, record, cells, angles, ears, ranges, table,
    out, updated, state, olds, sections, records, pieces, heard, shown, spectra, sems,
):
    groups = (live[0] + GROUP - 1) // GROUP
    origin = [lax.axis_index(a) * n for a, n in zip(("gx", "gy", "gz"), (16, 32, 128))]

    def fetch(g):
        return pltpu.make_async_copy(
            record.at[pl.ds(128 * GROUP * g, 128 * GROUP)], records.at[g], sems.at[g]
        )

    def bring(first, count, sem):
        rows = pl.ds(first, count)
        return [
            pltpu.make_async_copy(change.at[rows], state.at[rows], sems.at[sem]),
            pltpu.make_async_copy(old.at[rows], olds.at[rows], sems.at[sem + 1]),
            pltpu.make_async_copy(section.at[rows], sections.at[rows], sems.at[sem + 2]),
        ]

    def finish(c):
        state[c] = (0.75 * olds[c] + 0.25 * sections[c]) - state[c]

    density_in, rest_in = bring(0, 1, GROUPS), bring(1, 4, GROUPS + 3)
    density_out = pltpu.make_async_copy(state.at[0], updated.at[0], sems.at[GROUPS + 6])
    rest_out = pltpu.make_async_copy(
        state.at[pl.ds(1, 4)], updated.at[pl.ds(1, 4)], sems.at[GROUPS + 7]
    )
    for copy in density_in:
        copy.start()
    for g in range(GROUPS):
        pl.when(g < groups)(fetch(g).start)
    for copy in rest_in:
        copy.start()

    out[...] = jnp.zeros_like(out)
    place = lax.broadcasted_iota(jnp.int32, (8, 128), 0)
    half_turn = 0.5 / math.pi

    def tile(*rows):
        made = jnp.where(place == 0, rows[0], 0.0)
        for k, row in enumerate(rows[1:], 1):
            made = jnp.where(place == k, row, made)
        return made

    def direction(sine, cosine):
        return cosine[0:1] * cosine[1:2], cosine[0:1] * sine[1:2], sine[0:1]

    def turned_angles(pair):
        row = lax.broadcasted_iota(jnp.int32, pair.shape, 0)
        return pair * jnp.where(row == 0, 0.5 * half_turn, half_turn)

    for k in range(8):
        lanes = pl.ds(128 * k, 128)
        reach = ranges[:, lanes]
        spot = [reach * d for d in direction(*sin_cos(turned_angles(ears[:, lanes])))]
        far = (spot[0] * spot[0] + spot[1] * spot[1]) + spot[2] * spot[2]
        split = in_pieces(tile(*spot, jnp.ones_like(far), far))
        heard[:, lanes] = jnp.concatenate([split[t] for _, t in PAIRS], axis=0).astype(jnp.bfloat16)
        shown[:, lanes] = tile(*spot)

    for copy in density_in:
        copy.wait()
    finish(0)
    turned = jnp.concatenate(
        [jnp.transpose(state[0, pl.ds(128 * k, 128), :]) for k in range(4)], axis=1
    )
    for k, piece in enumerate(in_pieces(turned)):
        pieces[pl.ds(128 * k, 128), :] = piece.astype(jnp.bfloat16)
    density_out.start()

    def front(g, carry):
        cell = cells[g]
        grid_row = lax.broadcasted_iota(jnp.int32, (512, 128 * GROUP), 0)
        chosen = jnp.where(grid_row == cell // 128, 1.0, 0.0).astype(jnp.bfloat16)
        found = jnp.dot(pieces[...], chosen, preferred_element_type=jnp.float32)
        found = (found[:128] + found[128:256]) + found[256:]
        lane = lax.broadcasted_iota(jnp.int32, (128, 128 * GROUP), 0)
        sampled = jnp.sum(jnp.where(lane == cell % 128, found, 0.0), axis=0, keepdims=True)
        column = jnp.transpose(jnp.broadcast_to(sampled, (8, 128 * GROUP)))[:, 0:1]
        fetch(g).wait()
        sources = (records[g].astype(jnp.float32) * column).astype(jnp.bfloat16)
        made = lax.dot_general(
            table[...], sources, (((1,), (1,)), ((), ())), preferred_element_type=jnp.float32
        ).astype(jnp.bfloat16)
        for k in range(GROUP):
            spectra[GROUP * g + k] = made[:, 128 * k : 128 * (k + 1)]
        return carry

    lax.fori_loop(0, groups, front, 0)

    for copy in rest_in:
        copy.wait()
    for c in range(1, 5):
        finish(c)
    rest_out.start()
    order = (place + 1).astype(jnp.float32)

    def features(b, alive):
        cell = cells[b // GROUP, :, pl.ds(pl.multiple_of(128 * lax.rem(b, GROUP), 128), 128)]
        along = (cell >> 12, (cell >> 7) & 31, cell & 127)
        spot = [
            ((origin[d] + along[d]).astype(jnp.float32) + 0.5) * (1.0 / counts[d]) - 0.5
            for d in range(3)
        ]
        lanes = pl.ds(pl.multiple_of(128 * b, 128), 128)
        normal = direction(*sin_cos(turned_angles(angles[:, lanes])))
        normal = [n * (alive * (0.25 / math.pi)) for n in normal]
        across = -((normal[0] * spot[0] + normal[1] * spot[1]) + normal[2] * spot[2])
        square = (spot[0] * spot[0] + spot[1] * spot[1]) + spot[2] * spot[2]
        twice = [-2.0 * p for p in spot]
        facing = in_pieces(tile(*normal, across))
        apart = in_pieces(tile(*twice, square, jnp.ones_like(square)))
        seen = jnp.concatenate(
            [jnp.concatenate([facing[s], apart[s]], axis=1) for s, _ in PAIRS], axis=0
        ).astype(jnp.bfloat16)
        return seen, jnp.sum(tile(*twice), axis=1, keepdims=True)

    def turns_of(centre, first):
        apart = shown[:, pl.ds(first, 128)] + centre * (1.0 / 256.0)
        square = jnp.sum(apart * apart, axis=0, keepdims=True)
        return square * lax.rsqrt(square) * (WAVE_STEP * half_turn)

    def weights_of(seen, o):
        both = lax.dot_general(
            seen,
            heard[:, OBS_CHUNK * o : OBS_CHUNK * (o + 1)],
            (((0,), (0,)), ((), ())),
            preferred_element_type=jnp.float32,
        )
        return (both[:128] / both[128:]).astype(jnp.bfloat16)

    def add_turned(centre, o, product):
        for h in range(OBS_CHUNK // 128):
            lanes = slice(128 * h, 128 * h + 128)
            base = turns_of(centre, OBS_CHUNK * o + 128 * h)
            sine, cosine = sin_cos(base * order)
            step_s = jnp.broadcast_to(sine[7:8], (8, 128))
            step_c = jnp.broadcast_to(cosine[7:8], (8, 128))
            before_s = sine * step_c - cosine * step_s
            before_c = cosine * step_c + sine * step_s
            twice = step_c + step_c
            for a in range(FREQS // 8):
                re = product[8 * a : 8 * a + 8, lanes]
                im = product[FREQS + 8 * a : FREQS + 8 * a + 8, lanes]
                out[o, 0, 2 * a + h] += re * cosine + im * sine
                out[o, 1, 2 * a + h] += im * cosine - re * sine
                if a + 1 < FREQS // 8:
                    sine, before_s = twice * sine - before_s, sine
                    cosine, before_c = twice * cosine - before_c, cosine

    def back(pair, carry):
        blocks = []
        for k in range(PAIR):
            b = PAIR * pair + k
            alive = jnp.where(b < live[0], 1.0, 0.0)
            blocks.append((*features(b, alive), spectra[b]))
        for o in range(1024 // OBS_CHUNK):
            for seen, centre, spectrum in blocks:
                product = jnp.dot(
                    spectrum, weights_of(seen, o), preferred_element_type=jnp.float32
                )
                add_turned(centre, o, product)
        return carry

    lax.fori_loop(0, (live[0] + PAIR - 1) // PAIR, back, 0)
    density_out.wait()
    rest_out.wait()


def panel_sums(counts, live_count, change, old, section, record, cells, angles, ears, ranges, table):
    vmem, anywhere = pl.BlockSpec(memory_space=pltpu.VMEM), pl.BlockSpec(memory_space=pl.ANY)
    bf16, f32 = jnp.bfloat16, jnp.float32
    return pl.pallas_call(
        functools.partial(panel_kernel, counts),
        out_shape=(
            jax.ShapeDtypeStruct((1024 // OBS_CHUNK, 2, TILES, 8, 128), f32),
            jax.ShapeDtypeStruct((5, 512, 128), f32),
        ),
        in_specs=[pl.BlockSpec(memory_space=pltpu.SMEM)] + [anywhere] * 4 + [vmem] * 5,
        out_specs=(vmem, anywhere),
        scratch_shapes=[pltpu.VMEM((5, 512, 128), f32)] * 3
        + [
            pltpu.VMEM((GROUPS, 128 * GROUP, 512), bf16),
            pltpu.VMEM((384, 512), bf16),
            pltpu.VMEM((8 * len(PAIRS), 1024), bf16),
            pltpu.VMEM((8, 1024), f32),
            pltpu.VMEM((32, 256, 128), bf16),
            pltpu.SemaphoreType.DMA((GROUPS + 8,)),
        ],
        compiler_params=pltpu.CompilerParams(vmem_limit_bytes=63 * 2**20),
        cost_estimate=pl.CostEstimate(
            flops=4_000_000_000, bytes_accessed=8_000_000, transcendentals=0
        ),
        name="panels",
    )(live_count, change, old, section, record, cells, angles, ears, ranges, table)


def local(
    state_old,
    state_section,
    panel_record,
    panel_cell,
    panel_angles,
    owned_blocks,
    listener_angles,
    listener_range,
):
    cells = state_section.shape[1:]
    counts = tuple(n * lax.axis_size(a) for n, a in zip(cells, ("gx", "gy", "gz")))
    section = state_section.reshape(5, 512, 128)
    change = flow_change(section, counts, COURANT / max(counts))
    part, updated = panel_sums(
        counts,
        owned_blocks,
        change,
        state_old.reshape(5, 512, 128),
        section,
        panel_record,
        panel_cell.reshape(GROUPS, 1, 128 * GROUP),
        panel_angles,
        listener_angles,
        listener_range.reshape(1, -1),
        dft_table(panel_record.shape[1], FREQS),
    )
    return updated.reshape(state_section.shape), summed_spectra(part)


def solution(mesh):
    return jax.shard_map(
        local,
        mesh=mesh,
        in_specs=(
            P(None, "gx", "gy", "gz"),
            P(None, "gx", "gy", "gz"),
            P(("gx", "gy", "gz"), None),
            P(("gx", "gy", "gz"), None),
            P(None, ("gx", "gy", "gz")),
            P(("gx", "gy", "gz")),
            P(),
            P(),
        ),
        out_specs=(P(None, "gx", "gy", "gz"), P(None, "gz", None)),
        check_vma=False,
    )
```

```python
import functools
import math

import jax
import jax.numpy as jnp
import numpy as np
from jax import lax
from jax.experimental import pallas as pl
from jax.experimental.pallas import tpu as pltpu
from jax.sharding import PartitionSpec as P

FREQS = 128
GAMMA_GAS = 4.4
PRESSURE_INF = 1.0
WENO_EPS = 1e-06
WAVE_STEP = 0.25
COURANT = 0.08

SCALE = 4.0
EPS = 0.75 * 4.0 * SCALE * SCALE * WENO_EPS


MESH = pl.DeviceIdType.MESH
TILES = 32


def sum_kernel(part, out, kept, came0, sums, came1, total, came2, mine, full, other, s0, r0, s1, r1, s2, r2, s3, r3, s4, r4, keep):
    gx, gy, gz = (lax.axis_index(a) for a in ("gx", "gy", "gz"))
    core, upper = lax.rem(gy, 2), gy // 2
    m = gx * 2 + upper
    partner = {"gx": gx, "gy": upper * 2 + (1 - core), "gz": gz}

    def along(k):
        return {"gx": gx, "gy": gy, "gz": lax.rem(gz + k, 4)}

    def chip(r):
        t = lax.rem(m + r, TILES)
        return t, {"gx": t // 2, "gy": lax.rem(t, 2) * 2 + core, "gz": gz}

    keeps = [
        pltpu.make_async_copy(part.at[lax.rem(gz + k, 4), core], kept.at[k], keep.at[k])
        for k in range(4)
    ]
    for copy in keeps:
        copy.start()
    barrier = pltpu.get_barrier_semaphore()

    def greet(device):
        pl.semaphore_signal(barrier, inc=1, device_id=device, device_id_type=MESH)

    greet(partner)
    for k in (1, 2, 3):
        greet(along(k))

    def greet_chip(r, carry):
        greet(chip(r)[1])
        return carry

    lax.fori_loop(1, TILES, greet_chip, 0)
    pl.semaphore_wait(barrier, TILES + 3)

    def remote(src, dst, send, recv, device):
        return pltpu.make_async_remote_copy(
            src_ref=src, dst_ref=dst, send_sem=send, recv_sem=recv, device_id=device, device_id_type=MESH
        )

    shares, along_gz = {}, {}
    for k in (2, 1, 3, 0):
        shares[k] = remote(
            part.at[lax.rem(gz + k, 4), 1 - core], came0.at[k], s0.at[k], r0.at[k], partner
        )
        shares[k].start()
    for k in (2, 1, 3, 0):
        keeps[k].wait()
        shares[k].wait_recv()
        sums[k] = kept[k] + came0[k]
        if k > 0:
            along_gz[k] = remote(sums.at[k], came1.at[k - 1], s1.at[k - 1], r1.at[k - 1], along(k))
            along_gz[k].start()
    for k in (1, 3, 2):
        along_gz[k].wait_recv()
    total[...] = (sums[0] + came1[0]) + (came1[1] + came1[2])

    def scatter(r, carry):
        t, device = chip(r)
        remote(total.at[t], came2.at[r - 1], s2, r2, device).start()
        return carry

    lax.fori_loop(1, TILES, scatter, 0)
    pltpu.make_async_copy(came2, came2, r2).wait()
    own = total[m]
    for r in range(TILES - 1):
        own = own + came2[r]
    mine[...] = own
    full[m] = own

    def gather(r, carry):
        remote(mine, full.at[m], s3, r3, chip(r)[1]).start()
        return carry

    lax.fori_loop(1, TILES, gather, 0)
    pltpu.make_async_copy(came2, came2, r3).wait()
    swap = remote(full, other, s4, r4, partner)
    swap.start()

    def lay(which, tiles):
        for h in range(2):
            for a in range(16):
                out[which, pl.ds(8 * a, 8), pl.ds(128 * h, 128)] = tiles[2 * a + h]

    lay(core, full)
    swap.wait_recv()
    lay(1 - core, other)
    for k in (0, 1, 2, 3):
        shares[k].wait_send()
        if k > 0:
            along_gz[k].wait_send()
    pltpu.make_async_copy(came2, came2, s2).wait()
    pltpu.make_async_copy(came2, came2, s3).wait()
    swap.wait_send()


def summed_spectra(part):
    vmem = pl.BlockSpec(memory_space=pltpu.VMEM)
    f32 = jnp.float32
    tiles = (TILES, 8, 128)
    dma = pltpu.SemaphoreType.DMA
    return pl.pallas_call(
        sum_kernel,
        out_shape=jax.ShapeDtypeStruct((2, FREQS, 256), f32),
        in_specs=[pl.BlockSpec(memory_space=pl.ANY)],
        out_specs=vmem,
        scratch_shapes=[
            pltpu.VMEM((4, *tiles), f32),
            pltpu.VMEM((4, *tiles), f32),
            pltpu.VMEM((4, *tiles), f32),
            pltpu.VMEM((3, *tiles), f32),
            pltpu.VMEM(tiles, f32),
            pltpu.VMEM((TILES - 1, 8, 128), f32),
            pltpu.VMEM((8, 128), f32),
            pltpu.VMEM(tiles, f32),
            pltpu.VMEM(tiles, f32),
            dma((4,)),
            dma((4,)),
            dma((3,)),
            dma((3,)),
            dma,
            dma,
            dma,
            dma,
            dma,
            dma,
            dma((4,)),
        ],
        compiler_params=pltpu.CompilerParams(
            vmem_limit_bytes=63 * 2**20, collective_id=1, has_side_effects=True
        ),
        name="sum_spectra",
    )(part)


def flux_of(state, axis_d):
    density, energy = state[0], state[4]
    momenta = state[1:4]
    inverse = 1.0 / density
    velocity = [m * inverse for m in momenta]
    kinetic = 0.5 * (momenta[0] * velocity[0] + momenta[1] * velocity[1] + momenta[2] * velocity[2])
    pressure = (GAMMA_GAS - 1.0) * (energy - kinetic) - GAMMA_GAS * PRESSURE_INF * SCALE
    normal = velocity[axis_d]
    square = GAMMA_GAS * (pressure + PRESSURE_INF * SCALE) * inverse
    sound = square * lax.rsqrt(square)
    rows = [momenta[axis_d]]
    for component in range(3):
        carried = momenta[component] * normal
        rows.append(carried + pressure if component == axis_d else carried)
    rows.append((energy + pressure) * normal)
    return rows, jnp.abs(normal) + sound


def weno_terms(e0, e1, e2, d1, d2):
    q1, q2 = 0.75 * d1, 0.75 * d2
    base1 = d1 * q1 + EPS
    base2 = d2 * q2 + EPS
    t0 = e0 * (e0 + q1) + base1
    t1 = e1 * (e1 + q1) + base1
    t2 = e2 * (e2 - q2) + base2
    p01, p02, p12 = t0 * t1, t0 * t2, t1 * t2
    wa = p12 * p12
    wb = 6.0 * (p02 * p02)
    wc = 1.5 * (p01 * p01)
    return wa * (e0 - e1) + wc * (e1 - e2), (wa + wb) + (wc + wc)


def face_value(alpha, df, dq, fsum):
    aq = [alpha * v for v in dq]
    up = [df[j] + aq[j] for j in range(4)]
    dn = [None] + [df[j] - aq[j] for j in range(1, 5)]
    num_p, den_p = weno_terms(up[1] - up[0], up[2] - up[1], up[3] - up[2], up[1], up[2])
    num_m, den_m = weno_terms(dn[4] - dn[3], dn[3] - dn[2], dn[2] - dn[1], -dn[3], -dn[2])
    ratio = (num_p * den_m + num_m * den_p) / (den_p * den_m)
    return fsum + ((0.5 * (up[1] - dn[3]) - aq[2]) + ratio) * (1.0 / 3.0)


def differences(planes, dq, df, fs, m2, axis_d, group, length, unroll):
    def load(r, j):
        return [planes[c, j, pl.ds(8 * r, 8), :] for c in range(5)]

    def step(k, carry):
        for u in range(unroll):
            after = []
            for (r, start), (state, flux, speed) in zip(group, carry):
                j, rows = start + unroll * k + u, pl.ds(8 * r, 8)
                next_state = load(r, j + 1)
                next_flux, next_speed = flux_of(next_state, axis_d)
                for c in range(5):
                    dq[c, j, rows, :] = next_state[c] - state[c]
                    df[c, j, rows, :] = next_flux[c] - flux[c]
                    fs[c, j, rows, :] = next_flux[c] + flux[c]
                m2[j, rows, :] = jnp.maximum(next_speed, speed)
                after.append((next_state, next_flux, next_speed))
            carry = after
        return carry

    begin = []
    for r, start in group:
        state = load(r, start)
        begin.append((state, *flux_of(state, axis_d)))
    lax.fori_loop(0, length, step, begin)


def face_fluxes(dq, df, fs, m2, faces, chunks, count, which):
    def face(k, carry):
        i = which(k)
        for r in range(chunks):
            rows = pl.ds(8 * r, 8)
            alpha = jnp.maximum(jnp.maximum(m2[i, rows, :], m2[i + 2, rows, :]), m2[i + 4, rows, :])
            for c in range(5):
                faces[c, i, rows, :] = face_value(
                    alpha,
                    [df[c, i + j, rows, :] for j in range(5)],
                    [dq[c, i + j, rows, :] for j in range(5)],
                    fs[c, i + 2, rows, :],
                )
        return carry

    lax.fori_loop(0, count, face, 0)


def z_turn(q, turned):
    for c in range(5):
        for blk in range(4):
            tile = jnp.transpose(q[c, pl.ds(128 * blk, 128), :]) * SCALE
            turned[c, pl.ds(160 * blk + 8, 72), :] = tile[:72]
            turned[c, pl.ds(160 * blk + 80, 72), :] = tile[56:]


def z_part(coef, out, turned, planes, dq, df, fs, m2, faces, diff):
    def gather(j, carry):
        for c in range(5):
            planes[c, j] = turned[c, pl.ds(j + 5, 8, stride=80), :]
        return carry

    lax.fori_loop(0, 70, gather, 0, unroll=2)
    differences(planes, dq, df, fs, m2, 2, ((0, 0), (0, 33)), 12, 3)
    face_fluxes(dq, df, fs, m2, faces, 1, 65, lambda k: k)

    def difference(i, carry):
        for c in range(5):
            diff[c, pl.ds(pl.multiple_of(8 * i, 8), 8), :] = coef * (faces[c, i + 1] - faces[c, i])
        return carry

    lax.fori_loop(0, 64, difference, 0, unroll=2)
    for c in range(5):
        for blk in range(4):
            tile = jnp.concatenate(
                [diff[c, pl.ds(2 * blk + half, 64, stride=8), :] for half in range(2)], axis=0
            )
            out[c, pl.ds(128 * blk, 128), :] = jnp.transpose(tile)


def y_inner(planes, dq, df, fs, m2, faces):
    both = ((0, 3), (1, 3))
    differences(planes, dq, df, fs, m2, 1, both, 10, 3)
    differences(planes, dq, df, fs, m2, 1, ((0, 33), (1, 33)), 1, 1)
    face_fluxes(dq, df, fs, m2, faces, 2, 27, lambda k: k + 3)


def y_part(coef, out, planes, dq, df, fs, m2, faces, diff):
    differences(planes, dq, df, fs, m2, 1, ((0, 0), (1, 0)), 1, 3)
    differences(planes, dq, df, fs, m2, 1, ((0, 34), (1, 34)), 1, 3)
    face_fluxes(dq, df, fs, m2, faces, 2, 6, lambda k: k + 27 * (k // 3))

    def difference(i, carry):
        for c in range(5):
            diff[c, pl.ds(pl.multiple_of(16 * i, 16), 16), :] = coef * (
                faces[c, i + 1] - faces[c, i]
            )
        return carry

    lax.fori_loop(0, 32, difference, 0)

    def back(x, carry):
        for c in range(5):
            for y8 in range(4):
                rows = pl.ds(pl.multiple_of(32 * x + 8 * y8, 8), 8)
                out[c, rows, :] += diff[c, pl.ds(128 * y8 + x, 8, stride=16), :]
        return carry

    lax.fori_loop(0, 16, back, 0)


def x_inner(planes, dq, df, fs, m2, faces):
    differences(planes, dq, df, fs, m2, 0, ((0, 3), (1, 3)), 5, 3)
    differences(planes, dq, df, fs, m2, 0, ((2, 3), (3, 3)), 5, 3)
    face_fluxes(dq, df, fs, m2, faces, 4, 11, lambda k: k + 3)


def x_part(coef, add, out, planes, dq, df, fs, m2, faces):
    for start in (0, 18):
        differences(planes, dq, df, fs, m2, 0, ((0, start), (1, start)), 1, 3)
        differences(planes, dq, df, fs, m2, 0, ((2, start), (3, start)), 1, 3)
    face_fluxes(dq, df, fs, m2, faces, 4, 6, lambda k: k + 11 * (k // 3))

    def finish(i, carry):
        rows = pl.ds(pl.multiple_of(32 * i, 32), 32)
        for c in range(5):
            out[c, rows, :] = add[c, rows, :] + coef * (faces[c, i + 1] - faces[c, i])
        return carry

    lax.fori_loop(0, 16, finish, 0)


def flow_kernel(coefs, q_in, out, q, turned, diff, add, send, recv, q_sem, *spaces):
    here = {a: lax.axis_index(a) for a in ("gx", "gy", "gz")}

    def beside(axis, step):
        return {**here, axis: lax.rem(here[axis] + step, lax.axis_size(axis))}

    sides = {a: (beside(a, 1), beside(a, lax.axis_size(a) - 1)) for a in here}
    fetch_q = pltpu.make_async_copy(q_in, q, q_sem)
    fetch_q.start()
    barrier = pltpu.get_barrier_semaphore()
    for up, down in sides.values():
        for device in (up, down):
            pl.semaphore_signal(barrier, inc=1, device_id=device, device_id_type=MESH)

    planes_x, planes_y = spaces[12], spaces[6]
    fetch_q.wait()

    def gather_x(j, carry):
        for c in range(5):
            planes_x[c, j + 3] = q[c, pl.ds(pl.multiple_of(32 * j, 32), 32), :] * SCALE
        return carry

    lax.fori_loop(0, 16, gather_x, 0)

    def gather_y(j, carry):
        for c in range(5):
            for h in range(2):
                planes_y[c, j + 3, pl.ds(8 * h, 8), :] = (
                    q[c, pl.ds(j + 256 * h, 8, stride=32), :] * SCALE
                )
        return carry

    lax.fori_loop(0, 32, gather_y, 0)
    pl.semaphore_wait(barrier, 6)
    slots = iter(range(12))

    def move(src, dst, device):
        k = next(slots)
        copy = pltpu.make_async_remote_copy(
            src_ref=src,
            dst_ref=dst,
            send_sem=send.at[k],
            recv_sem=recv.at[k],
            device_id=device,
            device_id_type=MESH,
        )
        copy.start()
        return copy

    along_y = [
        move(planes_y.at[:, pl.ds(32, 3)], planes_y.at[:, pl.ds(0, 3)], sides["gy"][0]),
        move(planes_y.at[:, pl.ds(3, 3)], planes_y.at[:, pl.ds(35, 3)], sides["gy"][1]),
    ]
    along_x = [
        move(planes_x.at[:, pl.ds(16, 3)], planes_x.at[:, pl.ds(0, 3)], sides["gx"][0]),
        move(planes_x.at[:, pl.ds(3, 3)], planes_x.at[:, pl.ds(19, 3)], sides["gx"][1]),
    ]
    z_turn(q, turned)
    along_z = []
    for blk in range(4):
        low, high = turned.at[:, pl.ds(160 * blk, 8)], turned.at[:, pl.ds(160 * blk + 152, 8)]
        first, last = turned.at[:, pl.ds(160 * blk + 8, 8)], turned.at[:, pl.ds(160 * blk + 144, 8)]
        along_z.append(move(last, low, sides["gz"][0]))
        along_z.append(move(first, high, sides["gz"][1]))
    y_inner(*spaces[6:12])
    for copy in along_z:
        copy.wait_recv()
    z_part(coefs[2], add, turned, *spaces[0:6], diff)
    x_inner(*spaces[12:18])
    for copy in along_y:
        copy.wait_recv()
    y_part(coefs[1], add, *spaces[6:12], diff)
    for copy in along_x:
        copy.wait_recv()
    x_part(coefs[0], add, out, *spaces[12:18])
    for copy in along_x + along_y + along_z:
        copy.wait_send()


def sweep_scratch(cells, rows):
    f32 = jnp.float32
    return [
        pltpu.VMEM((5, cells + 6, rows, 128), f32),
        pltpu.VMEM((5, cells + 5, rows, 128), f32),
        pltpu.VMEM((5, cells + 5, rows, 128), f32),
        pltpu.VMEM((5, cells + 5, rows, 128), f32),
        pltpu.VMEM((cells + 5, rows, 128), f32),
        pltpu.VMEM((5, cells + 1, rows, 128), f32),
    ]


def flow_change(section, counts, step_size):
    f32 = jnp.float32
    coefs = [0.25 * step_size * n / (2.0 * SCALE) for n in counts]
    return pl.pallas_call(
        functools.partial(flow_kernel, coefs),
        out_shape=jax.ShapeDtypeStruct((5, 512, 128), f32),
        in_specs=[pl.BlockSpec(memory_space=pl.ANY)],
        scratch_shapes=[pltpu.VMEM((5, 512, 128), f32), pltpu.VMEM((5, 640, 128), f32)]
        + [pltpu.VMEM((5, 512, 128), f32)] * 2
        + [pltpu.SemaphoreType.DMA((12,)), pltpu.SemaphoreType.DMA((12,)), pltpu.SemaphoreType.DMA]
        + sweep_scratch(64, 8)
        + sweep_scratch(32, 16)
        + sweep_scratch(16, 32),
        compiler_params=pltpu.CompilerParams(
            vmem_limit_bytes=63 * 2**20, collective_id=0, has_side_effects=True
        ),
        cost_estimate=pl.CostEstimate(flops=100_000_000, bytes_accessed=6_000_000, transcendentals=0),
        name="flow",
    )(section)


def dft_table(sample_count, freq_count):
    times = np.arange(sample_count)[None, :]
    orders = np.arange(1, freq_count + 1)[:, None]
    phases = 2.0 * math.pi / sample_count * (times * orders % sample_count)
    scaling = 1.0 / math.sqrt(sample_count)
    table = np.concatenate([np.cos(phases), -np.sin(phases)], axis=0).astype(np.float32) * scaling
    return jnp.asarray(table.astype(np.float32).astype(jnp.bfloat16))


def sin_cos(turns):
    rest = turns - jnp.round(turns)
    half = rest * rest
    s = (3.1996934769709044, -14.868610848632139, 42.01616577638672, -76.70155116950977,
         81.60502462208919, -41.341697068940945, 6.283185307179586)
    c = (6.529609897637814, -25.96831291454545, 60.167831622681774, -85.45016553628534,
         64.93911898307624, -19.73920453207708, 1.0)
    sine = jnp.full_like(half, s[0])
    for k in s[1:]:
        sine = sine * half + k
    cosine = jnp.full_like(half, c[0])
    for k in c[1:]:
        cosine = cosine * half + k
    return sine * rest, cosine


OBS_CHUNK = 256


def in_pieces(values):
    pieces = []
    for _ in range(3):
        piece = values.astype(jnp.bfloat16).astype(jnp.float32)
        pieces.append(piece)
        values = values - piece
    return pieces


PAIRS = ((0, 0), (0, 1), (1, 0), (0, 2), (1, 1), (2, 0))


GROUP = 4
GROUPS = 8
PAIR = 2


def panel_kernel(
    counts, live, change, old, section, record, cells, angles, ears, ranges, table,
    out, updated, state, olds, sections, records, pieces, heard, shown, spectra, sems,
):
    groups = (live[0] + GROUP - 1) // GROUP
    origin = [lax.axis_index(a) * n for a, n in zip(("gx", "gy", "gz"), (16, 32, 128))]

    def fetch(g):
        return pltpu.make_async_copy(
            record.at[pl.ds(128 * GROUP * g, 128 * GROUP)], records.at[g], sems.at[g]
        )

    def bring(first, count, sem):
        rows = pl.ds(first, count)
        return [
            pltpu.make_async_copy(change.at[rows], state.at[rows], sems.at[sem]),
            pltpu.make_async_copy(old.at[rows], olds.at[rows], sems.at[sem + 1]),
            pltpu.make_async_copy(section.at[rows], sections.at[rows], sems.at[sem + 2]),
        ]

    def finish(c):
        state[c] = (0.75 * olds[c] + 0.25 * sections[c]) - state[c]

    density_in, rest_in = bring(0, 1, GROUPS), bring(1, 4, GROUPS + 3)
    density_out = pltpu.make_async_copy(state.at[0], updated.at[0], sems.at[GROUPS + 6])
    rest_out = pltpu.make_async_copy(
        state.at[pl.ds(1, 4)], updated.at[pl.ds(1, 4)], sems.at[GROUPS + 7]
    )
    for copy in density_in:
        copy.start()
    for g in range(GROUPS):
        pl.when(g < groups)(fetch(g).start)
    for copy in rest_in:
        copy.start()

    out[...] = jnp.zeros_like(out)
    place = lax.broadcasted_iota(jnp.int32, (8, 128), 0)
    half_turn = 0.5 / math.pi

    def tile(*rows):
        made = jnp.where(place == 0, rows[0], 0.0)
        for k, row in enumerate(rows[1:], 1):
            made = jnp.where(place == k, row, made)
        return made

    def direction(sine, cosine):
        return cosine[0:1] * cosine[1:2], cosine[0:1] * sine[1:2], sine[0:1]

    def turned_angles(pair):
        row = lax.broadcasted_iota(jnp.int32, pair.shape, 0)
        return pair * jnp.where(row == 0, 0.5 * half_turn, half_turn)

    for k in range(8):
        lanes = pl.ds(128 * k, 128)
        reach = ranges[:, lanes]
        spot = [reach * d for d in direction(*sin_cos(turned_angles(ears[:, lanes])))]
        far = (spot[0] * spot[0] + spot[1] * spot[1]) + spot[2] * spot[2]
        split = in_pieces(tile(*spot, jnp.ones_like(far), far))
        heard[:, lanes] = jnp.concatenate([split[t] for _, t in PAIRS], axis=0).astype(jnp.bfloat16)
        shown[:, lanes] = tile(*spot)

    for copy in density_in:
        copy.wait()
    finish(0)
    turned = jnp.concatenate(
        [jnp.transpose(state[0, pl.ds(128 * k, 128), :]) for k in range(4)], axis=1
    )
    for k, piece in enumerate(in_pieces(turned)):
        pieces[pl.ds(128 * k, 128), :] = piece.astype(jnp.bfloat16)
    density_out.start()

    def front(g, carry):
        cell = cells[g]
        grid_row = lax.broadcasted_iota(jnp.int32, (512, 128 * GROUP), 0)
        chosen = jnp.where(grid_row == cell // 128, 1.0, 0.0).astype(jnp.bfloat16)
        found = jnp.dot(pieces[...], chosen, preferred_element_type=jnp.float32)
        found = (found[:128] + found[128:256]) + found[256:]
        lane = lax.broadcasted_iota(jnp.int32, (128, 128 * GROUP), 0)
        sampled = jnp.sum(jnp.where(lane == cell % 128, found, 0.0), axis=0, keepdims=True)
        column = jnp.transpose(jnp.broadcast_to(sampled, (8, 128 * GROUP)))[:, 0:1]
        fetch(g).wait()
        sources = (records[g].astype(jnp.float32) * column).astype(jnp.bfloat16)
        made = lax.dot_general(
            table[...], sources, (((1,), (1,)), ((), ())), preferred_element_type=jnp.float32
        ).astype(jnp.bfloat16)
        for k in range(GROUP):
            spectra[GROUP * g + k] = made[:, 128 * k : 128 * (k + 1)]
        return carry

    lax.fori_loop(0, groups, front, 0)

    order = (place + 1).astype(jnp.float32)

    def features(b, alive):
        cell = cells[b // GROUP, :, pl.ds(pl.multiple_of(128 * lax.rem(b, GROUP), 128), 128)]
        along = (cell >> 12, (cell >> 7) & 31, cell & 127)
        spot = [
            ((origin[d] + along[d]).astype(jnp.float32) + 0.5) * (1.0 / counts[d]) - 0.5
            for d in range(3)
        ]
        lanes = pl.ds(pl.multiple_of(128 * b, 128), 128)
        normal = direction(*sin_cos(turned_angles(angles[:, lanes])))
        normal = [n * (alive * (0.25 / math.pi)) for n in normal]
        across = -((normal[0] * spot[0] + normal[1] * spot[1]) + normal[2] * spot[2])
        square = (spot[0] * spot[0] + spot[1] * spot[1]) + spot[2] * spot[2]
        twice = [-2.0 * p for p in spot]
        facing = in_pieces(tile(*normal, across))
        apart = in_pieces(tile(*twice, square, jnp.ones_like(square)))
        seen = jnp.concatenate(
            [jnp.concatenate([facing[s], apart[s]], axis=1) for s, _ in PAIRS], axis=0
        ).astype(jnp.bfloat16)
        return seen, jnp.sum(tile(*twice), axis=1, keepdims=True)

    def turns_of(centre, first):
        apart = shown[:, pl.ds(first, 128)] + centre * (1.0 / 256.0)
        square = jnp.sum(apart * apart, axis=0, keepdims=True)
        return square * lax.rsqrt(square) * (WAVE_STEP * half_turn)

    def weights_of(seen, o):
        both = lax.dot_general(
            seen,
            heard[:, OBS_CHUNK * o : OBS_CHUNK * (o + 1)],
            (((0,), (0,)), ((), ())),
            preferred_element_type=jnp.float32,
        )
        return (both[:128] / both[128:]).astype(jnp.bfloat16)

    def add_turned(centre, o, product):
        for h in range(OBS_CHUNK // 128):
            lanes = slice(128 * h, 128 * h + 128)
            base = turns_of(centre, OBS_CHUNK * o + 128 * h)
            sine, cosine = sin_cos(base * order)
            step_s = jnp.broadcast_to(sine[7:8], (8, 128))
            step_c = jnp.broadcast_to(cosine[7:8], (8, 128))
            before_s = sine * step_c - cosine * step_s
            before_c = cosine * step_c + sine * step_s
            twice = step_c + step_c
            for a in range(FREQS // 8):
                re = product[8 * a : 8 * a + 8, lanes]
                im = product[FREQS + 8 * a : FREQS + 8 * a + 8, lanes]
                out[o, 0, 2 * a + h] += re * cosine + im * sine
                out[o, 1, 2 * a + h] += im * cosine - re * sine
                if a + 1 < FREQS // 8:
                    sine, before_s = twice * sine - before_s, sine
                    cosine, before_c = twice * cosine - before_c, cosine

    def back(pair, carry):
        blocks = []
        for k in range(PAIR):
            b = PAIR * pair + k
            alive = jnp.where(b < live[0], 1.0, 0.0)
            blocks.append((*features(b, alive), spectra[b]))
        for o in range(1024 // OBS_CHUNK):
            for seen, centre, spectrum in blocks:
                product = jnp.dot(
                    spectrum, weights_of(seen, o), preferred_element_type=jnp.float32
                )
                add_turned(centre, o, product)
        return carry

    lax.fori_loop(0, (live[0] + PAIR - 1) // PAIR, back, 0)
    for copy in rest_in:
        copy.wait()
    for c in range(1, 5):
        finish(c)
    rest_out.start()
    density_out.wait()
    rest_out.wait()


def panel_sums(counts, live_count, change, old, section, record, cells, angles, ears, ranges, table):
    vmem, anywhere = pl.BlockSpec(memory_space=pltpu.VMEM), pl.BlockSpec(memory_space=pl.ANY)
    bf16, f32 = jnp.bfloat16, jnp.float32
    return pl.pallas_call(
        functools.partial(panel_kernel, counts),
        out_shape=(
            jax.ShapeDtypeStruct((1024 // OBS_CHUNK, 2, TILES, 8, 128), f32),
            jax.ShapeDtypeStruct((5, 512, 128), f32),
        ),
        in_specs=[pl.BlockSpec(memory_space=pltpu.SMEM)] + [anywhere] * 4 + [vmem] * 5,
        out_specs=(vmem, anywhere),
        scratch_shapes=[pltpu.VMEM((5, 512, 128), f32)] * 3
        + [
            pltpu.VMEM((GROUPS, 128 * GROUP, 512), bf16),
            pltpu.VMEM((384, 512), bf16),
            pltpu.VMEM((8 * len(PAIRS), 1024), bf16),
            pltpu.VMEM((8, 1024), f32),
            pltpu.VMEM((32, 256, 128), bf16),
            pltpu.SemaphoreType.DMA((GROUPS + 8,)),
        ],
        compiler_params=pltpu.CompilerParams(vmem_limit_bytes=63 * 2**20),
        cost_estimate=pl.CostEstimate(
            flops=4_000_000_000, bytes_accessed=8_000_000, transcendentals=0
        ),
        name="panels",
    )(live_count, change, old, section, record, cells, angles, ears, ranges, table)


def local(
    state_old,
    state_section,
    panel_record,
    panel_cell,
    panel_angles,
    owned_blocks,
    listener_angles,
    listener_range,
):
    cells = state_section.shape[1:]
    counts = tuple(n * lax.axis_size(a) for n, a in zip(cells, ("gx", "gy", "gz")))
    section = state_section.reshape(5, 512, 128)
    change = flow_change(section, counts, COURANT / max(counts))
    part, updated = panel_sums(
        counts,
        owned_blocks,
        change,
        state_old.reshape(5, 512, 128),
        section,
        panel_record,
        panel_cell.reshape(GROUPS, 1, 128 * GROUP),
        panel_angles,
        listener_angles,
        listener_range.reshape(1, -1),
        dft_table(panel_record.shape[1], FREQS),
    )
    return updated.reshape(state_section.shape), jnp.transpose(summed_spectra(part), (0, 2, 1))


def solution(mesh):
    return jax.shard_map(
        local,
        mesh=mesh,
        in_specs=(
            P(None, "gx", "gy", "gz"),
            P(None, "gx", "gy", "gz"),
            P(("gx", "gy", "gz"), None),
            P(("gx", "gy", "gz"), None),
            P(None, ("gx", "gy", "gz")),
            P(("gx", "gy", "gz")),
            P(),
            P(),
        ),
        out_specs=(P(None, "gx", "gy", "gz"), P(None, "gz", None)),
        check_vma=False,
    )
```
